16 devices in a mesh: data: 2 (over y, z), dap: 8 (over x, core).
Axes of the slice: x: 4, y: 2, z: 1, core: 2. Of those that a mesh axis runs over, the one named last changes fastest.
The devices are a block of a 4x4x8 slice.
Arguments:
- msa_act: bfloat16 [4, 128, 96, 64], P('data', 'dap'), parts along dimension 0
- pair_act: bfloat16 [4, 96, 96, 128], P('data', 'dap'), parts along dimension 0
- msa_mask: int32 [4, 128, 96], P('data'), parts along dimension 0
- res_mask: int32 [4, 96], P('data'), parts along dimension 0
- w_row_bias: bfloat16 [128, 8], replicated
- w_row_qkvg: bfloat16 [64, 4, 8, 8], replicated
- w_row_out: bfloat16 [8, 8, 64], replicated
- w_col_qkvg: bfloat16 [64, 4, 8, 8], replicated
- w_col_out: bfloat16 [8, 8, 64], replicated
- w_opm_ac: bfloat16 [64, 2, 32], replicated
- w_opm_out: bfloat16 [32, 32, 128], replicated
- w_ts_bias: bfloat16 [128, 4], replicated
- w_ts_qkvg: bfloat16 [128, 4, 4, 32], replicated
- w_ts_out: bfloat16 [4, 32, 128], replicated
- w_te_bias: bfloat16 [128, 4], replicated
- w_te_qkvg: bfloat16 [128, 4, 4, 32], replicated
- w_te_out: bfloat16 [4, 32, 128], replicated
Outputs:
- output 1: bfloat16 [4, 128, 96, 64], P('data', 'dap'), parts along dimension 0
- output 2: bfloat16 [4, 96, 96, 128], P('data', 'dap'), parts along dimension 0
There are 2 independent parts. The reference program is written for one: setup_inputs(seed, part) draws one part's arguments, and reference() takes and returns one part's arrays. A program takes and returns all parts, laid end to end along the dimension named above; an argument that names none is the same for every part.
All inputs are finite; a program needn't handle non-finite values.
Results may differ from the reference program's by a relative error of at most 0.0157901.
Values are sent between devices in bfloat16 or wider.
A program may use at most 768 MiB of HBM per device.

```python
import jax
import jax.numpy as jnp
from jax import lax

CROPS = 2
NS = 128
NR = 96
C_M = 64
C_Z = 128
MSA_HEADS = 8
MSA_HEAD = 8
TRI_HEADS = 4
TRI_HEAD = 32
OPM_DIM = 32
SCORE_ELEMS = 8388608
MASK_SCALE = 10000.0
LN_EPS = 1e-5
OPM_EPS = 1e-3


def as_float(tensor):
    return tensor.astype(jnp.float32)


def layer_norm(tensor):
    x_float = tensor.astype(jnp.float32)
    mean_val = jnp.mean(x_float, axis=-1, keepdims=True)
    centred = x_float - mean_val
    var_val = jnp.mean(centred * centred, axis=-1, keepdims=True)
    return (centred * lax.rsqrt(var_val + LN_EPS)).astype(jnp.bfloat16)


def mask_to_bias(mask):
    return (mask.astype(jnp.float32) - 1.0) * MASK_SCALE


def rows_per_map(n_rows, per_row):
    return max(1, min(n_rows, SCORE_ELEMS // per_row))


def gated_attention(x_row, key_bias, pair_bias, w_qkvg, w_out):
    normed = layer_norm(x_row)
    proj_all = jnp.einsum('lc,cghd->glhd', as_float(normed), as_float(w_qkvg))
    queries = proj_all[0].astype(jnp.bfloat16)
    keys_bf = proj_all[1].astype(jnp.bfloat16)
    values_bf = proj_all[2].astype(jnp.bfloat16)
    gate_sig = jax.nn.sigmoid(proj_all[3])
    inv_sqrt = queries.shape[-1] ** -0.5
    logits = jnp.einsum('qhd,khd->hqk', as_float(queries), as_float(keys_bf)) * inv_sqrt + key_bias
    if pair_bias is not None:
        logits = logits + as_float(pair_bias)
    attn_prob = jax.nn.softmax(logits, axis=-1).astype(jnp.bfloat16)
    mixed = jnp.einsum('hqk,khd->qhd', as_float(attn_prob), as_float(values_bf)) * gate_sig
    update = jnp.einsum('qhd,hdc->qc', as_float(mixed.astype(jnp.bfloat16)), as_float(w_out))
    return (x_row.astype(jnp.float32) + update).astype(jnp.bfloat16)


def attend_rows(row_stack, key_rows, pair_bias, w_qkvg, w_out):
    n_rows = row_stack.shape[0]
    length = row_stack.shape[1]
    n_heads = w_qkvg.shape[2]
    return lax.map(lambda row_in: gated_attention(row_in[0], row_in[1], pair_bias, w_qkvg, w_out),
                   (row_stack, key_rows), batch_size=rows_per_map(n_rows, n_heads * length * length))


def pair_bias_of(pair_act, w_bias):
    return jnp.einsum('ijc,ch->hij', as_float(layer_norm(pair_act)), as_float(w_bias)).astype(jnp.bfloat16)


def triangle_start(pair_act, res_mask, w_bias, w_qkvg, w_out):
    n_res = pair_act.shape[0]
    key_rows = jnp.broadcast_to(mask_to_bias(res_mask)[None, :], (n_res, n_res))
    return attend_rows(pair_act, key_rows, pair_bias_of(pair_act, w_bias), w_qkvg, w_out)


def outer_product_mean(msa_act, pair_act, msa_mask, w_opm_ac, w_opm_out):
    mask_t = msa_mask.astype(jnp.float32).T
    proj_ac = jnp.einsum('sic,cpe->pise', as_float(layer_norm(msa_act)), as_float(w_opm_ac)).astype(jnp.bfloat16)
    left_proj = as_float(proj_ac[0]) * mask_t[:, :, None]
    right_proj = as_float(proj_ac[1]) * mask_t[:, :, None]
    norm_pairs = jnp.dot(mask_t, mask_t.T)
    n_res = right_proj.shape[0]
    width = right_proj.shape[2]

    def one_row(row_in):
        left_row, norm_row, pair_row = row_in
        outer = jnp.einsum('se,jsf->jef', left_row, right_proj) / (norm_row[:, None, None] + OPM_EPS)
        update = jnp.einsum('jef,efc->jc', as_float(outer.astype(jnp.bfloat16)), as_float(w_opm_out))
        return (pair_row.astype(jnp.float32) + update).astype(jnp.bfloat16)

    return lax.map(one_row, (left_proj, norm_pairs, pair_act), batch_size=rows_per_map(n_res, n_res * width * width))


def evoformer_crop(msa_act, pair_act, msa_mask, res_mask, weights):
    (w_row_bias, w_row_qkvg, w_row_out, w_col_qkvg, w_col_out, w_opm_ac, w_opm_out,
     w_ts_bias, w_ts_qkvg, w_ts_out, w_te_bias, w_te_qkvg, w_te_out) = weights
    msa_act = attend_rows(msa_act, mask_to_bias(msa_mask), pair_bias_of(pair_act, w_row_bias), w_row_qkvg, w_row_out)
    msa_cols = attend_rows(jnp.swapaxes(msa_act, 0, 1), mask_to_bias(msa_mask.T), None, w_col_qkvg, w_col_out)
    msa_act = jnp.swapaxes(msa_cols, 0, 1)
    pair_act = outer_product_mean(msa_act, pair_act, msa_mask, w_opm_ac, w_opm_out)
    pair_act = triangle_start(pair_act, res_mask, w_ts_bias, w_ts_qkvg, w_ts_out)
    pair_cols = triangle_start(jnp.swapaxes(pair_act, 0, 1), res_mask, w_te_bias, w_te_qkvg, w_te_out)
    return msa_act, jnp.swapaxes(pair_cols, 0, 1)


def normal_weight(key, shape, fan_in, gain):
    return (jax.random.normal(key, shape, jnp.float32) * (gain * fan_in ** -0.5)).astype(jnp.bfloat16)


def qkvg_weight(key, width, n_heads, head_dim):
    gains = jnp.array([1.5, 1.5, 1.0, 1.0], jnp.float32)[None, :, None, None]
    draw = jax.random.normal(key, (width, 4, n_heads, head_dim), jnp.float32)
    return (draw * gains * width ** -0.5).astype(jnp.bfloat16)


def setup_inputs(seed: int = 0, part: int = 0) -> dict:
    part_keys = jax.random.split(jax.random.fold_in(jax.random.key(seed), part), 5)
    w_keys = jax.random.split(jax.random.key(seed + 1), 13)
    base = jax.random.normal(part_keys[0], (CROPS, 1, NR, C_M), jnp.float32)
    noise = jax.random.normal(part_keys[1], (CROPS, NS, NR, C_M), jnp.float32)
    msa_act = (0.6 * base + 0.8 * noise).astype(jnp.bfloat16)
    pair_act = jax.random.normal(part_keys[2], (CROPS, NR, NR, C_Z), jnp.float32).astype(jnp.bfloat16)
    msa_mask = (jax.random.randint(part_keys[3], (CROPS, NS, NR), 0, 5) > 0).astype(jnp.int32)
    res_mask = (jax.random.randint(part_keys[4], (CROPS, NR), 0, 4) > 0).astype(jnp.int32)
    msa_width = MSA_HEADS * MSA_HEAD
    tri_width = TRI_HEADS * TRI_HEAD
    return {
        'msa_act': msa_act,
        'pair_act': pair_act,
        'msa_mask': msa_mask,
        'res_mask': res_mask,
        'w_row_bias': normal_weight(w_keys[0], (C_Z, MSA_HEADS), C_Z, 2.0),
        'w_row_qkvg': qkvg_weight(w_keys[1], C_M, MSA_HEADS, MSA_HEAD),
        'w_row_out': normal_weight(w_keys[2], (MSA_HEADS, MSA_HEAD, C_M), msa_width, 1.0),
        'w_col_qkvg': qkvg_weight(w_keys[3], C_M, MSA_HEADS, MSA_HEAD),
        'w_col_out': normal_weight(w_keys[4], (MSA_HEADS, MSA_HEAD, C_M), msa_width, 1.0),
        'w_opm_ac': normal_weight(w_keys[5], (C_M, 2, OPM_DIM), C_M, 1.0),
        'w_opm_out': normal_weight(w_keys[6], (OPM_DIM, OPM_DIM, C_Z), OPM_DIM * OPM_DIM, 1.0),
        'w_ts_bias': normal_weight(w_keys[7], (C_Z, TRI_HEADS), C_Z, 2.0),
        'w_ts_qkvg': qkvg_weight(w_keys[8], C_Z, TRI_HEADS, TRI_HEAD),
        'w_ts_out': normal_weight(w_keys[9], (TRI_HEADS, TRI_HEAD, C_Z), tri_width, 1.0),
        'w_te_bias': normal_weight(w_keys[10], (C_Z, TRI_HEADS), C_Z, 2.0),
        'w_te_qkvg': qkvg_weight(w_keys[11], C_Z, TRI_HEADS, TRI_HEAD),
        'w_te_out': normal_weight(w_keys[12], (TRI_HEADS, TRI_HEAD, C_Z), tri_width, 1.0),
    }


def reference(msa_act, pair_act, msa_mask, res_mask, w_row_bias, w_row_qkvg, w_row_out, w_col_qkvg, w_col_out,
              w_opm_ac, w_opm_out, w_ts_bias, w_ts_qkvg, w_ts_out, w_te_bias, w_te_qkvg, w_te_out):
    weights = (w_row_bias, w_row_qkvg, w_row_out, w_col_qkvg, w_col_out, w_opm_ac, w_opm_out,
               w_ts_bias, w_ts_qkvg, w_ts_out, w_te_bias, w_te_qkvg, w_te_out)
    msa_out, pair_out = lax.map(lambda crop_in: evoformer_crop(crop_in[0], crop_in[1], crop_in[2], crop_in[3], weights),
                                (msa_act, pair_act, msa_mask, res_mask))
    return msa_out, pair_out
```

```python
import functools
import math

import jax
import jax.numpy as jnp
from jax import lax
from jax.experimental import pallas as pl
from jax.experimental.pallas import tpu as pltpu
from jax.sharding import PartitionSpec as P

MASK_SCALE = 10000.0
LN_EPS = 1e-5
OPM_EPS = 1e-3
N_WEIGHTS = 13
PART_AXIS = 'data'
GROUP_AXIS = 'dap'
LOG2E = math.log2(math.e)
PAD_BIAS = -1e30
LANES = 128
SLOT = 16
F32 = jnp.float32
BF16 = jnp.bfloat16
NN = (((1,), (0,)), ((), ()))
NT = (((1,), (1,)), ((), ()))
TN = (((0,), (0,)), ((), ()))


def mm(lhs, rhs, dims=NN):
    return lax.dot_general(lhs, rhs, dims, preferred_element_type=F32)


def layer_norm(x_float):
    mean_val = jnp.mean(x_float, axis=-1, keepdims=True)
    centred = x_float - mean_val
    var_val = jnp.mean(centred * centred, axis=-1, keepdims=True)
    return (centred * lax.rsqrt(var_val + LN_EPS)).astype(BF16)


def iota(shape, axis):
    return lax.broadcasted_iota(jnp.int32, shape, axis)


def attend(keys, q_t, v_t, gate_t, bias_of, head_mask, n_heads, width):
    scale2 = LOG2E * width ** -0.5
    outs = []
    for pair in range(n_heads // 2):
        heads = (2 * pair, 2 * pair + 1)
        rhs = jnp.concatenate([q_t * head_mask[h] for h in heads], axis=1)
        raw = mm(keys, rhs)
        probs, scales = [], []
        for t, h in enumerate(heads):
            x = raw[:, t * LANES:(t + 1) * LANES] * scale2 + bias_of(h)
            e = jnp.exp2(x - jnp.max(x, axis=0, keepdims=True))
            scales.append(1.0 / jnp.sum(e, axis=0, keepdims=True))
            probs.append(e.astype(BF16))
        mixed = mm(v_t[2 * pair * width:2 * (pair + 1) * width], jnp.concatenate(probs, axis=1))
        outs.append(mixed[:width, :LANES] * scales[0])
        outs.append(mixed[width:, LANES:] * scales[1])
    return (jnp.concatenate(outs, axis=0) * gate_t).astype(BF16)


def body(cfg, *refs):
    n = cfg['n']
    (m_in, z_in, mask_in, res_in, w_rb, w_rq, w_ro, w_cq, w_co, w_ac, w_oo,
     w_sb, w_sq, w_so, w_eb, w_eq, w_eo, m_out, z_out,
     ag_r, ag_c, ag_s, ag_e, snd_m, rcv_m, snd_b, rcv_b, snd_z, rcv_z, zback,
     zw, xw, kbuf, qbuf, vbuf, gbuf, bias, obuf, stg_m, stg_c, stg_b, stg_z, abuf,
     mask_t, mask_r, res_r, hm8, hm4, wt_r, wt_c, wt_s, wt_e, wt_ac, w_oo_t, w_ro2, wt_b,
     send_sem, recv_sem) = refs
    crops, seqs, n_res, c_m = m_in.shape
    res = z_in.shape[1]
    c_z = z_in.shape[3]
    half = seqs // 2
    heads_m, heads_z = cfg['heads_m'], cfg['heads_z']
    d_m, d_z = c_m // heads_m, c_z // heads_z
    n_seq = n * seqs
    me = lax.axis_index(GROUP_AXIS)

    barrier = pltpu.get_barrier_semaphore()
    for r in range(1, n):
        pl.semaphore_signal(barrier, inc=1, device_id={GROUP_AXIS: lax.rem(me + r, n)},
                            device_id_type=pl.DeviceIdType.MESH)
    pl.semaphore_wait(barrier, n - 1)

    def copies(exch, c, src_of, dst):
        out = []
        for r in range(1, n):
            peer = lax.rem(me + r, n)
            out.append(pltpu.make_async_remote_copy(
                src_ref=src_of(peer), dst_ref=dst, send_sem=send_sem.at[exch, c, r], recv_sem=recv_sem.at[exch, c, r],
                device_id={GROUP_AXIS: peer}, device_id_type=pl.DeviceIdType.MESH))
        return out

    def arrivals(exch, c, slot_of):
        for r in range(1, n):
            sender = lax.rem(me + n - r, n)
            ref = slot_of(sender)
            pltpu.make_async_remote_copy(
                src_ref=ref, dst_ref=ref, send_sem=send_sem.at[exch, c, r], recv_sem=recv_sem.at[exch, c, r],
                device_id={GROUP_AXIS: sender}, device_id_type=pl.DeviceIdType.MESH).wait_recv()

    def gather_copies(exch, c, buf):
        return copies(exch, c, lambda peer: buf.at[c, me], buf.at[c, me])

    def gather_wait(exch, c, buf):
        arrivals(exch, c, lambda sender: buf.at[c, sender])

    def swap_copies(exch, c, snd, rcv):
        return copies(exch, c, lambda peer: snd.at[c, peer], rcv.at[c, me])

    def start(descs):
        for d in descs:
            d.start()

    def finish(descs):
        for d in descs:
            d.wait_send()

    def loop(count, fn):
        def step(i, carry):
            fn(i)
            return carry
        lax.fori_loop(0, count, step, 0)

    def pad_matrix():
        row, col = iota((LANES, n_res), 0), iota((LANES, n_res), 1)
        hit = (col == (row // SLOT) * res + row % SLOT) & (row % SLOT < res)
        return jnp.where(hit, 1.0, 0.0).astype(BF16)

    def head_rows(heads, width, ref):
        for h in range(heads):
            row = iota((heads * width, LANES), 0)
            ref[h] = jnp.where((row >= h * width) & (row < (h + 1) * width), 1.0, 0.0).astype(BF16)

    pad = pad_matrix()
    head_rows(heads_m, d_m, hm8)
    head_rows(heads_z, d_z, hm4)
    row, col = iota((LANES, LANES), 0), iota((LANES, LANES), 1)
    seq_of = ((col % (n_seq // 2)) // half) * seqs + (col // (n_seq // 2)) * half + col % half
    seq_perm = jnp.where(row == seq_of, 1.0, 0.0).astype(BF16)
    for c in range(crops):
        mask_bf = mask_in[c].astype(F32).astype(BF16)
        mask_t[c] = mm(mm(pad, mask_bf, NT).astype(BF16), seq_perm)
        mask_r[c] = mm(mask_bf, pad, NT)
    res_r[...] = mm(res_in[...].astype(F32).astype(BF16), pad, NT)

    def flip(w, ref):
        ref[...] = w.astype(F32).T.astype(BF16)

    flip(w_rq[...], wt_r)
    flip(w_cq[...], wt_c)
    flip(w_sq[...], wt_s)
    flip(w_eq[...], wt_e)
    flip(w_ac[...], wt_ac)
    for k, w in enumerate((w_rb, w_sb, w_eb)):
        wt_b[k] = jnp.zeros(wt_b.shape[1:], BF16)
        wt_b[k, :w.shape[1], :] = w[...].astype(F32).T.astype(BF16)
    w_ro2[...] = jnp.zeros(w_ro2.shape, BF16)
    w_ro2[:c_m, :c_m] = w_ro[...]
    w_ro2[c_m:, c_m:] = w_ro[...]
    o_w = w_ac.shape[1] // 2
    stg_z[:o_w * o_w, :] = w_oo[...].astype(F32)

    def oo_step(f):
        w_oo_t[pl.ds(pl.multiple_of(f * o_w, o_w), o_w), :] = stg_z[pl.ds(f, o_w, stride=o_w), :].astype(BF16)

    loop(o_w, oo_step)
    stg_b[...] = jnp.zeros(stg_b.shape, F32)
    stg_c[...] = jnp.zeros(stg_c.shape, F32)

    def put_bias(y, k, heads, i):
        b = mm(wt_b[k], y, NT)
        for h in range(heads):
            stg_b[h, pl.ds(i, 1), :] = b[h:h + 1, :]

    def project(y, wt, width, slot):
        p = mm(wt[...], y, NT)
        kbuf[slot, :, :width] = p[width:2 * width].T.astype(BF16)
        qbuf[slot, :width] = p[:width].astype(BF16)
        vbuf[slot, :width] = p[2 * width:3 * width].astype(BF16)
        gbuf[slot, :width] = jax.nn.sigmoid(p[3 * width:])

    def column(rowvec):
        return jnp.broadcast_to(rowvec, (LANES, LANES)).T

    def pad_bias(rowvec):
        lane = iota((1, LANES), 1)
        return jnp.where(lane % SLOT < res, (rowvec - 1.0) * (MASK_SCALE * LOG2E), PAD_BIAS)

    def row_bias(c):
        def step(i):
            z = mm(pad, z_in[c, i])
            zw[c, i] = z.astype(BF16)
            put_bias(layer_norm(z), 0, heads_m, i)
        loop(res, step)
        ag_r[c, me] = stg_b[...].astype(BF16)
        start(gather_copies(0, c, ag_r))

    loop(crops, row_bias)

    def row_attention(c):
        def prep(s):
            x2 = mm(pad, jnp.concatenate([m_in[c, s], m_in[c, s + half]], axis=1))
            xw[s] = x2
            for t in range(2):
                project(layer_norm(x2[:, t * c_m:(t + 1) * c_m]), wt_r, c_m, s + t * half)
        loop(half, prep)
        gather_wait(0, c, ag_r)
        for h in range(heads_m):
            b = jnp.concatenate([ag_r[c, p, h].astype(F32) for p in range(n)], axis=0)
            bias[h] = b.T * LOG2E

        def step(s):
            outs = []
            for t in range(2):
                slot = s + t * half
                mcol = column(pad_bias(mask_r[c, pl.ds(me * seqs + slot, 1), :]))
                outs.append(attend(kbuf[slot, :, :c_m], qbuf[slot, :c_m], vbuf[slot, :c_m], gbuf[slot, :c_m],
                                   lambda h: bias[h] + mcol, hm8, heads_m, d_m))
            x2 = xw[s] + mm(jnp.concatenate(outs, axis=0), w_ro2[...], TN)
            for p in range(n):
                stg_m[pl.ds(p * res * half + s, res, stride=half), :] = x2[p * SLOT:p * SLOT + res]
        loop(half, step)
        for p in range(n):
            snd_m[c, p] = stg_m[p * res * half:(p + 1) * res * half, :].reshape(res, half, LANES).astype(BF16)
        rcv_m[c, me] = snd_m[c, me]
        start(swap_copies(1, c, snd_m, rcv_m))

    loop(crops, row_attention)

    def col_attention(c):
        for r in range(1, n):
            pass
        arrivals(1, c, lambda sender: rcv_m.at[c, sender])

        def prep(i):
            x2 = jnp.concatenate([rcv_m[c, q, i].astype(F32) for q in range(n)], axis=0)
            x = jnp.concatenate([x2[:, :c_m], x2[:, c_m:]], axis=0)
            xw[i, :, :c_m] = x
            project(layer_norm(x), wt_c, c_m, i)
        loop(res, prep)

        def step(i):
            mrow = mask_t[c, pl.ds(me * SLOT + i, 1), :]
            mcol = column((mrow - 1.0) * (MASK_SCALE * LOG2E))
            out_t = attend(kbuf[i, :, :c_m], qbuf[i, :c_m], vbuf[i, :c_m], gbuf[i, :c_m],
                           lambda h: mcol, hm8, heads_m, d_m)
            x = (xw[i, :, :c_m] + mm(out_t, w_co[...], TN)).astype(BF16).astype(F32)
            x2 = jnp.concatenate([x[:n_seq // 2], x[n_seq // 2:]], axis=1)
            for q in range(n):
                snd_b[c, q, i] = x2[q * half:(q + 1) * half].astype(BF16)
            ac = mm(wt_ac[...], layer_norm(x), NT).astype(BF16).astype(F32) * mrow
            abuf[c, pl.ds(pl.multiple_of(i * o_w, o_w), o_w), :] = ac[:o_w].astype(BF16)
            stg_c[pl.ds(i, o_w, stride=SLOT), :] = ac[o_w:]
        loop(res, step)
        ag_c[c, me] = stg_c[...].reshape(o_w, SLOT, LANES).astype(BF16)
        start(gather_copies(2, c, ag_c))
        rcv_b[c, me] = snd_b[c, me]
        start(swap_copies(3, c, snd_b, rcv_b))

    loop(crops, col_attention)

    def outer_product(c):
        gather_wait(2, c, ag_c)
        stg_b[...] = jnp.zeros(stg_b.shape, F32)
        mloc = mask_t[c, pl.ds(pl.multiple_of(me * SLOT, SLOT), SLOT), :].astype(BF16)
        gbuf[0, :SLOT] = 1.0 / (mm(mloc, mask_t[c].astype(BF16), NT) + OPM_EPS)

        def outer(f):
            rhs = jnp.concatenate([ag_c[c, p, f] for p in range(n)], axis=0)
            out = mm(abuf[c], rhs, NT)
            for i in range(res):
                obuf[i, pl.ds(pl.multiple_of(f * o_w, o_w), o_w), :] = (
                    out[i * o_w:(i + 1) * o_w] * gbuf[0, i:i + 1, :]).astype(BF16)
        loop(o_w, outer)
        w_t = w_oo_t[...]

        def update(i2):
            rhs = jnp.concatenate([obuf[2 * i2], obuf[2 * i2 + 1]], axis=1)
            upd = mm(w_t, rhs, TN)
            for t in range(2):
                i = 2 * i2 + t
                z = (zw[c, i].astype(F32) + upd[:, t * LANES:(t + 1) * LANES].T).astype(BF16)
                zw[c, i] = z
                put_bias(layer_norm(z.astype(F32)), 1, heads_z, i)
        loop(res // 2, update)
        ag_s[c, me] = stg_b[:heads_z].astype(BF16)
        start(gather_copies(4, c, ag_s))

    loop(crops, outer_product)

    stg_z[...] = jnp.zeros(stg_z.shape, F32)

    def tri_start(c):
        def prep(i):
            project(layer_norm(zw[c, i].astype(F32)), wt_s, c_z, i)
        loop(res, prep)
        gather_wait(4, c, ag_s)
        mcol = column(pad_bias(res_r[pl.ds(c, 1), :]))
        for h in range(heads_z):
            b = jnp.concatenate([ag_s[c, p, h].astype(F32) for p in range(n)], axis=0)
            bias[h] = b.T * LOG2E + mcol
        stg_b[...] = jnp.zeros(stg_b.shape, F32)

        def step(i):
            out_t = attend(kbuf[i], qbuf[i], vbuf[i], gbuf[i], lambda h: bias[h], hm4, heads_z, d_z)
            z = (zw[c, i].astype(F32) + mm(out_t, w_so[...], TN)).astype(BF16).astype(F32)
            stg_z[pl.ds(i, LANES, stride=SLOT), :] = z
            put_bias(layer_norm(z), 2, heads_z, i)
        loop(res, step)
        ag_e[c, me] = stg_b[:heads_z].astype(BF16)
        start(gather_copies(5, c, ag_e))

        def pack(p):
            base = pl.multiple_of(p * SLOT * SLOT, SLOT * SLOT)
            snd_z[c, p] = stg_z[pl.ds(base, res * SLOT), :].reshape(res, SLOT, LANES).astype(BF16)
        loop(n, pack)
        rcv_z[c, me] = snd_z[c, me]
        start(swap_copies(6, c, snd_z, rcv_z))

    loop(crops, tri_start)

    def tri_end(c):
        arrivals(6, c, lambda sender: rcv_z.at[c, sender])

        def prep(j):
            x = jnp.concatenate([rcv_z[c, q, j] for q in range(n)], axis=0).astype(F32)
            project(layer_norm(x), wt_e, c_z, j)
        loop(res, prep)
        gather_wait(5, c, ag_e)
        mcol = column(pad_bias(res_r[pl.ds(c, 1), :]))
        for h in range(heads_z):
            b = jnp.concatenate([ag_e[c, p, h].astype(F32) for p in range(n)], axis=0)
            bias[h] = b * LOG2E + mcol

        def step(j):
            out_t = attend(kbuf[j], qbuf[j], vbuf[j], gbuf[j], lambda h: bias[h], hm4, heads_z, d_z)
            upd = mm(out_t, w_eo[...], TN)
            for q in range(n):
                rcv_z[c, q, j] = (rcv_z[c, q, j].astype(F32) + upd[q * SLOT:(q + 1) * SLOT]).astype(BF16)
        loop(res, step)
        zback[c, me] = rcv_z[c, me]
        start(swap_copies(7, c, rcv_z, zback))

    loop(crops, tri_end)

    def put_m(c):
        arrivals(3, c, lambda sender: rcv_b.at[c, sender])
        stg_m[...] = rcv_b[c].astype(F32).reshape(n * res * half, LANES)

        def step(s):
            x2 = stg_m[pl.ds(s, n_res, stride=half), :]
            m_out[c, s] = x2[:, :c_m].astype(BF16)
            m_out[c, s + half] = x2[:, c_m:].astype(BF16)
        loop(half, step)

    loop(crops, put_m)

    def put_z(c):
        arrivals(7, c, lambda sender: zback.at[c, sender])

        def unpack(p):
            base = pl.multiple_of(p * SLOT * SLOT, SLOT * SLOT)
            stg_z[pl.ds(base, res * SLOT), :] = zback[c, p].astype(F32).reshape(res * SLOT, LANES)
        loop(n, unpack)

        def step(i):
            x = stg_z[pl.ds(i, LANES, stride=SLOT), :].astype(BF16)
            z_out[c, i] = mm(pad, x, TN).astype(BF16)
        loop(res, step)

    loop(crops, put_z)

    def drain(c):
        finish(gather_copies(0, c, ag_r))
        finish(swap_copies(1, c, snd_m, rcv_m))
        finish(gather_copies(2, c, ag_c))
        finish(swap_copies(3, c, snd_b, rcv_b))
        finish(gather_copies(4, c, ag_s))
        finish(gather_copies(5, c, ag_e))
        finish(swap_copies(6, c, snd_z, rcv_z))
        finish(swap_copies(7, c, rcv_z, zback))

    loop(crops, drain)


def solution(mesh):
    n = mesh.shape[GROUP_AXIS]
    rows_spec = P(PART_AXIS, GROUP_AXIS, None, None)
    in_specs = (rows_spec, rows_spec, P(PART_AXIS, None, None), P(PART_AXIS, None)) + (P(),) * N_WEIGHTS

    def local_block(m, z, msa_mask, res_mask, w_rb, w_rq, w_ro, w_cq, w_co, w_ac, w_oo, w_sb, w_sq, w_so,
                    w_eb, w_eq, w_eo):
        crops, seqs, n_res, c_m = m.shape
        res, c_z = z.shape[1], z.shape[3]
        heads_m, heads_z = w_rq.shape[2], w_sq.shape[2]
        o_w = w_ac.shape[2]
        half = seqs // 2
        assert n * SLOT == LANES and res <= SLOT and n * seqs == LANES and 2 * c_m == LANES and c_z == LANES
        flat = lambda w: w.reshape(w.shape[0], -1)
        tall = lambda w: w.reshape(-1, w.shape[-1])
        args = (m, z, msa_mask, res_mask, w_rb, flat(w_rq), tall(w_ro), flat(w_cq), tall(w_co), flat(w_ac), tall(w_oo),
                w_sb, flat(w_sq), tall(w_so), w_eb, flat(w_eq), tall(w_eo))
        vm = pltpu.VMEM
        slots = max(seqs, res)
        scratch = [
            vm((crops, n, heads_m, SLOT, LANES), BF16),
            vm((crops, n, o_w, SLOT, LANES), BF16),
            vm((crops, n, heads_z, SLOT, LANES), BF16),
            vm((crops, n, heads_z, SLOT, LANES), BF16),
            vm((crops, n, res, half, LANES), BF16),
            vm((crops, n, res, half, LANES), BF16),
            vm((crops, n, res, half, LANES), BF16),
            vm((crops, n, res, half, LANES), BF16),
            vm((crops, n, res, SLOT, LANES), BF16),
            vm((crops, n, res, SLOT, LANES), BF16),
            vm((crops, n, res, SLOT, LANES), BF16),
            vm((crops, res, LANES, LANES), BF16),
            vm((slots, LANES, LANES), F32),
            vm((slots, LANES, LANES), BF16),
            vm((slots, LANES, LANES), BF16),
            vm((slots, LANES, LANES), BF16),
            vm((slots, LANES, LANES), F32),
            vm((heads_m, LANES, LANES), F32),
            vm((res, o_w * o_w, LANES), BF16),
            vm((n * res * half, LANES), F32),
            vm((o_w * SLOT, LANES), F32),
            vm((heads_m, SLOT, LANES), F32),
            vm((LANES * SLOT, LANES), F32),
            vm((crops, res * o_w, LANES), BF16),
            vm((crops, LANES, LANES), F32),
            vm((crops, n * seqs, LANES), F32),
            vm((crops, LANES), F32),
            vm((heads_m, c_m, LANES), BF16),
            vm((heads_z, c_z, LANES), BF16),
            vm((4 * c_m, c_m), BF16),
            vm((4 * c_m, c_m), BF16),
            vm((4 * c_z, c_z), BF16),
            vm((4 * c_z, c_z), BF16),
            vm((2 * o_w, c_m), BF16),
            vm((o_w * o_w, LANES), BF16),
            vm((LANES, LANES), BF16),
            vm((3, SLOT, LANES), BF16),
            pltpu.SemaphoreType.DMA((8, crops, n)),
            pltpu.SemaphoreType.DMA((8, crops, n)),
        ]
        cfg = dict(n=n, heads_m=heads_m, heads_z=heads_z)
        spec = pl.BlockSpec(memory_space=pltpu.VMEM)
        return pl.pallas_call(
            functools.partial(body, cfg),
            out_shape=(jax.ShapeDtypeStruct(m.shape, BF16), jax.ShapeDtypeStruct(z.shape, BF16)),
            in_specs=[spec] * len(args),
            out_specs=(spec, spec),
            scratch_shapes=scratch,
            compiler_params=pltpu.CompilerParams(collective_id=0, has_side_effects=True,
                                                 vmem_limit_bytes=60 * 1024 * 1024),
        )(*args)

    return jax.shard_map(local_block, mesh=mesh, in_specs=in_specs, out_specs=(rows_spec, rows_spec),
                         check_vma=False)
```

```python
import functools
import math

import jax
import jax.numpy as jnp
from jax import lax
from jax.experimental import pallas as pl
from jax.experimental.pallas import tpu as pltpu
from jax.sharding import PartitionSpec as P

MASK_SCALE = 10000.0
LN_EPS = 1e-5
OPM_EPS = 1e-3
N_WEIGHTS = 13
PART_AXIS = 'data'
GROUP_AXIS = 'dap'
LOG2E = math.log2(math.e)
PAD_BIAS = -1e30
LANES = 128
SLOT = 16
F32 = jnp.float32
BF16 = jnp.bfloat16
NN = (((1,), (0,)), ((), ()))
NT = (((1,), (1,)), ((), ()))
TN = (((0,), (0,)), ((), ()))


def mm(lhs, rhs, dims=NN):
    return lax.dot_general(lhs, rhs, dims, preferred_element_type=F32)


def layer_norm(x_float):
    mean_val = jnp.mean(x_float, axis=-1, keepdims=True)
    centred = x_float - mean_val
    var_val = jnp.mean(centred * centred, axis=-1, keepdims=True)
    return (centred * lax.rsqrt(var_val + LN_EPS)).astype(BF16)


def iota(shape, axis):
    return lax.broadcasted_iota(jnp.int32, shape, axis)


def body(cfg, *refs):
    n = cfg['n']
    (m_in, z_in, mask_in, res_in, w_rb, w_rq, w_ro, w_cq, w_co, w_ac, w_oo,
     w_sb, w_sq, w_so, w_eb, w_eq, w_eo, m_out, z_out,
     ag_r, ag_c, ag_s, ag_e, snd_m, rcv_m, snd_b, rcv_b, snd_z, rcv_z, zback,
     zw, xw, kbuf, qbuf, vbuf, gbuf, bias, obuf, stg_m, stg_c, stg_b, stg_z, abuf,
     mask_t, mask_r, res_r, raw, prob, inv, norm, hm8, hm4, wt_r, wt_c, wt_s, wt_e, wt_ac, w_oo_t, w_ro2, wt_b,
     send_sem, recv_sem) = refs
    crops, seqs, n_res, c_m = m_in.shape
    res = z_in.shape[1]
    c_z = z_in.shape[3]
    half = seqs // 2
    heads_m, heads_z = cfg['heads_m'], cfg['heads_z']
    d_m, d_z = c_m // heads_m, c_z // heads_z
    n_seq = n * seqs
    me = lax.axis_index(GROUP_AXIS)

    barrier = pltpu.get_barrier_semaphore()
    for r in range(1, n):
        pl.semaphore_signal(barrier, inc=1, device_id={GROUP_AXIS: lax.rem(me + r, n)},
                            device_id_type=pl.DeviceIdType.MESH)
    pl.semaphore_wait(barrier, n - 1)

    def copies(exch, c, src_of, dst):
        out = []
        for r in range(1, n):
            peer = lax.rem(me + r, n)
            out.append(pltpu.make_async_remote_copy(
                src_ref=src_of(peer), dst_ref=dst, send_sem=send_sem.at[exch, c, r], recv_sem=recv_sem.at[exch, c, r],
                device_id={GROUP_AXIS: peer}, device_id_type=pl.DeviceIdType.MESH))
        return out

    def arrivals(exch, c, slot_of):
        for r in range(1, n):
            sender = lax.rem(me + n - r, n)
            ref = slot_of(sender)
            pltpu.make_async_remote_copy(
                src_ref=ref, dst_ref=ref, send_sem=send_sem.at[exch, c, r], recv_sem=recv_sem.at[exch, c, r],
                device_id={GROUP_AXIS: sender}, device_id_type=pl.DeviceIdType.MESH).wait_recv()

    def gather_copies(exch, c, buf):
        return copies(exch, c, lambda peer: buf.at[c, me], buf.at[c, me])

    def gather_wait(exch, c, buf):
        arrivals(exch, c, lambda sender: buf.at[c, sender])

    def swap_copies(exch, c, snd, rcv):
        return copies(exch, c, lambda peer: snd.at[c, peer], rcv.at[c, me])

    def start(descs):
        for d in descs:
            d.start()

    def finish(descs):
        for d in descs:
            d.wait_send()

    def loop(count, fn):
        def step(i, carry):
            fn(i)
            return carry
        lax.fori_loop(0, count, step, 0)

    def pad_matrix():
        row, col = iota((LANES, n_res), 0), iota((LANES, n_res), 1)
        hit = (col == (row // SLOT) * res + row % SLOT) & (row % SLOT < res)
        return jnp.where(hit, 1.0, 0.0).astype(BF16)

    def head_rows(heads, width, ref):
        for h in range(heads):
            row = iota((heads * width, LANES), 0)
            ref[h] = jnp.where((row >= h * width) & (row < (h + 1) * width), 1.0, 0.0).astype(BF16)

    pad = pad_matrix()
    head_rows(heads_m, d_m, hm8)
    head_rows(heads_z, d_z, hm4)
    row, col = iota((LANES, LANES), 0), iota((LANES, LANES), 1)
    seq_of = ((col % (n_seq // 2)) // half) * seqs + (col // (n_seq // 2)) * half + col % half
    seq_perm = jnp.where(row == seq_of, 1.0, 0.0).astype(BF16)
    for c in range(crops):
        mask_bf = mask_in[c].astype(F32).astype(BF16)
        mask_t[c] = mm(mm(pad, mask_bf, NT).astype(BF16), seq_perm)
        mask_r[c] = mm(mask_bf, pad, NT)
    res_r[...] = mm(res_in[...].astype(F32).astype(BF16), pad, NT)

    def flip(w, ref):
        ref[...] = w.astype(F32).T.astype(BF16)

    flip(w_rq[...], wt_r)
    flip(w_cq[...], wt_c)
    flip(w_sq[...], wt_s)
    flip(w_eq[...], wt_e)
    flip(w_ac[...], wt_ac)
    for k, w in enumerate((w_rb, w_sb, w_eb)):
        wt_b[k] = jnp.zeros(wt_b.shape[1:], BF16)
        wt_b[k, :w.shape[1], :] = w[...].astype(F32).T.astype(BF16)
    w_ro2[...] = jnp.zeros(w_ro2.shape, BF16)
    w_ro2[:c_m, :c_m] = w_ro[...]
    w_ro2[c_m:, c_m:] = w_ro[...]
    o_w = w_ac.shape[1] // 2
    stg_z[:o_w * o_w, :] = w_oo[...].astype(F32)

    for k in range(0, o_w, LANES // o_w):
        rows = [stg_z[pl.ds(f, o_w, stride=o_w), :] for f in range(k, k + LANES // o_w)]
        w_oo_t[:, k * o_w:k * o_w + LANES] = jnp.concatenate(rows, axis=0).T.astype(BF16)

    stg_b[...] = jnp.zeros(stg_b.shape, F32)
    stg_c[...] = jnp.zeros(stg_c.shape, F32)

    def grouped(count, size, fn):
        while count % size:
            size -= 1

        def step(b, carry):
            fn([b * size + t for t in range(size)])
            return carry
        lax.fori_loop(0, count // size, step, 0)

    def put_bias(ys, k, heads, rows):
        b = mm(wt_b[k], jnp.concatenate(ys, axis=0), NT)
        for t, i in enumerate(rows):
            for h in range(heads):
                stg_b[h, pl.ds(i, 1), :] = b[h:h + 1, t * LANES:(t + 1) * LANES]

    def project(ys, wt, wk, width, slots):
        y = jnp.concatenate(ys, axis=0)
        p = mm(wt[...], y, NT)
        keys = mm(y, wk)
        for t, slot in enumerate(slots):
            cut = slice(t * LANES, (t + 1) * LANES)
            kbuf[slot, :, :width] = keys[cut].astype(BF16)
            qbuf[slot, :width] = p[:width, cut].astype(BF16)
            vbuf[slot, :width] = p[2 * width:3 * width, cut].astype(BF16)
            gbuf[slot, :width] = jax.nn.sigmoid(p[3 * width:, cut])

    def column(rowvec):
        return jnp.broadcast_to(rowvec, (LANES, LANES)).T

    def pad_bias(rowvec):
        lane = iota((1, LANES), 1)
        return jnp.where(lane % SLOT < res, (rowvec - 1.0) * (MASK_SCALE * LOG2E), PAD_BIAS)

    def attention(rows, heads, width, head_mask, bias_of, mask_of):
        c = heads * width
        scale2 = LOG2E * width ** -0.5

        def logits(idx):
            for i in idx:
                q_t, keys = qbuf[i, :c], kbuf[i, :, :c]
                for pair in range(heads // 2):
                    rhs = jnp.concatenate([q_t * head_mask[2 * pair], q_t * head_mask[2 * pair + 1]], axis=1)
                    raw[i, pair] = mm(keys, rhs)
        grouped(rows, cfg['k_logits'], logits)

        def softmax(idx):
            for i in idx:
                mcol = mask_of(i)
                for h in range(heads):
                    cut = slice((h % 2) * LANES, (h % 2 + 1) * LANES)
                    x = raw[i, h // 2, :, cut] * scale2
                    if bias_of is not None:
                        x = x + bias_of(h)
                    if mcol is not None:
                        x = x + mcol
                    e = jnp.exp2(x - jnp.max(x, axis=0, keepdims=True))
                    inv[i, h:h + 1, :] = 1.0 / jnp.sum(e, axis=0, keepdims=True)
                    prob[i, h // 2, :, cut] = e.astype(BF16)
        grouped(rows, cfg['k_softmax'], softmax)

    def mixed(idx, heads, width):
        c = heads * width
        raws = [[mm(vbuf[i, 2 * p * width:2 * (p + 1) * width], prob[i, p]) for p in range(heads // 2)] for i in idx]
        outs = []
        for i, r in zip(idx, raws):
            parts = []
            for p in range(heads // 2):
                parts.append(r[p][:width, :LANES] * inv[i, 2 * p:2 * p + 1, :])
                parts.append(r[p][width:, LANES:] * inv[i, 2 * p + 1:2 * p + 2, :])
            outs.append((jnp.concatenate(parts, axis=0) * gbuf[i, :c]).astype(BF16))
        return outs

    def row_bias(c):
        def step(idx):
            zs = [mm(pad, z_in[c, i]) for i in idx]
            for i, z in zip(idx, zs):
                zw[c, i] = z.astype(BF16)
            put_bias([layer_norm(z) for z in zs], 0, heads_m, idx)
        grouped(res, 4, step)
        ag_r[c, me] = stg_b[...].astype(BF16)
        start(gather_copies(0, c, ag_r))

    loop(crops, row_bias)

    def row_attention(c):
        def prep(idx):
            xs = [mm(pad, jnp.concatenate([m_in[c, s], m_in[c, s + half]], axis=1)) for s in idx]
            for s, x2 in zip(idx, xs):
                xw[s] = x2
            ys = [layer_norm(x2[:, t * c_m:(t + 1) * c_m]) for x2 in xs for t in range(2)]
            project(ys, wt_r, w_rq[:, c_m:2 * c_m], c_m, [s + t * half for s in idx for t in range(2)])
        grouped(half, 2, prep)
        gather_wait(0, c, ag_r)
        for h in range(heads_m):
            b = jnp.concatenate([ag_r[c, p, h].astype(F32) for p in range(n)], axis=0)
            bias[h] = b.T * LOG2E
        attention(seqs, heads_m, d_m, hm8, lambda h: bias[h],
                  lambda i: column(pad_bias(mask_r[c, pl.ds(me * seqs + i, 1), :])))

        def step(idx):
            outs = mixed([s + t * half for s in idx for t in range(2)], heads_m, d_m)
            upds = [mm(jnp.concatenate(outs[2 * k:2 * k + 2], axis=0), w_ro2[...], TN) for k in range(len(idx))]
            for s, upd in zip(idx, upds):
                x2 = xw[s] + upd
                for p in range(n):
                    stg_m[pl.ds(p * res * half + s, res, stride=half), :] = x2[p * SLOT:p * SLOT + res]
        grouped(half, 2, step)
        for p in range(n):
            snd_m[c, p] = stg_m[p * res * half:(p + 1) * res * half, :].reshape(res, half, LANES).astype(BF16)
        rcv_m[c, me] = snd_m[c, me]
        start(swap_copies(1, c, snd_m, rcv_m))

    loop(crops, row_attention)

    def col_attention(c):
        arrivals(1, c, lambda sender: rcv_m.at[c, sender])

        def prep(idx):
            xs = []
            for i in idx:
                x2 = jnp.concatenate([rcv_m[c, q, i].astype(F32) for q in range(n)], axis=0)
                xs.append(jnp.concatenate([x2[:, :c_m], x2[:, c_m:]], axis=0))
            for i, x in zip(idx, xs):
                xw[i, :, :c_m] = x
            project([layer_norm(x) for x in xs], wt_c, w_cq[:, c_m:2 * c_m], c_m, idx)
        grouped(res, 4, prep)

        def mask_row(i):
            return mask_t[c, pl.ds(me * SLOT + i, 1), :]

        attention(res, heads_m, d_m, hm8, None, lambda i: column((mask_row(i) - 1.0) * (MASK_SCALE * LOG2E)))

        def step(idx):
            upds = [mm(o, w_co[...], TN) for o in mixed(idx, heads_m, d_m)]
            xs = [(xw[i, :, :c_m] + upd).astype(BF16).astype(F32) for i, upd in zip(idx, upds)]
            ac = mm(wt_ac[...], jnp.concatenate([layer_norm(x) for x in xs], axis=0), NT).astype(BF16).astype(F32)
            for t, (i, x) in enumerate(zip(idx, xs)):
                x2 = jnp.concatenate([x[:n_seq // 2], x[n_seq // 2:]], axis=1)
                for q in range(n):
                    snd_b[c, q, i] = x2[q * half:(q + 1) * half].astype(BF16)
                part = ac[:, t * LANES:(t + 1) * LANES] * mask_row(i)
                abuf[c, pl.ds(pl.multiple_of(i * o_w, o_w), o_w), :] = part[:o_w].astype(BF16)
                stg_c[pl.ds(i, o_w, stride=SLOT), :] = part[o_w:]
        grouped(res, 4, step)
        ag_c[c, me] = stg_c[...].reshape(o_w, SLOT, LANES).astype(BF16)
        start(gather_copies(2, c, ag_c))
        rcv_b[c, me] = snd_b[c, me]
        start(swap_copies(3, c, snd_b, rcv_b))

    loop(crops, col_attention)

    def outer_product(c):
        gather_wait(2, c, ag_c)
        stg_b[...] = jnp.zeros(stg_b.shape, F32)
        mloc = mask_t[c, pl.ds(pl.multiple_of(me * SLOT, SLOT), SLOT), :].astype(BF16)
        norm[...] = 1.0 / (mm(mloc, mask_t[c].astype(BF16), NT) + OPM_EPS)

        def outer(fs):
            outs = []
            for k in range(0, len(fs), 2):
                rhs = jnp.concatenate([ag_c[c, p, f] for f in fs[k:k + 2] for p in range(n)], axis=0)
                outs.append(mm(abuf[c], rhs, NT))
            for k, f in enumerate(fs):
                out = outs[k // 2][:, (k % 2) * LANES:(k % 2 + 1) * LANES]
                for i in range(res):
                    obuf[i, pl.ds(pl.multiple_of(f * o_w, o_w), o_w), :] = (
                        out[i * o_w:(i + 1) * o_w] * norm[i:i + 1, :]).astype(BF16)
        grouped(o_w, 4, outer)

        def update(idx):
            rhs = [jnp.concatenate([obuf[i] for i in idx[k:k + 2]], axis=1) for k in range(0, len(idx), 2)]
            upds = [mm(w_oo_t[...], r) for r in rhs]
            for k, i in enumerate(idx):
                upd = upds[k // 2][:, (k % 2) * LANES:(k % 2 + 1) * LANES].T
                zw[c, i] = (zw[c, i].astype(F32) + upd).astype(BF16)
        grouped(res, 4, update)

        def bias_rows(idx):
            put_bias([layer_norm(zw[c, i].astype(F32)) for i in idx], 1, heads_z, idx)
        grouped(res, 4, bias_rows)
        ag_s[c, me] = stg_b[:heads_z].astype(BF16)
        start(gather_copies(4, c, ag_s))

    loop(crops, outer_product)

    stg_z[...] = jnp.zeros(stg_z.shape, F32)

    def tri_start(c):
        def prep(idx):
            project([layer_norm(zw[c, i].astype(F32)) for i in idx], wt_s, w_sq[:, c_z:2 * c_z], c_z, idx)
        grouped(res, 4, prep)
        gather_wait(4, c, ag_s)
        mcol = column(pad_bias(res_r[pl.ds(c, 1), :]))
        for h in range(heads_z):
            b = jnp.concatenate([ag_s[c, p, h].astype(F32) for p in range(n)], axis=0)
            bias[h] = b.T * LOG2E + mcol
        stg_b[...] = jnp.zeros(stg_b.shape, F32)
        attention(res, heads_z, d_z, hm4, lambda h: bias[h], lambda i: None)

        def step(idx):
            upds = [mm(o, w_so[...], TN) for o in mixed(idx, heads_z, d_z)]
            zs = [(zw[c, i].astype(F32) + upd).astype(BF16).astype(F32) for i, upd in zip(idx, upds)]
            for i, z in zip(idx, zs):
                stg_z[pl.ds(i, LANES, stride=SLOT), :] = z
            put_bias([layer_norm(z) for z in zs], 2, heads_z, idx)
        grouped(res, 4, step)
        ag_e[c, me] = stg_b[:heads_z].astype(BF16)
        start(gather_copies(5, c, ag_e))

        def pack(p):
            base = pl.multiple_of(p * SLOT * SLOT, SLOT * SLOT)
            snd_z[c, p] = stg_z[pl.ds(base, res * SLOT), :].reshape(res, SLOT, LANES).astype(BF16)
        loop(n, pack)
        rcv_z[c, me] = snd_z[c, me]
        start(swap_copies(6, c, snd_z, rcv_z))

    loop(crops, tri_start)

    def tri_end(c):
        arrivals(6, c, lambda sender: rcv_z.at[c, sender])

        def prep(idx):
            xs = [jnp.concatenate([rcv_z[c, q, j] for q in range(n)], axis=0).astype(F32) for j in idx]
            project([layer_norm(x) for x in xs], wt_e, w_eq[:, c_z:2 * c_z], c_z, idx)
        grouped(res, 4, prep)
        gather_wait(5, c, ag_e)
        mcol = column(pad_bias(res_r[pl.ds(c, 1), :]))
        for h in range(heads_z):
            b = jnp.concatenate([ag_e[c, p, h].astype(F32) for p in range(n)], axis=0)
            bias[h] = b * LOG2E + mcol
        attention(res, heads_z, d_z, hm4, lambda h: bias[h], lambda i: None)

        def step(idx):
            upds = [mm(o, w_eo[...], TN) for o in mixed(idx, heads_z, d_z)]
            for j, upd in zip(idx, upds):
                for q in range(n):
                    rcv_z[c, q, j] = (rcv_z[c, q, j].astype(F32) + upd[q * SLOT:(q + 1) * SLOT]).astype(BF16)
        grouped(res, 4, step)
        zback[c, me] = rcv_z[c, me]
        start(swap_copies(7, c, rcv_z, zback))

    loop(crops, tri_end)

    def put_m(c):
        arrivals(3, c, lambda sender: rcv_b.at[c, sender])
        stg_m[...] = rcv_b[c].astype(F32).reshape(n * res * half, LANES)

        def step(s):
            x2 = stg_m[pl.ds(s, n_res, stride=half), :]
            m_out[c, s] = x2[:, :c_m].astype(BF16)
            m_out[c, s + half] = x2[:, c_m:].astype(BF16)
        loop(half, step)

    loop(crops, put_m)

    def put_z(c):
        arrivals(7, c, lambda sender: zback.at[c, sender])

        def unpack(p):
            base = pl.multiple_of(p * SLOT * SLOT, SLOT * SLOT)
            stg_z[pl.ds(base, res * SLOT), :] = zback[c, p].astype(F32).reshape(res * SLOT, LANES)
        loop(n, unpack)

        def step(i):
            x = stg_z[pl.ds(i, LANES, stride=SLOT), :].astype(BF16)
            z_out[c, i] = mm(pad, x, TN).astype(BF16)
        loop(res, step)

    loop(crops, put_z)

    def drain(c):
        finish(gather_copies(0, c, ag_r))
        finish(swap_copies(1, c, snd_m, rcv_m))
        finish(gather_copies(2, c, ag_c))
        finish(swap_copies(3, c, snd_b, rcv_b))
        finish(gather_copies(4, c, ag_s))
        finish(gather_copies(5, c, ag_e))
        finish(swap_copies(6, c, snd_z, rcv_z))
        finish(swap_copies(7, c, rcv_z, zback))

    loop(crops, drain)


def solution(mesh):
    n = mesh.shape[GROUP_AXIS]
    rows_spec = P(PART_AXIS, GROUP_AXIS, None, None)
    in_specs = (rows_spec, rows_spec, P(PART_AXIS, None, None), P(PART_AXIS, None)) + (P(),) * N_WEIGHTS

    def local_block(m, z, msa_mask, res_mask, w_rb, w_rq, w_ro, w_cq, w_co, w_ac, w_oo, w_sb, w_sq, w_so,
                    w_eb, w_eq, w_eo):
        crops, seqs, n_res, c_m = m.shape
        res, c_z = z.shape[1], z.shape[3]
        heads_m, heads_z = w_rq.shape[2], w_sq.shape[2]
        o_w = w_ac.shape[2]
        half = seqs // 2
        assert n * SLOT == LANES and res <= SLOT and n * seqs == LANES and 2 * c_m == LANES and c_z == LANES
        flat = lambda w: w.reshape(w.shape[0], -1)
        tall = lambda w: w.reshape(-1, w.shape[-1])
        args = (m, z, msa_mask, res_mask, w_rb, flat(w_rq), tall(w_ro), flat(w_cq), tall(w_co), flat(w_ac), tall(w_oo),
                w_sb, flat(w_sq), tall(w_so), w_eb, flat(w_eq), tall(w_eo))
        vm = pltpu.VMEM
        slots = max(seqs, res)
        scratch = [
            vm((crops, n, heads_m, SLOT, LANES), BF16),
            vm((crops, n, o_w, SLOT, LANES), BF16),
            vm((crops, n, heads_z, SLOT, LANES), BF16),
            vm((crops, n, heads_z, SLOT, LANES), BF16),
            vm((crops, n, res, half, LANES), BF16),
            vm((crops, n, res, half, LANES), BF16),
            vm((crops, n, res, half, LANES), BF16),
            vm((crops, n, res, half, LANES), BF16),
            vm((crops, n, res, SLOT, LANES), BF16),
            vm((crops, n, res, SLOT, LANES), BF16),
            vm((crops, n, res, SLOT, LANES), BF16),
            vm((crops, res, LANES, LANES), BF16),
            vm((slots, LANES, LANES), F32),
            vm((slots, LANES, LANES), BF16),
            vm((slots, LANES, LANES), BF16),
            vm((slots, LANES, LANES), BF16),
            vm((slots, LANES, LANES), F32),
            vm((heads_m, LANES, LANES), F32),
            vm((res, o_w * o_w, LANES), BF16),
            vm((n * res * half, LANES), F32),
            vm((o_w * SLOT, LANES), F32),
            vm((heads_m, SLOT, LANES), F32),
            vm((LANES * SLOT, LANES), F32),
            vm((crops, res * o_w, LANES), BF16),
            vm((crops, LANES, LANES), F32),
            vm((crops, n * seqs, LANES), F32),
            vm((crops, LANES), F32),
            vm((slots, heads_m // 2, LANES, 2 * LANES), F32),
            vm((slots, heads_m // 2, LANES, 2 * LANES), BF16),
            vm((slots, heads_m, LANES), F32),
            vm((SLOT, LANES), F32),
            vm((heads_m, c_m, LANES), BF16),
            vm((heads_z, c_z, LANES), BF16),
            vm((4 * c_m, c_m), BF16),
            vm((4 * c_m, c_m), BF16),
            vm((4 * c_z, c_z), BF16),
            vm((4 * c_z, c_z), BF16),
            vm((2 * o_w, c_m), BF16),
            vm((LANES, o_w * o_w), BF16),
            vm((LANES, LANES), BF16),
            vm((3, SLOT, LANES), BF16),
            pltpu.SemaphoreType.DMA((8, crops, n)),
            pltpu.SemaphoreType.DMA((8, crops, n)),
        ]
        cfg = dict(n=n, heads_m=heads_m, heads_z=heads_z, k_logits=2, k_softmax=1)
        spec = pl.BlockSpec(memory_space=pltpu.VMEM)
        return pl.pallas_call(
            functools.partial(body, cfg),
            out_shape=(jax.ShapeDtypeStruct(m.shape, BF16), jax.ShapeDtypeStruct(z.shape, BF16)),
            in_specs=[spec] * len(args),
            out_specs=(spec, spec),
            scratch_shapes=scratch,
            compiler_params=pltpu.CompilerParams(collective_id=0, has_side_effects=True,
                                                 vmem_limit_bytes=60 * 1024 * 1024),
        )(*args)

    return jax.shard_map(local_block, mesh=mesh, in_specs=in_specs, out_specs=(rows_spec, rows_spec),
                         check_vma=False)
```

```python
import functools
import math

import jax
import jax.numpy as jnp
from jax import lax
from jax.experimental import pallas as pl
from jax.experimental.pallas import tpu as pltpu
from jax.sharding import PartitionSpec as P

MASK_SCALE = 10000.0
LN_EPS = 1e-5
OPM_EPS = 1e-3
N_WEIGHTS = 13
PART_AXIS = 'data'
GROUP_AXIS = 'dap'
LOG2E = math.log2(math.e)
PAD_BIAS = -1e30
LANES = 128
SLOT = 16
F32 = jnp.float32
BF16 = jnp.bfloat16
NN = (((1,), (0,)), ((), ()))
NT = (((1,), (1,)), ((), ()))
TN = (((0,), (0,)), ((), ()))


def mm(lhs, rhs, dims=NN):
    return lax.dot_general(lhs, rhs, dims, preferred_element_type=F32)


def layer_norm(x_float):
    mean_val = jnp.mean(x_float, axis=-1, keepdims=True)
    centred = x_float - mean_val
    var_val = jnp.mean(centred * centred, axis=-1, keepdims=True)
    return (centred * lax.rsqrt(var_val + LN_EPS)).astype(BF16)


def layer_norm_t(x_float):
    mean_val = jnp.mean(x_float, axis=0, keepdims=True)
    centred = x_float - mean_val
    var_val = jnp.mean(centred * centred, axis=0, keepdims=True)
    return (centred * lax.rsqrt(var_val + LN_EPS)).astype(BF16)


def iota(shape, axis):
    return lax.broadcasted_iota(jnp.int32, shape, axis)


def body(cfg, *refs):
    n = cfg['n']
    (m_in, z_in, mask_in, res_in, w_rb, wt_r, w_ro, wt_c, w_co, w_ac, w_oo,
     w_sb, wt_s, w_so, w_eb, wt_e, w_eo, m_out, z_out,
     ag_r, ag_c, ag_s, ag_e, snd_m, rcv_m, snd_b, rcv_b, snd_z, rcv_z, zback,
     zw, xw, kbuf, qbuf, vbuf, gbuf, bias, obuf, stg_m, stg_c, stg_b, stg_z, abuf,
     mask_t, mask_r, res_r, raw, prob, inv, norm, hm8, hm4, wt_ro, wt_co, w_oo_t, wt_b, pad_t,
     send_sem, recv_sem) = refs
    crops, seqs, c_m, n_res = m_in.shape
    res = z_in.shape[1]
    c_z = z_in.shape[3]
    half = seqs // 2
    heads_m, heads_z = cfg['heads_m'], cfg['heads_z']
    d_m, d_z = c_m // heads_m, c_z // heads_z
    n_seq = n * seqs
    slots, pieces = cfg['slots'], cfg['pieces']
    me = lax.axis_index(GROUP_AXIS)

    barrier = pltpu.get_barrier_semaphore()
    for r in range(1, n):
        pl.semaphore_signal(barrier, inc=1, device_id={GROUP_AXIS: lax.rem(me + r, n)},
                            device_id_type=pl.DeviceIdType.MESH)
    pl.semaphore_wait(barrier, n - 1)

    def copies(exch, c, src_of, dst):
        out = []
        for r in range(1, n):
            peer = lax.rem(me + r, n)
            out.append(pltpu.make_async_remote_copy(
                src_ref=src_of(peer), dst_ref=dst, send_sem=send_sem.at[exch, c, r], recv_sem=recv_sem.at[exch, c, r],
                device_id={GROUP_AXIS: peer}, device_id_type=pl.DeviceIdType.MESH))
        return out

    def arrivals(exch, c, slot_of):
        for r in range(1, n):
            sender = lax.rem(me + n - r, n)
            ref = slot_of(sender)
            pltpu.make_async_remote_copy(
                src_ref=ref, dst_ref=ref, send_sem=send_sem.at[exch, c, r], recv_sem=recv_sem.at[exch, c, r],
                device_id={GROUP_AXIS: sender}, device_id_type=pl.DeviceIdType.MESH).wait_recv()

    def gather_copies(exch, c, buf):
        return copies(exch, c, lambda peer: buf.at[c, me], buf.at[c, me])

    def gather_wait(exch, c, buf):
        arrivals(exch, c, lambda sender: buf.at[c, sender])

    def swap_copies(exch, c, snd, rcv):
        return copies(exch, c, lambda peer: snd.at[c, peer], rcv.at[c, me])

    chips, core, chip = n // 2, lax.rem(me, 2), me // 2
    ahead = 1 - 2 * core

    def device(offset, other=False):
        return lax.rem(chip + offset + chips, chips) * 2 + ((1 - core) if other else core)

    def block_copy(c, block, peer, slot):
        return pltpu.make_async_remote_copy(
            src_ref=ag_c.at[c, block], dst_ref=ag_c.at[c, block], send_sem=send_sem.at[2, c, slot],
            recv_sem=recv_sem.at[2, c, block], device_id={GROUP_AXIS: peer}, device_id_type=pl.DeviceIdType.MESH)

    def block_wait(c, block):
        block_copy(c, block, block, 0).wait_recv()

    def relay_own(c):
        for slot, peer in enumerate((device(1), device(-1), device(0, True))):
            block_copy(c, me, peer, slot).start()

    def relay_near(c):
        block_wait(c, device(-1))
        block_wait(c, device(1))
        block_copy(c, device(-ahead), device(ahead), 3).start()
        block_copy(c, device(-1), device(0, True), 4).start()
        block_copy(c, device(1), device(0, True), 5).start()

    def relay_far(c):
        block_wait(c, device(2))
        block_copy(c, device(2), device(0, True), 6).start()

    def relay_done(c):
        for offset in range(chips):
            block_wait(c, device(offset, True))

    def start(descs):
        for d in descs:
            d.start()

    def finish(descs):
        for d in descs:
            d.wait_send()

    def loop(count, fn):
        def step(i, carry):
            fn(i)
            return carry
        lax.fori_loop(0, count, step, 0)

    def pad_matrix():
        row, col = iota((LANES, n_res), 0), iota((LANES, n_res), 1)
        hit = (col == (row // SLOT) * res + row % SLOT) & (row % SLOT < res)
        return jnp.where(hit, 1.0, 0.0).astype(BF16)

    def head_rows(heads, width, ref):
        for h in range(heads):
            row = iota((heads * width, LANES), 0)
            ref[h] = jnp.where((row >= h * width) & (row < (h + 1) * width), 1.0, 0.0).astype(BF16)

    pad = pad_matrix()
    pad_t[...] = pad.astype(F32).T.astype(BF16)
    head_rows(heads_m, d_m, hm8)
    head_rows(heads_z, d_z, hm4)
    row, col = iota((LANES, LANES), 0), iota((LANES, LANES), 1)
    seq_of = ((col % (n_seq // 2)) // half) * seqs + (col // (n_seq // 2)) * half + col % half
    seq_perm = jnp.where(row == seq_of, 1.0, 0.0).astype(BF16)
    for c in range(crops):
        mask_pad = mm(pad, mask_in[c].astype(F32).astype(BF16))
        mask_t[c] = mm(mask_pad.astype(BF16), seq_perm)
        mask_r[c] = mask_pad.T
    res_r[...] = mm(res_in[...].astype(F32).astype(BF16), pad, NT)
    for k, w in enumerate((w_rb, w_sb, w_eb)):
        wt_b[k] = jnp.zeros(wt_b.shape[1:], BF16)
        wt_b[k, :w.shape[0], :] = w[...]
    wt_ro[...] = w_ro[...].astype(F32).T.astype(BF16)
    wt_co[...] = w_co[...].astype(F32).T.astype(BF16)
    o_w = w_ac.shape[0] // 2
    stg_z[:o_w * o_w, :] = w_oo[...].astype(F32)
    for k in range(0, o_w, LANES // o_w):
        rows = [stg_z[pl.ds(f, o_w, stride=o_w), :] for f in range(k, k + LANES // o_w)]
        w_oo_t[:, k * o_w:k * o_w + LANES] = jnp.concatenate(rows, axis=0).T.astype(BF16)

    stg_b[...] = jnp.zeros(stg_b.shape, F32)
    stg_c[...] = jnp.zeros(stg_c.shape, F32)

    def grouped(count, size, fn):
        while count % size:
            size -= 1

        def step(b, carry):
            fn([b * size + t for t in range(size)])
            return carry
        lax.fori_loop(0, count // size, step, 0)

    def put_bias(y, k, heads, rows):
        b = mm(wt_b[k], y, NT)
        for t, i in enumerate(rows):
            for h in range(heads):
                stg_b[h, pl.ds(i, 1), :] = b[h:h + 1, t * LANES:(t + 1) * LANES]

    def keep(p, width, slots):
        for t, slot in enumerate(slots):
            part = slice(t * LANES, (t + 1) * LANES)
            qbuf[slot, :width] = p[:width, part].astype(BF16)
            kbuf[slot, :, :width] = p[width:2 * width, part].T.astype(BF16)
            vbuf[slot, :width] = p[2 * width:3 * width, part].astype(BF16)
            gbuf[slot, :width] = jax.nn.sigmoid(p[3 * width:, part])

    def column(rowvec):
        return jnp.broadcast_to(rowvec, (LANES, LANES)).T

    def pad_bias(rowvec):
        lane = iota((1, LANES), 1)
        return jnp.where(lane % SLOT < res, (rowvec - 1.0) * (MASK_SCALE * LOG2E), PAD_BIAS)

    def logits(idx, base, heads, width, head_mask):
        c = heads * width
        for i in idx:
            q_t, keys = qbuf[base + i, :c], kbuf[base + i, :, :c]
            for pair in range(heads // 2):
                rhs = jnp.concatenate([q_t * head_mask[2 * pair], q_t * head_mask[2 * pair + 1]], axis=1)
                raw[i, pair] = mm(keys, rhs)

    def softmax(idx, heads, width, bias_of, mask_of):
        scale2 = LOG2E * width ** -0.5
        for i in idx:
            mcol = mask_of(i)
            for h in range(heads):
                part = slice((h % 2) * LANES, (h % 2 + 1) * LANES)
                x = raw[i, h // 2, :, part] * scale2
                if bias_of is not None:
                    x = x + bias_of(h)
                if mcol is not None:
                    x = x + mcol
                e = jnp.exp2(x - jnp.max(x, axis=0, keepdims=True))
                inv[i, h:h + 1, :] = 1.0 / jnp.sum(e, axis=0, keepdims=True)
                prob[i, h // 2, :, part] = e.astype(BF16)

    def mixed(idx, base, heads, width):
        c = heads * width
        raws = [[mm(vbuf[base + i, 2 * p * width:2 * (p + 1) * width], prob[i, p]) for p in range(heads // 2)]
                for i in idx]
        outs = []
        for i, r in zip(idx, raws):
            parts = []
            for p in range(heads // 2):
                parts.append(r[p][:width, :LANES] * inv[i, 2 * p:2 * p + 1, :])
                parts.append(r[p][width:, LANES:] * inv[i, 2 * p + 1:2 * p + 2, :])
            outs.append((jnp.concatenate(parts, axis=0) * gbuf[base + i, :c]).astype(BF16))
        return outs

    def row_bias(c):
        def step(idx):
            zs = [mm(pad, z_in[c, i]) for i in idx]
            for i, z in zip(idx, zs):
                zw[c, i] = z.astype(BF16)
            put_bias(jnp.concatenate([layer_norm(z) for z in zs], axis=0), 0, heads_m, idx)
        grouped(res, 6, step)
        ag_r[c, me] = stg_b[...].astype(BF16)
        start(gather_copies(0, c, ag_r))

    loop(crops, row_bias)

    def row_prep(c):
        def prep(idx):
            x = mm(jnp.concatenate([m_in[c, s] for s in idx], axis=0), pad_t[...])
            xs = [x[t * c_m:(t + 1) * c_m] for t in range(len(idx))]
            for s, x_t in zip(idx, xs):
                xw[c * slots + s] = x_t
            keep(mm(wt_r[...], jnp.concatenate([layer_norm_t(x_t) for x_t in xs], axis=1)), c_m,
                 [c * slots + s for s in idx])
        grouped(seqs, 4, prep)

    loop(crops, row_prep)

    def row_attention(c):
        base = c * slots
        grouped(seqs, 4, lambda idx: logits(idx, base, heads_m, d_m, hm8))
        gather_wait(0, c, ag_r)
        for h in range(heads_m):
            b = jnp.concatenate([ag_r[c, p, h].astype(F32) for p in range(n)], axis=0)
            bias[h] = b.T * LOG2E
        grouped(seqs, 1, lambda idx: softmax(
            idx, heads_m, d_m, lambda h: bias[h],
            lambda i: column(pad_bias(mask_r[c, pl.ds(me * seqs + i, 1), :]))))

        def step(idx):
            both = [s + t * half for s in idx for t in range(2)]
            upd = mm(wt_ro[...], jnp.concatenate(mixed(both, base, heads_m, d_m), axis=1))
            new = [xw[base + s] + upd[:, t * LANES:(t + 1) * LANES] for t, s in enumerate(both)]
            for k, s in enumerate(idx):
                x2 = jnp.concatenate(new[2 * k:2 * k + 2], axis=0).T
                for p in range(n):
                    stg_m[pl.ds(p * res * half + s, res, stride=half), :] = x2[p * SLOT:p * SLOT + res]
        grouped(half, 2, step)
        for p in range(n):
            snd_m[c, p] = stg_m[p * res * half:(p + 1) * res * half, :].reshape(res, half, LANES).astype(BF16)
        rcv_m[c, me] = snd_m[c, me]
        start(swap_copies(1, c, snd_m, rcv_m))

    loop(crops, row_attention)

    def col_attention(c):
        base = c * slots
        arrivals(1, c, lambda sender: rcv_m.at[c, sender])
        hs = n_seq // 2

        def prep(idx):
            ys = []
            for k in range(0, len(idx), 2):
                x2 = jnp.concatenate([rcv_m[c, q, i].astype(F32) for i in idx[k:k + 2] for q in range(n)], axis=0).T
                for t, i in enumerate(idx[k:k + 2]):
                    x = jnp.concatenate([x2[:c_m, t * hs:(t + 1) * hs], x2[c_m:, t * hs:(t + 1) * hs]], axis=1)
                    xw[base + i] = x
                    ys.append(layer_norm_t(x))
            keep(mm(wt_c[...], jnp.concatenate(ys, axis=1)), c_m, [base + i for i in idx])
        grouped(res, 4, prep)

        def mask_row(i):
            return mask_t[c, pl.ds(me * SLOT + i, 1), :]

        grouped(res, 4, lambda idx: logits(idx, base, heads_m, d_m, hm8))

        @pl.when(c == 1)
        def _():
            relay_near(0)

        grouped(res, 1, lambda idx: softmax(
            idx, heads_m, d_m, None, lambda i: column((mask_row(i) - 1.0) * (MASK_SCALE * LOG2E))))

        @pl.when(c == 1)
        def _():
            relay_far(0)

        def step(idx):
            upd = mm(wt_co[...], jnp.concatenate(mixed(idx, base, heads_m, d_m), axis=1))
            xs = [(xw[base + i] + upd[:, t * LANES:(t + 1) * LANES]).astype(BF16).astype(F32)
                  for t, i in enumerate(idx)]
            ac = mm(w_ac[...], jnp.concatenate([layer_norm_t(x) for x in xs], axis=1)).astype(BF16).astype(F32)
            for k in range(0, len(idx), 2):
                two = jnp.concatenate([
                    jnp.concatenate([x[:, :hs] for x in xs[k:k + 2]], axis=1),
                    jnp.concatenate([x[:, hs:] for x in xs[k:k + 2]], axis=1)], axis=0).T
                for t, i in enumerate(idx[k:k + 2]):
                    for q in range(n):
                        snd_b[c, q, i] = two[t * hs + q * half:t * hs + (q + 1) * half].astype(BF16)
            for t, i in enumerate(idx):
                part = ac[:, t * LANES:(t + 1) * LANES] * mask_row(i)
                abuf[c, pl.ds(pl.multiple_of(i * o_w, o_w), o_w), :] = part[:o_w].astype(BF16)
                stg_c[pl.ds(i, o_w, stride=SLOT), :] = part[o_w:]
        grouped(res, 4, step)
        ag_c[c, me] = stg_c[...].reshape(o_w, SLOT, LANES).astype(BF16)
        relay_own(c)
        rcv_b[c, me] = snd_b[c, me]
        start(swap_copies(3, c, snd_b, rcv_b))

    loop(crops, col_attention)

    def outer_product(c):
        base = c * slots
        relay_done(c)
        stg_b[...] = jnp.zeros(stg_b.shape, F32)
        mloc = mask_t[c, pl.ds(pl.multiple_of(me * SLOT, SLOT), SLOT), :].astype(BF16)
        norm[...] = 1.0 / (mm(mloc, mask_t[c].astype(BF16), NT) + OPM_EPS)

        def outer(fs):
            outs = []
            for k in range(0, len(fs), 2):
                rhs = jnp.concatenate([ag_c[c, p, f] for f in fs[k:k + 2] for p in range(n)], axis=0)
                outs.append(mm(abuf[c], rhs, NT))
            for k, f in enumerate(fs):
                out = outs[k // 2][:, (k % 2) * LANES:(k % 2 + 1) * LANES]
                for i in range(res):
                    obuf[i, pl.ds(pl.multiple_of(f * o_w, o_w), o_w), :] = (
                        out[i * o_w:(i + 1) * o_w] * norm[i:i + 1, :]).astype(BF16)
        grouped(o_w, 4, outer)

        @pl.when(c == 0)
        def _():
            relay_near(1)

        def update(idx):
            rhs = [jnp.concatenate([obuf[i] for i in idx[k:k + 2]], axis=1) for k in range(0, len(idx), 2)]
            upds = [mm(w_oo_t[...], r) for r in rhs]
            for k, i in enumerate(idx):
                upd = upds[k // 2][:, (k % 2) * LANES:(k % 2 + 1) * LANES].T
                zw[c, i] = (zw[c, i].astype(F32) + upd).astype(BF16)
        grouped(res, 4, update)

        @pl.when(c == 0)
        def _():
            relay_far(1)

        def prep(idx):
            y = jnp.concatenate([layer_norm(zw[c, i].astype(F32)) for i in idx], axis=0)
            put_bias(y, 1, heads_z, idx)
            keep(mm(wt_s[...], y, NT), c_z, [base + i for i in idx])
        grouped(res, 4, prep)
        ag_s[c, me] = stg_b[:heads_z].astype(BF16)
        start(gather_copies(4, c, ag_s))

    loop(crops, outer_product)

    stg_z[...] = jnp.zeros(stg_z.shape, F32)

    def tri_start(c):
        base = c * slots
        grouped(res, 4, lambda idx: logits(idx, base, heads_z, d_z, hm4))
        gather_wait(4, c, ag_s)
        mcol = column(pad_bias(res_r[pl.ds(c, 1), :]))
        for h in range(heads_z):
            b = jnp.concatenate([ag_s[c, p, h].astype(F32) for p in range(n)], axis=0)
            bias[h] = b.T * LOG2E + mcol
        stg_b[...] = jnp.zeros(stg_b.shape, F32)
        grouped(res, 2, lambda idx: softmax(idx, heads_z, d_z, lambda h: bias[h], lambda i: None))

        def step(idx):
            upds = [mm(o, w_so[...], TN) for o in mixed(idx, base, heads_z, d_z)]
            zs = [(zw[c, i].astype(F32) + upd).astype(BF16).astype(F32) for i, upd in zip(idx, upds)]
            for i, z in zip(idx, zs):
                stg_z[pl.ds(i, LANES, stride=SLOT), :] = z
            put_bias(jnp.concatenate([layer_norm(z) for z in zs], axis=0), 2, heads_z, idx)
        grouped(res, 4, step)
        ag_e[c, me] = stg_b[:heads_z].astype(BF16)
        start(gather_copies(5, c, ag_e))

        def pack(p):
            rows = stg_z[pl.ds(pl.multiple_of(p * SLOT * SLOT, SLOT * SLOT), res * SLOT), :]
            snd_z[c, p] = rows.reshape(res, SLOT, LANES).astype(BF16)
        loop(n, pack)
        rcv_z[c, me] = snd_z[c, me]
        start(swap_copies(6, c, snd_z, rcv_z))

    loop(crops, tri_start)

    part_rows = res // pieces

    def piece_copies(c, g):
        window = pl.ds(g * part_rows, part_rows)
        return copies(7 + g, c, lambda peer: rcv_z.at[c, peer, window], zback.at[c, me, window])

    def tri_end(c):
        base = c * slots
        arrivals(6, c, lambda sender: rcv_z.at[c, sender])

        def prep(idx):
            ys = [layer_norm(jnp.concatenate([rcv_z[c, q, j].astype(F32) for q in range(n)], axis=0)) for j in idx]
            keep(mm(wt_e[...], jnp.concatenate(ys, axis=0), NT), c_z, [base + j for j in idx])
        grouped(res, 4, prep)
        gather_wait(5, c, ag_e)
        mcol = column(pad_bias(res_r[pl.ds(c, 1), :]))
        for h in range(heads_z):
            b = jnp.concatenate([ag_e[c, p, h].astype(F32) for p in range(n)], axis=0)
            bias[h] = b * LOG2E + mcol

        def step(g):
            idx = [g * part_rows + t for t in range(part_rows)]
            logits(idx, base, heads_z, d_z, hm4)
            softmax(idx, heads_z, d_z, lambda h: bias[h], lambda i: None)
            upds = [mm(o, w_eo[...], TN) for o in mixed(idx, base, heads_z, d_z)]
            for j, upd in zip(idx, upds):
                for q in range(n):
                    rcv_z[c, q, j] = (rcv_z[c, q, j].astype(F32) + upd[q * SLOT:(q + 1) * SLOT]).astype(BF16)
            start(piece_copies(c, g))
        loop(pieces, step)
        zback[c, me] = rcv_z[c, me]

    loop(crops, tri_end)

    def put_m(c):
        arrivals(3, c, lambda sender: rcv_b.at[c, sender])
        stg_m[...] = rcv_b[c].astype(F32).reshape(n * res * half, LANES)

        def step(idx):
            for s in idx:
                x2 = stg_m[pl.ds(s, n_res, stride=half), :].T
                m_out[c, s] = x2[:c_m].astype(BF16)
                m_out[c, s + half] = x2[c_m:].astype(BF16)
        grouped(half, 4, step)

    loop(crops, put_m)

    def put_z(c):
        for g in range(pieces):
            window = pl.ds(g * part_rows, part_rows)
            arrivals(7 + g, c, lambda sender: zback.at[c, sender, window])

        def unpack(p):
            base = pl.multiple_of(p * SLOT * SLOT, SLOT * SLOT)
            stg_z[pl.ds(base, res * SLOT), :] = zback[c, p].astype(F32).reshape(res * SLOT, LANES)
        loop(n, unpack)

        def step(idx):
            xs = [stg_z[pl.ds(i, LANES, stride=SLOT), :].astype(BF16) for i in idx]
            for k in range(0, len(idx), 2):
                out = mm(pad_t[...], jnp.concatenate(xs[k:k + 2], axis=1))
                for t, i in enumerate(idx[k:k + 2]):
                    z_out[c, i] = out[:, t * LANES:(t + 1) * LANES].astype(BF16)
        grouped(res, 6, step)

    loop(crops, put_z)

    def drain(c):
        finish(gather_copies(0, c, ag_r))
        finish(swap_copies(1, c, snd_m, rcv_m))
        for slot in range(n - 1):
            block_copy(c, me, device(1), slot).wait_send()
        finish(swap_copies(3, c, snd_b, rcv_b))
        finish(gather_copies(4, c, ag_s))
        finish(gather_copies(5, c, ag_e))
        finish(swap_copies(6, c, snd_z, rcv_z))
        for g in range(pieces):
            finish(piece_copies(c, g))

    loop(crops, drain)


def solution(mesh):
    n = mesh.shape[GROUP_AXIS]
    rows_spec = P(PART_AXIS, GROUP_AXIS, None, None)
    in_specs = (rows_spec, rows_spec, P(PART_AXIS, None, None), P(PART_AXIS, None)) + (P(),) * N_WEIGHTS

    def local_block(m, z, msa_mask, res_mask, w_rb, w_rq, w_ro, w_cq, w_co, w_ac, w_oo, w_sb, w_sq, w_so,
                    w_eb, w_eq, w_eo):
        crops, seqs, n_res, c_m = m.shape
        res, c_z = z.shape[1], z.shape[3]
        heads_m, heads_z = w_rq.shape[2], w_sq.shape[2]
        o_w = w_ac.shape[2]
        half = seqs // 2
        assert n == 8 and crops == 2 and res % 3 == 0 and n * SLOT == LANES and res <= SLOT and n * seqs == LANES and 2 * c_m == LANES and c_z == LANES
        flat = lambda w: jnp.moveaxis(w, 0, -1).reshape(-1, w.shape[0])
        tall = lambda w: w.reshape(-1, w.shape[-1])
        args = (m.swapaxes(2, 3), z, msa_mask.swapaxes(1, 2), res_mask, w_rb.T, flat(w_rq), tall(w_ro), flat(w_cq),
                tall(w_co), flat(w_ac), tall(w_oo), w_sb.T, flat(w_sq), tall(w_so), w_eb.T, flat(w_eq), tall(w_eo))
        vm = pltpu.VMEM
        slots = max(seqs, res)
        scratch = [
            vm((crops, n, heads_m, SLOT, LANES), BF16),
            vm((crops, n, o_w, SLOT, LANES), BF16),
            vm((crops, n, heads_z, SLOT, LANES), BF16),
            vm((crops, n, heads_z, SLOT, LANES), BF16),
            vm((crops, n, res, half, LANES), BF16),
            vm((crops, n, res, half, LANES), BF16),
            vm((crops, n, res, half, LANES), BF16),
            vm((crops, n, res, half, LANES), BF16),
            vm((crops, n, res, SLOT, LANES), BF16),
            vm((crops, n, res, SLOT, LANES), BF16),
            vm((crops, n, res, SLOT, LANES), BF16),
            vm((crops, res, LANES, LANES), BF16),
            vm((crops * slots, c_m, LANES), F32),
            vm((crops * slots, LANES, LANES), BF16),
            vm((crops * slots, LANES, LANES), BF16),
            vm((crops * slots, LANES, LANES), BF16),
            vm((crops * slots, LANES, LANES), F32),
            vm((heads_m, LANES, LANES), F32),
            vm((res, o_w * o_w, LANES), BF16),
            vm((n * res * half, LANES), F32),
            vm((o_w * SLOT, LANES), F32),
            vm((heads_m, SLOT, LANES), F32),
            vm((LANES * SLOT, LANES), F32),
            vm((crops, res * o_w, LANES), BF16),
            vm((crops, LANES, LANES), F32),
            vm((crops, n * seqs, LANES), F32),
            vm((crops, LANES), F32),
            vm((slots, heads_m // 2, LANES, 2 * LANES), F32),
            vm((slots, heads_m // 2, LANES, 2 * LANES), BF16),
            vm((slots, heads_m, LANES), F32),
            vm((SLOT, LANES), F32),
            vm((heads_m, c_m, LANES), BF16),
            vm((heads_z, c_z, LANES), BF16),
            vm((c_m, c_m), BF16),
            vm((c_m, c_m), BF16),
            vm((LANES, o_w * o_w), BF16),
            vm((3, SLOT, LANES), BF16),
            vm((n_res, LANES), BF16),
            pltpu.SemaphoreType.DMA((12, crops, n)),
            pltpu.SemaphoreType.DMA((12, crops, n)),
        ]
        cfg = dict(n=n, heads_m=heads_m, heads_z=heads_z, slots=slots, pieces=3)
        spec = pl.BlockSpec(memory_space=pltpu.VMEM)
        m_new, z_new = pl.pallas_call(
            functools.partial(body, cfg),
            out_shape=(jax.ShapeDtypeStruct((crops, seqs, c_m, n_res), BF16), jax.ShapeDtypeStruct(z.shape, BF16)),
            in_specs=[spec] * len(args),
            out_specs=(spec, spec),
            scratch_shapes=scratch,
            compiler_params=pltpu.CompilerParams(collective_id=0, has_side_effects=True,
                                                 vmem_limit_bytes=60 * 1024 * 1024),
        )(*args)
        return m_new.swapaxes(2, 3), z_new

    return jax.shard_map(local_block, mesh=mesh, in_specs=in_specs, out_specs=(rows_spec, rows_spec),
                         check_vma=False)
```

```python
import functools
import math

import jax
import jax.numpy as jnp
import numpy as np
from jax import lax
from jax.experimental import pallas as pl
from jax.experimental.pallas import tpu as pltpu
from jax.sharding import PartitionSpec as P

MASK_SCALE = 10000.0
LN_EPS = 1e-5
OPM_EPS = 1e-3
N_WEIGHTS = 13
PART_AXIS = 'data'
GROUP_AXIS = 'dap'
LOG2E = math.log2(math.e)
AUG = 16
LANES = 128
SLOT = 16
F32 = jnp.float32
BF16 = jnp.bfloat16
NN = (((1,), (0,)), ((), ()))
NT = (((1,), (1,)), ((), ()))
TN = (((0,), (0,)), ((), ()))


def mm(lhs, rhs, dims=NN):
    return lax.dot_general(lhs, rhs, dims, preferred_element_type=F32)


def layer_norm(x_float):
    mean_val = jnp.mean(x_float, axis=-1, keepdims=True)
    centred = x_float - mean_val
    var_val = jnp.mean(centred * centred, axis=-1, keepdims=True)
    return (centred * lax.rsqrt(var_val + LN_EPS)).astype(BF16)


def layer_norm_t(x_float):
    mean_val = jnp.mean(x_float, axis=0, keepdims=True)
    centred = x_float - mean_val
    var_val = jnp.mean(centred * centred, axis=0, keepdims=True)
    return (centred * lax.rsqrt(var_val + LN_EPS)).astype(BF16)


def iota(shape, axis):
    return lax.broadcasted_iota(jnp.int32, shape, axis)


def body(cfg, *refs):
    pl.run_scoped(functools.partial(scoped_body, cfg, refs), *cfg['local'])


def scoped_body(cfg, refs, *local):
    n = cfg['n']
    (m_in, z_in, mask_in, res_in, w_rb, wt_r, w_ro, wt_c, w_co, w_ac, w_oo,
     w_sb, wt_s, w_so, w_eb, wt_e, w_eo, m_out, z_out,
     ag_r, ag_c, ag_s, ag_e, snd_m, rcv_m, snd_b, rcv_b, snd_z, rcv_z, snd_y, zback, send_sem, recv_sem) = refs
    (zw, xw, kbuf, qbuf, vbuf, gbuf, bias, obuf, stg_m, stg_c, stg_b, stg_z, abuf,
     mask_t, mask_r, res_r, raw, prob, inv, norm, hm8, hm4, wt_ro, wt_co, w_oo_t, wt_b, aug, one_rows, xs) = local
    crops, seqs, c_m, n_res = m_in.shape
    res = z_in.shape[1]
    c_z = z_in.shape[3]
    half = seqs // 2
    heads_m, heads_z = cfg['heads_m'], cfg['heads_z']
    d_m, d_z = c_m // heads_m, c_z // heads_z
    n_seq = n * seqs
    slots, pieces = cfg['slots'], cfg['pieces']
    me = lax.axis_index(GROUP_AXIS)

    barrier = pltpu.get_barrier_semaphore()
    for r in range(1, n):
        pl.semaphore_signal(barrier, inc=1, device_id={GROUP_AXIS: lax.rem(me + r, n)},
                            device_id_type=pl.DeviceIdType.MESH)
    pl.semaphore_wait(barrier, n - 1)

    def copies(exch, c, src_of, dst):
        out = []
        for r in range(1, n):
            peer = lax.rem(me + r, n)
            out.append(pltpu.make_async_remote_copy(
                src_ref=src_of(peer), dst_ref=dst, send_sem=send_sem.at[exch, c, r], recv_sem=recv_sem.at[exch, c, r],
                device_id={GROUP_AXIS: peer}, device_id_type=pl.DeviceIdType.MESH))
        return out

    def arrivals(exch, c, slot_of):
        for r in range(1, n):
            sender = lax.rem(me + n - r, n)
            ref = slot_of(sender)
            pltpu.make_async_remote_copy(
                src_ref=ref, dst_ref=ref, send_sem=send_sem.at[exch, c, r], recv_sem=recv_sem.at[exch, c, r],
                device_id={GROUP_AXIS: sender}, device_id_type=pl.DeviceIdType.MESH).wait_recv()

    def gather_copies(exch, c, buf):
        return copies(exch, c, lambda peer: buf.at[c, me], buf.at[c, me])

    def gather_wait(exch, c, buf):
        arrivals(exch, c, lambda sender: buf.at[c, sender])

    def swap_copies(exch, c, snd, rcv):
        return copies(exch, c, lambda peer: snd.at[c, peer], rcv.at[c, me])

    chips, core, chip = n // 2, lax.rem(me, 2), me // 2
    ahead = 1 - 2 * core

    def device(offset, other=False):
        return lax.rem(chip + offset + chips, chips) * 2 + ((1 - core) if other else core)

    def block_copy(c, block, peer, slot):
        return pltpu.make_async_remote_copy(
            src_ref=ag_c.at[c, block], dst_ref=ag_c.at[c, block], send_sem=send_sem.at[2, c, slot],
            recv_sem=recv_sem.at[2, c, block], device_id={GROUP_AXIS: peer}, device_id_type=pl.DeviceIdType.MESH)

    def block_wait(c, block):
        block_copy(c, block, block, 0).wait_recv()

    def relay_own(c):
        for slot, peer in enumerate((device(1), device(-1), device(0, True))):
            block_copy(c, me, peer, slot).start()

    def relay_near(c):
        block_wait(c, device(-1))
        block_wait(c, device(1))
        block_copy(c, device(-ahead), device(ahead), 3).start()
        block_copy(c, device(-1), device(0, True), 4).start()
        block_copy(c, device(1), device(0, True), 5).start()

    def relay_far(c):
        block_wait(c, device(2))
        block_copy(c, device(2), device(0, True), 6).start()

    def relay_done(c):
        for offset in range(chips):
            block_wait(c, device(offset, True))

    def start(descs):
        for d in descs:
            d.start()

    def finish(descs):
        for d in descs:
            d.wait_send()

    def loop(count, fn):
        def step(i, carry):
            fn(i)
            return carry
        lax.fori_loop(0, count, step, 0)

    def pad_matrix():
        row, col = iota((LANES, n_res), 0), iota((LANES, n_res), 1)
        hit = (col == (row // SLOT) * res + row % SLOT) & (row % SLOT < res)
        return jnp.where(hit, 1.0, 0.0).astype(BF16)

    def head_rows(heads, width, ref):
        for h in range(heads):
            row = iota((heads * width, LANES), 0)
            ref[h] = jnp.where((row >= h * width) & (row < (h + 1) * width), 1.0, 0.0).astype(BF16)

    pad = pad_matrix()
    tail = jnp.where(iota((n_res, LANES), 0) == iota((n_res, LANES), 1), 1.0, 0.0).astype(BF16)
    head_rows(heads_m, d_m, hm8)
    head_rows(heads_z, d_z, hm4)
    row, col = iota((LANES, LANES), 0), iota((LANES, LANES), 1)
    seq_of = ((col % (n_seq // 2)) // half) * seqs + (col // (n_seq // 2)) * half + col % half
    seq_perm = jnp.where(row == seq_of, 1.0, 0.0).astype(BF16)
    for c in range(crops):
        mask_bf = mask_in[c].astype(F32).astype(BF16)
        mask_t[c] = mm(mm(pad, mask_bf).astype(BF16), seq_perm)
        mask_r[c] = mm(mask_bf, tail, TN)
    res_r[...] = mm(res_in[...].astype(F32).astype(BF16), tail)
    term = MASK_SCALE * d_m ** 0.5
    aug[...] = jnp.zeros(aug.shape, F32)
    ones = jnp.zeros((AUG, 2 * LANES), F32)
    for k in range(3):
        piece = float(np.array(term, dtype=BF16))
        term = term - piece
        aug[k:k + 1, :] = jnp.full((1, LANES), piece, F32)
        ones = jnp.where(iota(ones.shape, 0) == k, 1.0, ones)
    one_rows[...] = ones.astype(BF16)
    for k, w in enumerate((w_rb, w_sb, w_eb)):
        wt_b[k] = jnp.zeros(wt_b.shape[1:], BF16)
        wt_b[k, :w.shape[0], :] = w[...]
    wt_ro[...] = w_ro[...].astype(F32).T.astype(BF16)
    wt_co[...] = w_co[...].astype(F32).T.astype(BF16)
    o_w = w_ac.shape[0] // 2
    stg_z[:o_w * o_w, :] = w_oo[...].astype(F32)
    for k in range(0, o_w, LANES // o_w):
        rows = [stg_z[pl.ds(f, o_w, stride=o_w), :] for f in range(k, k + LANES // o_w)]
        w_oo_t[:, k * o_w:k * o_w + LANES] = jnp.concatenate(rows, axis=0).T.astype(BF16)

    stg_b[...] = jnp.zeros(stg_b.shape, F32)
    stg_c[...] = jnp.zeros(stg_c.shape, F32)

    def grouped(count, size, fn):
        while count % size:
            size -= 1

        def step(b, carry):
            fn([b * size + t for t in range(size)])
            return carry
        lax.fori_loop(0, count // size, step, 0)

    def put_bias(y, k, heads, rows):
        b = mm(wt_b[k], y, NT)
        for t, i in enumerate(rows):
            for h in range(heads):
                stg_b[h, pl.ds(i, 1), :] = b[h:h + 1, t * LANES:(t + 1) * LANES]

    def stack(ys):
        fill = jnp.zeros((LANES - n_res, ys[0].shape[1]), BF16)
        return jnp.concatenate([part for y in ys for part in (y, fill)], axis=0)

    def dense(x):
        return jnp.concatenate([x[p * SLOT:p * SLOT + res] for p in range(n)], axis=0)

    def keep(p, width, slots, length, mask_rows=None):
        for t, slot in enumerate(slots):
            part = slice(t * LANES, (t + 1) * LANES)
            keys = p[width:2 * width, part]
            if mask_rows is not None:
                keys = jnp.concatenate([keys, (mask_rows[t] - 1.0) * aug[...]], axis=0)
            qbuf[slot, :width] = p[:width, part].astype(BF16)
            kbuf[slot, :length, :keys.shape[0]] = keys.T[:length].astype(BF16)
            vbuf[slot, :width] = p[2 * width:3 * width, part].astype(BF16)
            gbuf[slot, :width] = jax.nn.sigmoid(p[3 * width:, part])

    def column(rowvec):
        return jnp.broadcast_to(rowvec, (LANES, LANES)).T[:n_res]

    def gathered_bias(buf, c, heads, width, flip, add):
        for h in range(heads):
            b = dense(jnp.concatenate([buf[c, p, h].astype(F32) for p in range(n)], axis=0))
            if flip:
                b = jnp.concatenate([b, jnp.zeros((LANES - n_res, LANES), F32)], axis=0).T[:n_res]
            b = b * width ** 0.5
            bias[h] = b if add is None else b + add

    def logits(idx, base, heads, width, head_mask, length, masked):
        c = heads * width
        for i in idx:
            q_t, keys = qbuf[base + i, :c], kbuf[base + i, :length, :c + (AUG if masked else 0)]
            for pair in range(heads // 2):
                rhs = jnp.concatenate([q_t * head_mask[2 * pair], q_t * head_mask[2 * pair + 1]], axis=1)
                if masked:
                    rhs = jnp.concatenate([rhs, one_rows[...]], axis=0)
                raw[i, pair, :length] = mm(keys, rhs)

    def softmax(idx, heads, width, length, biased):
        scale2 = LOG2E * width ** -0.5
        for i in idx:
            for h in range(heads):
                part = slice((h % 2) * LANES, (h % 2 + 1) * LANES)
                x = raw[i, h // 2, :length, part]
                if biased:
                    x = x + bias[h]
                e = jnp.exp2((x - jnp.max(x, axis=0, keepdims=True)) * scale2)
                inv[i, h:h + 1, :] = 1.0 / jnp.sum(e, axis=0, keepdims=True)
                prob[i, h // 2, :length, part] = e.astype(BF16)

    def mixed(idx, base, heads, width, length):
        c = heads * width
        raws = [[mm(vbuf[base + i, 2 * p * width:2 * (p + 1) * width, :length], prob[i, p, :length])
                 for p in range(heads // 2)] for i in idx]
        outs = []
        for i, r in zip(idx, raws):
            parts = []
            for p in range(heads // 2):
                parts.append(r[p][:width, :LANES] * inv[i, 2 * p:2 * p + 1, :])
                parts.append(r[p][width:, LANES:] * inv[i, 2 * p + 1:2 * p + 2, :])
            outs.append((jnp.concatenate(parts, axis=0) * gbuf[base + i, :c]).astype(BF16))
        return outs

    def row_bias(c):
        def step(idx):
            put_bias(stack([layer_norm(z_in[c, i].astype(F32)) for i in idx]), 0, heads_m, idx)
        grouped(res, 6, step)
        ag_r[c, me] = stg_b[...].astype(BF16)
        start(gather_copies(0, c, ag_r))

    loop(crops, row_bias)

    def row_prep(c):
        def prep(idx):
            fill = jnp.zeros((c_m, LANES - n_res), F32)
            ms = [jnp.concatenate([m_in[c, s].astype(F32), fill], axis=1) for s in idx]
            keep(mm(wt_r[...], jnp.concatenate([layer_norm_t(x) for x in ms], axis=1)), c_m,
                 [c * slots + s for s in idx], n_res, [mask_r[c, pl.ds(me * seqs + s, 1), :] for s in idx])
            for s, x in zip(idx, ms):
                xw[c * slots + s] = x
        grouped(seqs, 4, prep)

    loop(crops, row_prep)

    def row_attention(c):
        base = c * slots
        grouped(seqs, 4, lambda idx: logits(idx, base, heads_m, d_m, hm8, n_res, True))
        gather_wait(0, c, ag_r)
        gathered_bias(ag_r, c, heads_m, d_m, True, None)
        grouped(seqs, 1, lambda idx: softmax(idx, heads_m, d_m, n_res, True))

        def step(idx):
            both = [s + t * half for s in idx for t in range(2)]
            upd = mm(wt_ro[...], jnp.concatenate(mixed(both, base, heads_m, d_m, n_res), axis=1))
            new = [xw[base + s] + upd[:, t * LANES:(t + 1) * LANES] for t, s in enumerate(both)]
            for k, s in enumerate(idx):
                x2 = jnp.concatenate(new[2 * k:2 * k + 2], axis=0).T
                stg_m[pl.ds(s, n_res, stride=half), :] = x2[:n_res]
        grouped(half, 4, step)
        for p in range(n):
            snd_m[c, p] = stg_m[p * res * half:(p + 1) * res * half, :].reshape(res, half, LANES).astype(BF16)
        rcv_m[c, me] = snd_m[c, me]
        start(swap_copies(1, c, snd_m, rcv_m))

    loop(crops, row_attention)

    def col_attention(c):
        base = c * slots
        arrivals(1, c, lambda sender: rcv_m.at[c, sender])
        hs = n_seq // 2

        def mask_row(i):
            return mask_t[c, pl.ds(me * SLOT + i, 1), :]

        def prep(idx):
            ys = []
            for k in range(0, len(idx), 2):
                x2 = jnp.concatenate([rcv_m[c, q, i].astype(F32) for i in idx[k:k + 2] for q in range(n)], axis=0).T
                for t, i in enumerate(idx[k:k + 2]):
                    x = jnp.concatenate([x2[:c_m, t * hs:(t + 1) * hs], x2[c_m:, t * hs:(t + 1) * hs]], axis=1)
                    xw[base + i] = x
                    ys.append(layer_norm_t(x))
            keep(mm(wt_c[...], jnp.concatenate(ys, axis=1)), c_m, [base + i for i in idx], LANES,
                 [mask_row(i) for i in idx])
        grouped(res, 4, prep)
        grouped(res, 4, lambda idx: logits(idx, base, heads_m, d_m, hm8, LANES, True))

        @pl.when(c == 1)
        def _():
            relay_near(0)

        grouped(res, 1, lambda idx: softmax(idx, heads_m, d_m, LANES, False))

        @pl.when(c == 1)
        def _():
            relay_far(0)

        def step(idx):
            upd = mm(wt_co[...], jnp.concatenate(mixed(idx, base, heads_m, d_m, LANES), axis=1))
            new = [(xw[base + i] + upd[:, t * LANES:(t + 1) * LANES]).astype(BF16).astype(F32)
                  for t, i in enumerate(idx)]
            ac = mm(w_ac[...], jnp.concatenate([layer_norm_t(x) for x in new], axis=1)).astype(BF16).astype(F32)
            for k in range(0, len(idx), 2):
                two = jnp.concatenate([
                    jnp.concatenate([x[:, :hs] for x in new[k:k + 2]], axis=1),
                    jnp.concatenate([x[:, hs:] for x in new[k:k + 2]], axis=1)], axis=0).T
                for t, i in enumerate(idx[k:k + 2]):
                    for q in range(n):
                        snd_b[c, q, i] = two[t * hs + q * half:t * hs + (q + 1) * half].astype(BF16)
            for t, i in enumerate(idx):
                part = ac[:, t * LANES:(t + 1) * LANES] * mask_row(i)
                abuf[c, pl.ds(pl.multiple_of(i * o_w, o_w), o_w), :] = part[:o_w].astype(BF16)
                stg_c[pl.ds(i, o_w, stride=SLOT), :] = part[o_w:]
        grouped(res, 4, step)
        ag_c[c, me] = stg_c[...].reshape(o_w, SLOT, LANES).astype(BF16)
        relay_own(c)
        rcv_b[c, me] = snd_b[c, me]
        start(swap_copies(3, c, snd_b, rcv_b))

    loop(crops, col_attention)

    def outer_product(c):
        base = c * slots
        relay_done(c)
        stg_b[...] = jnp.zeros(stg_b.shape, F32)
        mloc = mask_t[c, pl.ds(pl.multiple_of(me * SLOT, SLOT), SLOT), :].astype(BF16)
        norm[...] = 1.0 / (mm(mloc, mask_t[c].astype(BF16), NT) + OPM_EPS)

        def outer(fs):
            outs = []
            for k in range(0, len(fs), 2):
                rhs = jnp.concatenate([ag_c[c, p, f] for f in fs[k:k + 2] for p in range(n)], axis=0)
                outs.append(mm(abuf[c], rhs, NT))
            for k, f in enumerate(fs):
                out = outs[k // 2][:, (k % 2) * LANES:(k % 2 + 1) * LANES]
                for i in range(res):
                    obuf[i, pl.ds(pl.multiple_of(f * o_w, o_w), o_w), :] = (
                        out[i * o_w:(i + 1) * o_w] * norm[i:i + 1, :]).astype(BF16)
        grouped(o_w, 4, outer)

        @pl.when(c == 0)
        def _():
            relay_near(1)

        def update(idx):
            rhs = [jnp.concatenate([obuf[i] for i in idx[k:k + 2]], axis=1) for k in range(0, len(idx), 2)]
            upds = [mm(w_oo_t[...], r) for r in rhs]
            for k, i in enumerate(idx):
                upd = upds[k // 2][:, (k % 2) * LANES:(k % 2 + 1) * LANES].T
                zw[c, i] = (z_in[c, i].astype(F32) + dense(upd)).astype(BF16)
        grouped(res, 4, update)

        @pl.when(c == 0)
        def _():
            relay_far(1)

        def prep(idx):
            y = stack([layer_norm(zw[c, i].astype(F32)) for i in idx])
            put_bias(y, 1, heads_z, idx)
            keep(mm(wt_s[...], y, NT), c_z, [base + i for i in idx], n_res)
        grouped(res, 4, prep)
        ag_s[c, me] = stg_b[:heads_z].astype(BF16)
        start(gather_copies(4, c, ag_s))

    loop(crops, outer_product)

    def res_bias(c):
        return column((res_r[pl.ds(c, 1), :] - 1.0) * (MASK_SCALE * d_z ** 0.5))

    def tri_start(c):
        base = c * slots
        grouped(res, 4, lambda idx: logits(idx, base, heads_z, d_z, hm4, n_res, False))
        gather_wait(4, c, ag_s)
        gathered_bias(ag_s, c, heads_z, d_z, True, res_bias(c))
        stg_b[...] = jnp.zeros(stg_b.shape, F32)
        grouped(res, 2, lambda idx: softmax(idx, heads_z, d_z, n_res, True))

        def step(idx):
            upds = [mm(o, w_so[...], TN) for o in mixed(idx, base, heads_z, d_z, n_res)]
            zs = [(zw[c, i].astype(F32) + upd[:n_res]).astype(BF16).astype(F32) for i, upd in zip(idx, upds)]
            for i, z in zip(idx, zs):
                stg_z[pl.ds(i, n_res, stride=res), :] = z
            put_bias(stack([layer_norm(z) for z in zs]), 2, heads_z, idx)
        grouped(res, 4, step)
        ag_e[c, me] = stg_b[:heads_z].astype(BF16)
        start(gather_copies(5, c, ag_e))

        for p in range(n):
            snd_z[c, p] = stg_z[p * res * res:(p + 1) * res * res, :].astype(BF16)
        rcv_z[c, me] = snd_z[c, me]
        start(swap_copies(6, c, snd_z, rcv_z))

    loop(crops, tri_start)

    part_rows = res // pieces

    def piece_copies(c, g):
        return copies(7 + g, c, lambda peer: snd_y.at[c, g, peer], zback.at[c, g, me])

    def tri_end(c):
        base = c * slots
        arrivals(6, c, lambda sender: rcv_z.at[c, sender])
        for q in range(n):
            block = rcv_z[c, q].astype(F32)
            for j in range(res):
                xs[j, q * res:(q + 1) * res, :] = block[j * res:(j + 1) * res]

        def prep(idx):
            keep(mm(wt_e[...], stack([layer_norm(xs[j]) for j in idx]), NT), c_z, [base + j for j in idx], n_res)
        grouped(res, 4, prep)
        gather_wait(5, c, ag_e)
        gathered_bias(ag_e, c, heads_z, d_z, False, res_bias(c))

        def step(g):
            idx = [g * part_rows + t for t in range(part_rows)]
            logits(idx, base, heads_z, d_z, hm4, n_res, False)
            softmax(idx, heads_z, d_z, n_res, True)
            upds = [mm(o, w_eo[...], TN) for o in mixed(idx, base, heads_z, d_z, n_res)]
            for t, (j, upd) in enumerate(zip(idx, upds)):
                stg_m[pl.ds(t, n_res, stride=part_rows), :] = xs[j] + upd[:n_res]
            size = res * part_rows
            for q in range(n):
                snd_y[c, g, q] = stg_m[q * size:(q + 1) * size, :].astype(BF16)
            start(piece_copies(c, g))
            zback[c, g, me] = snd_y[c, g, me]
        loop(pieces, step)

    loop(crops, tri_end)

    def put_m(c):
        arrivals(3, c, lambda sender: rcv_b.at[c, sender])
        stg_m[...] = rcv_b[c].astype(F32).reshape(n * res * half, LANES)

        def step(idx):
            for s in idx:
                x2 = stg_m[pl.ds(s, n_res, stride=half), :].T
                m_out[c, s] = x2[:c_m].astype(BF16)
                m_out[c, s + half] = x2[c_m:].astype(BF16)
        grouped(half, 4, step)

    loop(crops, put_m)

    def put_z(c):
        for g in range(pieces):
            arrivals(7 + g, c, lambda sender: zback.at[c, g, sender])
        for p in range(n):
            for g in range(pieces):
                block = zback[c, g, p].astype(F32)
                row0 = p * res + g * part_rows
                for i in range(res):
                    xs[i, row0:row0 + part_rows, :] = block[i * part_rows:(i + 1) * part_rows]

        def step(i):
            z_out[c, i] = xs[i].astype(BF16)
        for i in range(res):
            step(i)

    loop(crops, put_z)

    def drain(c):
        finish(gather_copies(0, c, ag_r))
        finish(swap_copies(1, c, snd_m, rcv_m))
        for slot in range(n - 1):
            block_copy(c, me, device(1), slot).wait_send()
        finish(swap_copies(3, c, snd_b, rcv_b))
        finish(gather_copies(4, c, ag_s))
        finish(gather_copies(5, c, ag_e))
        finish(swap_copies(6, c, snd_z, rcv_z))
        for g in range(pieces):
            finish(piece_copies(c, g))

    loop(crops, drain)


def solution(mesh):
    n = mesh.shape[GROUP_AXIS]
    rows_spec = P(PART_AXIS, GROUP_AXIS, None, None)
    in_specs = (rows_spec, rows_spec, P(PART_AXIS, None, None), P(PART_AXIS, None)) + (P(),) * N_WEIGHTS

    def local_block(m, z, msa_mask, res_mask, w_rb, w_rq, w_ro, w_cq, w_co, w_ac, w_oo, w_sb, w_sq, w_so,
                    w_eb, w_eq, w_eo):
        crops, seqs, n_res, c_m = m.shape
        res, c_z = z.shape[1], z.shape[3]
        heads_m, heads_z = w_rq.shape[2], w_sq.shape[2]
        o_w = w_ac.shape[2]
        half = seqs // 2
        assert n == 8 and crops == 2 and res % 3 == 0 and n * SLOT == LANES and res <= SLOT and n * seqs == LANES and 2 * c_m == LANES and c_z == LANES
        flat = lambda w: jnp.moveaxis(w, 0, -1).reshape(-1, w.shape[0])
        tall = lambda w: w.reshape(-1, w.shape[-1])
        args = (m.swapaxes(2, 3), z, msa_mask.swapaxes(1, 2), res_mask, w_rb.T, flat(w_rq), tall(w_ro), flat(w_cq),
                tall(w_co), flat(w_ac), tall(w_oo), w_sb.T, flat(w_sq), tall(w_so), w_eb.T, flat(w_eq), tall(w_eo))
        vm = pltpu.VMEM
        slots = max(seqs, res)
        pieces = 3
        piece = res * res // pieces
        scratch = [
            vm((crops, n, heads_m, SLOT, LANES), BF16),
            vm((crops, n, o_w, SLOT, LANES), BF16),
            vm((crops, n, heads_z, SLOT, LANES), BF16),
            vm((crops, n, heads_z, SLOT, LANES), BF16),
            vm((crops, n, res, half, LANES), BF16),
            vm((crops, n, res, half, LANES), BF16),
            vm((crops, n, res, half, LANES), BF16),
            vm((crops, n, res, half, LANES), BF16),
            vm((crops, n, res * res, LANES), BF16),
            vm((crops, n, res * res, LANES), BF16),
            vm((crops, pieces, n, piece, LANES), BF16),
            vm((crops, pieces, n, piece, LANES), BF16),
            pltpu.SemaphoreType.DMA((12, crops, n)),
            pltpu.SemaphoreType.DMA((12, crops, n)),
        ]
        local = [
            vm((crops, res, n_res, LANES), BF16),
            vm((crops * slots, c_m, LANES), F32),
            vm((crops * slots, LANES, LANES), BF16),
            vm((crops * slots, LANES, LANES), BF16),
            vm((crops * slots, LANES, LANES), BF16),
            vm((crops * slots, LANES, LANES), F32),
            vm((heads_m, n_res, LANES), F32),
            vm((res, o_w * o_w, LANES), BF16),
            vm((n * res * half, LANES), F32),
            vm((o_w * SLOT, LANES), F32),
            vm((heads_m, SLOT, LANES), F32),
            vm((n_res * res, LANES), F32),
            vm((crops, res * o_w, LANES), BF16),
            vm((crops, LANES, LANES), F32),
            vm((crops, n * seqs, LANES), F32),
            vm((crops, LANES), F32),
            vm((slots, heads_m // 2, LANES, 2 * LANES), F32),
            vm((slots, heads_m // 2, LANES, 2 * LANES), BF16),
            vm((slots, heads_m, LANES), F32),
            vm((SLOT, LANES), F32),
            vm((heads_m, c_m, LANES), BF16),
            vm((heads_z, c_z, LANES), BF16),
            vm((c_m, c_m), BF16),
            vm((c_m, c_m), BF16),
            vm((LANES, o_w * o_w), BF16),
            vm((3, SLOT, LANES), BF16),
            vm((AUG, LANES), F32),
            vm((AUG, 2 * LANES), BF16),
            vm((res, n_res, LANES), F32),
        ]
        cfg = dict(n=n, heads_m=heads_m, heads_z=heads_z, slots=slots, pieces=pieces, local=local)
        spec = pl.BlockSpec(memory_space=pltpu.VMEM)
        m_new, z_new = pl.pallas_call(
            functools.partial(body, cfg),
            out_shape=(jax.ShapeDtypeStruct((crops, seqs, c_m, n_res), BF16), jax.ShapeDtypeStruct(z.shape, BF16)),
            in_specs=[spec] * len(args),
            out_specs=(spec, spec),
            scratch_shapes=scratch,
            compiler_params=pltpu.CompilerParams(collective_id=0, has_side_effects=True,
                                                 vmem_limit_bytes=60 * 1024 * 1024),
        )(*args)
        return m_new.swapaxes(2, 3), z_new

    return jax.shard_map(local_block, mesh=mesh, in_specs=in_specs, out_specs=(rows_spec, rows_spec),
                         check_vma=False)
```

```python
import functools
import math

import jax
import jax.numpy as jnp
import numpy as np
from jax import lax
from jax.experimental import pallas as pl
from jax.experimental.pallas import tpu as pltpu
from jax.sharding import PartitionSpec as P

MASK_SCALE = 10000.0
LN_EPS = 1e-5
OPM_EPS = 1e-3
N_WEIGHTS = 13
PART_AXIS = 'data'
GROUP_AXIS = 'dap'
LOG2E = math.log2(math.e)
AUG = 16
LANES = 128
SLOT = 16
F32 = jnp.float32
BF16 = jnp.bfloat16
NN = (((1,), (0,)), ((), ()))
NT = (((1,), (1,)), ((), ()))
TN = (((0,), (0,)), ((), ()))


def mm(lhs, rhs, dims=NN):
    return lax.dot_general(lhs, rhs, dims, preferred_element_type=F32)


def layer_norm(x_float):
    mean_val = jnp.mean(x_float, axis=-1, keepdims=True)
    centred = x_float - mean_val
    var_val = jnp.mean(centred * centred, axis=-1, keepdims=True)
    return (centred * lax.rsqrt(var_val + LN_EPS)).astype(BF16)


def layer_norm_t(x_float):
    mean_val = jnp.mean(x_float, axis=0, keepdims=True)
    centred = x_float - mean_val
    var_val = jnp.mean(centred * centred, axis=0, keepdims=True)
    return (centred * lax.rsqrt(var_val + LN_EPS)).astype(BF16)


def iota(shape, axis):
    return lax.broadcasted_iota(jnp.int32, shape, axis)


def body(cfg, *refs):
    pl.run_scoped(functools.partial(scoped_body, cfg, refs), *cfg['local'])


def scoped_body(cfg, refs, *local):
    n = cfg['n']
    (m_in, z_in, mask_in, res_in, w_rb, wt_r, w_ro, wt_c, w_co, w_ac, w_oo,
     w_sb, wt_s, w_so, w_eb, wt_e, w_eo, m_out, z_out,
     ag_r, ag_c, ag_s, ag_e, snd_m, rcv_m, snd_b, rcv_b, snd_z, rcv_z, snd_y, zback, send_sem, recv_sem,
     ring_send, ring_recv) = refs
    (zw, xw, kbuf, qbuf, vbuf, gbuf, bias, obuf, stg_m, stg_c, stg_b, stg_z, abuf,
     mask_t, mask_r, res_r, raw, prob, inv, norm, hm8, hm4, wt_ro, wt_co, w_oo_t, wt_b, aug, one_rows, xs, mask_n) = local
    crops, seqs, c_m, n_res = m_in.shape
    res = z_in.shape[1]
    c_z = z_in.shape[3]
    half = seqs // 2
    heads_m, heads_z = cfg['heads_m'], cfg['heads_z']
    d_m, d_z = c_m // heads_m, c_z // heads_z
    n_seq = n * seqs
    slots, pieces = cfg['slots'], cfg['pieces']
    part_rows, n_blocks = res // pieces, crops * pieces
    me = lax.axis_index(GROUP_AXIS)

    barrier = pltpu.get_barrier_semaphore()
    for r in range(1, n):
        pl.semaphore_signal(barrier, inc=1, device_id={GROUP_AXIS: lax.rem(me + r, n)},
                            device_id_type=pl.DeviceIdType.MESH)
    pl.semaphore_wait(barrier, n - 1)

    def copies(exch, c, src_of, dst):
        out = []
        for r in range(1, n):
            peer = lax.rem(me + r, n)
            out.append(pltpu.make_async_remote_copy(
                src_ref=src_of(peer), dst_ref=dst, send_sem=send_sem.at[exch, c, r], recv_sem=recv_sem.at[exch, c, r],
                device_id={GROUP_AXIS: peer}, device_id_type=pl.DeviceIdType.MESH))
        return out

    def arrivals(exch, c, slot_of):
        for r in range(1, n):
            sender = lax.rem(me + n - r, n)
            ref = slot_of(sender)
            pltpu.make_async_remote_copy(
                src_ref=ref, dst_ref=ref, send_sem=send_sem.at[exch, c, r], recv_sem=recv_sem.at[exch, c, r],
                device_id={GROUP_AXIS: sender}, device_id_type=pl.DeviceIdType.MESH).wait_recv()

    def gather_copies(exch, c, buf):
        return copies(exch, c, lambda peer: buf.at[c, me], buf.at[c, me])

    def gather_wait(exch, c, buf):
        arrivals(exch, c, lambda sender: buf.at[c, sender])

    def swap_copies(exch, c, snd, rcv):
        return copies(exch, c, lambda peer: snd.at[c, peer], rcv.at[c, me])

    chips, core, chip = n // 2, lax.rem(me, 2), me // 2
    ahead = 1 - 2 * core

    def device(offset, other=False):
        return lax.rem(chip + offset + chips, chips) * 2 + ((1 - core) if other else core)

    def block_copy(k, block, peer, slot):
        c, g = k // pieces, lax.rem(k, pieces)
        return pltpu.make_async_remote_copy(
            src_ref=ag_c.at[c, g, block], dst_ref=ag_c.at[c, g, block], send_sem=ring_send.at[k, slot],
            recv_sem=ring_recv.at[k, block], device_id={GROUP_AXIS: peer}, device_id_type=pl.DeviceIdType.MESH)

    def block_wait(k, block):
        block_copy(k, block, block, 0).wait_recv()

    def relay_own(k):
        for slot, peer in enumerate((device(1), device(-1), device(0, True))):
            block_copy(k, me, peer, slot).start()

    def relay_near(k):
        block_wait(k, device(-1))
        block_wait(k, device(1))
        block_copy(k, device(-ahead), device(ahead), 3).start()
        block_copy(k, device(-1), device(0, True), 4).start()
        block_copy(k, device(1), device(0, True), 5).start()

    def relay_far(k):
        block_wait(k, device(2))
        block_copy(k, device(2), device(0, True), 6).start()

    def relay_done(k):
        for offset in range(chips):
            block_wait(k, device(offset, True))

    def start(descs):
        for d in descs:
            d.start()

    def finish(descs):
        for d in descs:
            d.wait_send()

    def loop(count, fn):
        def step(i, carry):
            fn(i)
            return carry
        lax.fori_loop(0, count, step, 0)

    def pad_matrix():
        row, col = iota((LANES, n_res), 0), iota((LANES, n_res), 1)
        hit = (col == (row // SLOT) * res + row % SLOT) & (row % SLOT < res)
        return jnp.where(hit, 1.0, 0.0).astype(BF16)

    def head_rows(heads, width, ref):
        for h in range(heads):
            row = iota((heads * width, LANES), 0)
            ref[h] = jnp.where((row >= h * width) & (row < (h + 1) * width), 1.0, 0.0).astype(BF16)

    pad = pad_matrix()
    tail = jnp.where(iota((n_res, LANES), 0) == iota((n_res, LANES), 1), 1.0, 0.0).astype(BF16)
    head_rows(heads_m, d_m, hm8)
    head_rows(heads_z, d_z, hm4)
    row, col = iota((LANES, LANES), 0), iota((LANES, LANES), 1)
    seq_of = ((col % (n_seq // 2)) // half) * seqs + (col // (n_seq // 2)) * half + col % half
    seq_perm = jnp.where(row == seq_of, 1.0, 0.0).astype(BF16)
    for c in range(crops):
        mask_bf = mask_in[c].astype(F32).astype(BF16)
        mask_t[c] = mm(mm(pad, mask_bf).astype(BF16), seq_perm)
        mask_n[c, :n_res] = mm(mask_bf, seq_perm).astype(BF16)
        mask_n[c, n_res:] = jnp.zeros((LANES - n_res, LANES), BF16)
        mask_r[c] = mm(mask_bf, tail, TN)
    res_r[...] = mm(res_in[...].astype(F32).astype(BF16), tail)
    term = MASK_SCALE * d_m ** 0.5
    aug[...] = jnp.zeros(aug.shape, F32)
    ones = jnp.zeros((AUG, 2 * LANES), F32)
    for k in range(3):
        piece = float(np.array(term, dtype=BF16))
        term = term - piece
        aug[k:k + 1, :] = jnp.full((1, LANES), piece, F32)
        ones = jnp.where(iota(ones.shape, 0) == k, 1.0, ones)
    one_rows[...] = ones.astype(BF16)
    for k, w in enumerate((w_rb, w_sb, w_eb)):
        wt_b[k] = jnp.zeros(wt_b.shape[1:], BF16)
        wt_b[k, :w.shape[0], :] = w[...]
    wt_ro[...] = w_ro[...].astype(F32).T.astype(BF16)
    wt_co[...] = w_co[...].astype(F32).T.astype(BF16)
    o_w = w_ac.shape[0] // 2
    stg_z[:o_w * o_w, :] = w_oo[...].astype(F32)
    for k in range(0, o_w, LANES // o_w):
        rows = [stg_z[pl.ds(f, o_w, stride=o_w), :] for f in range(k, k + LANES // o_w)]
        w_oo_t[:, k * o_w:k * o_w + LANES] = jnp.concatenate(rows, axis=0).T.astype(BF16)

    stg_b[...] = jnp.zeros(stg_b.shape, F32)

    def grouped(count, size, fn):
        while count % size:
            size -= 1

        def step(b, carry):
            fn([b * size + t for t in range(size)])
            return carry
        lax.fori_loop(0, count // size, step, 0)

    def put_bias(y, k, heads, rows):
        b = mm(wt_b[k], y, NT)
        for t, i in enumerate(rows):
            for h in range(heads):
                stg_b[h, pl.ds(i, 1), :] = b[h:h + 1, t * LANES:(t + 1) * LANES]

    def stack(ys):
        fill = jnp.zeros((LANES - n_res, ys[0].shape[1]), BF16)
        return jnp.concatenate([part for y in ys for part in (y, fill)], axis=0)

    def dense(x):
        return jnp.concatenate([x[p * SLOT:p * SLOT + res] for p in range(n)], axis=0)

    def keep(p, width, slots, length, mask_rows=None):
        for t, slot in enumerate(slots):
            part = slice(t * LANES, (t + 1) * LANES)
            keys = p[width:2 * width, part]
            if mask_rows is not None:
                keys = jnp.concatenate([keys, (mask_rows[t] - 1.0) * aug[...]], axis=0)
            qbuf[slot, :width] = p[:width, part].astype(BF16)
            kbuf[slot, :length, :keys.shape[0]] = keys.T[:length].astype(BF16)
            vbuf[slot, :width] = p[2 * width:3 * width, part].astype(BF16)
            gbuf[slot, :width] = jax.nn.sigmoid(p[3 * width:, part])

    def column(rowvec):
        return jnp.broadcast_to(rowvec, (LANES, LANES)).T[:n_res]

    def gathered_bias(buf, c, heads, width, flip, add):
        for h in range(heads):
            b = dense(jnp.concatenate([buf[c, p, h].astype(F32) for p in range(n)], axis=0))
            if flip:
                b = jnp.concatenate([b, jnp.zeros((LANES - n_res, LANES), F32)], axis=0).T[:n_res]
            b = b * width ** 0.5
            bias[h] = b if add is None else b + add

    def logits(idx, base, heads, width, head_mask, length, masked):
        c = heads * width
        for i in idx:
            q_t, keys = qbuf[base + i, :c], kbuf[base + i, :length, :c + (AUG if masked else 0)]
            for pair in range(heads // 2):
                rhs = jnp.concatenate([q_t * head_mask[2 * pair], q_t * head_mask[2 * pair + 1]], axis=1)
                if masked:
                    rhs = jnp.concatenate([rhs, one_rows[...]], axis=0)
                raw[i, pair, :length] = mm(keys, rhs)

    def softmax(idx, heads, width, length, biased):
        scale2 = LOG2E * width ** -0.5
        for i in idx:
            for h in range(heads):
                part = slice((h % 2) * LANES, (h % 2 + 1) * LANES)
                x = raw[i, h // 2, :length, part]
                if biased:
                    x = x + bias[h]
                e = jnp.exp2((x - jnp.max(x, axis=0, keepdims=True)) * scale2)
                inv[i, h:h + 1, :] = 1.0 / jnp.sum(e, axis=0, keepdims=True)
                prob[i, h // 2, :length, part] = e.astype(BF16)

    def mixed(idx, base, heads, width, length):
        c = heads * width
        raws = [[mm(vbuf[base + i, 2 * p * width:2 * (p + 1) * width, :length], prob[i, p, :length])
                 for p in range(heads // 2)] for i in idx]
        outs = []
        for i, r in zip(idx, raws):
            parts = []
            for p in range(heads // 2):
                parts.append(r[p][:width, :LANES] * inv[i, 2 * p:2 * p + 1, :])
                parts.append(r[p][width:, LANES:] * inv[i, 2 * p + 1:2 * p + 2, :])
            outs.append((jnp.concatenate(parts, axis=0) * gbuf[base + i, :c]).astype(BF16))
        return outs

    def row_bias(c):
        def step(idx):
            put_bias(stack([layer_norm(z_in[c, i].astype(F32)) for i in idx]), 0, heads_m, idx)
        grouped(res, 6, step)
        ag_r[c, me] = stg_b[...].astype(BF16)
        start(gather_copies(0, c, ag_r))

    loop(crops, row_bias)

    def row_prep(c):
        def prep(idx):
            fill = jnp.zeros((c_m, LANES - n_res), F32)
            ms = [jnp.concatenate([m_in[c, s].astype(F32), fill], axis=1) for s in idx]
            keep(mm(wt_r[...], jnp.concatenate([layer_norm_t(x) for x in ms], axis=1)), c_m,
                 [c * slots + s for s in idx], n_res, [mask_r[c, pl.ds(me * seqs + s, 1), :] for s in idx])
            for s, x in zip(idx, ms):
                xw[c * slots + s] = x
        grouped(seqs, 4, prep)

    loop(crops, row_prep)

    def row_attention(c):
        base = c * slots
        grouped(seqs, 4, lambda idx: logits(idx, base, heads_m, d_m, hm8, n_res, True))
        gather_wait(0, c, ag_r)
        gathered_bias(ag_r, c, heads_m, d_m, True, None)
        grouped(seqs, 1, lambda idx: softmax(idx, heads_m, d_m, n_res, True))

        def step(idx):
            both = [s + t * half for s in idx for t in range(2)]
            upd = mm(wt_ro[...], jnp.concatenate(mixed(both, base, heads_m, d_m, n_res), axis=1))
            new = [xw[base + s] + upd[:, t * LANES:(t + 1) * LANES] for t, s in enumerate(both)]
            for k, s in enumerate(idx):
                x2 = jnp.concatenate(new[2 * k:2 * k + 2], axis=0).T
                stg_m[pl.ds(s, n_res, stride=half), :] = x2[:n_res]
        grouped(half, 4, step)
        for p in range(n):
            snd_m[c, p] = stg_m[p * res * half:(p + 1) * res * half, :].reshape(res, half, LANES).astype(BF16)
        rcv_m[c, me] = snd_m[c, me]
        start(swap_copies(1, c, snd_m, rcv_m))

    loop(crops, row_attention)

    def col_attention(c):
        base = c * slots
        arrivals(1, c, lambda sender: rcv_m.at[c, sender])
        hs = n_seq // 2

        def mask_row(i):
            return mask_t[c, pl.ds(me * SLOT + i, 1), :]

        def prep(idx):
            ys = []
            for k in range(0, len(idx), 2):
                x2 = jnp.concatenate([rcv_m[c, q, i].astype(F32) for i in idx[k:k + 2] for q in range(n)], axis=0).T
                for t, i in enumerate(idx[k:k + 2]):
                    x = jnp.concatenate([x2[:c_m, t * hs:(t + 1) * hs], x2[c_m:, t * hs:(t + 1) * hs]], axis=1)
                    xw[base + i] = x
                    ys.append(layer_norm_t(x))
            keep(mm(wt_c[...], jnp.concatenate(ys, axis=1)), c_m, [base + i for i in idx], LANES,
                 [mask_row(i) for i in idx])
        grouped(res, 4, prep)

        def group(g):
            idx = [g * part_rows + t for t in range(part_rows)]
            logits(idx, base, heads_m, d_m, hm8, LANES, True)
            softmax(idx, heads_m, d_m, LANES, False)
            upd = mm(wt_co[...], jnp.concatenate(mixed(idx, base, heads_m, d_m, LANES), axis=1))
            new = [(xw[base + i] + upd[:, t * LANES:(t + 1) * LANES]).astype(BF16).astype(F32)
                   for t, i in enumerate(idx)]
            ac = mm(w_ac[...], jnp.concatenate([layer_norm_t(x) for x in new], axis=1)).astype(BF16).astype(F32)
            for t, i in enumerate(idx):
                part = ac[:, t * LANES:(t + 1) * LANES] * mask_row(i)
                ag_c[c, g, me, t] = part[o_w:].astype(BF16)
                abuf[c, pl.ds(pl.multiple_of(i * o_w, o_w), o_w), :] = part[:o_w].astype(BF16)
            k = c * pieces + g
            relay_own(k)

            @pl.when(k >= 2)
            def _():
                relay_near(k - 2)

            @pl.when(k >= 3)
            def _():
                relay_far(k - 3)

            for t in range(0, part_rows, 2):
                two = jnp.concatenate([
                    jnp.concatenate([x[:, :hs] for x in new[t:t + 2]], axis=1),
                    jnp.concatenate([x[:, hs:] for x in new[t:t + 2]], axis=1)], axis=0).T
                for u, i in enumerate(idx[t:t + 2]):
                    for q in range(n):
                        snd_b[c, q, i] = two[u * hs + q * half:u * hs + (q + 1) * half].astype(BF16)
        loop(pieces, group)
        rcv_b[c, me] = snd_b[c, me]

    loop(crops, col_attention)

    def outer_product(c):
        base = c * slots
        @pl.when(c == 0)
        def _():
            relay_near(n_blocks - 2)

        for g in range(pieces):
            relay_done(c * pieces + g)
        stg_b[...] = jnp.zeros(stg_b.shape, F32)
        mloc = mask_t[c, pl.ds(pl.multiple_of(me * SLOT, SLOT), SLOT), :].astype(BF16)
        norm[...] = 1.0 / (mm(mloc, mask_n[c], NT) + OPM_EPS)
        pitch = n_res + 8

        def spread(p):
            for g in range(pieces):
                for t in range(part_rows):
                    stg_c[pl.ds(p * res + g * part_rows + t, o_w, stride=pitch), :] = ag_c[c, g, p, t].astype(F32)
        loop(n, spread)

        def outer(fs):
            rows = [stg_c[pl.ds(pl.multiple_of(f * pitch, 8), n_res), :].astype(BF16) for f in fs]
            outs = [mm(abuf[c], stack(rows[k:k + 2]), NT) for k in range(0, len(fs), 2)]
            for k, f in enumerate(fs):
                out = outs[k // 2][:, (k % 2) * LANES:(k % 2 + 1) * LANES]
                for i in range(res):
                    obuf[i, pl.ds(pl.multiple_of(f * o_w, o_w), o_w), :] = (
                        out[i * o_w:(i + 1) * o_w] * norm[i:i + 1, :]).astype(BF16)
        grouped(o_w, 4, outer)

        @pl.when(c == 0)
        def _():
            relay_near(n_blocks - 1)
            relay_far(n_blocks - 3)

        def update(idx):
            rhs = [jnp.concatenate([obuf[i] for i in idx[k:k + 2]], axis=1) for k in range(0, len(idx), 2)]
            upds = [mm(w_oo_t[...], r) for r in rhs]
            for k, i in enumerate(idx):
                upd = upds[k // 2][:, (k % 2) * LANES:(k % 2 + 1) * LANES].T
                zw[c, i] = (z_in[c, i].astype(F32) + upd[:n_res]).astype(BF16)
        grouped(res, 4, update)

        @pl.when(c == 0)
        def _():
            relay_far(n_blocks - 2)
            relay_far(n_blocks - 1)

        def prep(idx):
            y = stack([layer_norm(zw[c, i].astype(F32)) for i in idx])
            put_bias(y, 1, heads_z, idx)
            keep(mm(wt_s[...], y, NT), c_z, [base + i for i in idx], n_res)
        grouped(res, 4, prep)
        ag_s[c, me] = stg_b[:heads_z].astype(BF16)
        start(gather_copies(4, c, ag_s))
        start(swap_copies(3, c, snd_b, rcv_b))

    loop(crops, outer_product)

    def res_bias(c):
        return column((res_r[pl.ds(c, 1), :] - 1.0) * (MASK_SCALE * d_z ** 0.5))

    def piece_copies(first, c, g, snd, rcv):
        return copies(first + g, c, lambda peer: snd.at[c, g, peer], rcv.at[c, g, me])

    def send_rows(zs, snd, c, g):
        for t, z in enumerate(zs):
            stg_m[pl.ds(t, n_res, stride=part_rows), :] = z
        size = res * part_rows
        for q in range(n):
            snd[c, g, q] = stg_m[q * size:(q + 1) * size, :].astype(BF16)

    def take_columns(first, c, rcv):
        for g in range(pieces):
            arrivals(first + g, c, lambda sender: rcv.at[c, g, sender])
        for p in range(n):
            for g in range(pieces):
                block = rcv[c, g, p].astype(F32)
                row0 = p * res + g * part_rows
                for j in range(res):
                    xs[j, row0:row0 + part_rows, :] = block[j * part_rows:(j + 1) * part_rows]

    def tri_start(c):
        base = c * slots
        gather_wait(4, c, ag_s)
        gathered_bias(ag_s, c, heads_z, d_z, True, res_bias(c))
        stg_b[...] = jnp.zeros(stg_b.shape, F32)

        def group(g):
            idx = [g * part_rows + t for t in range(part_rows)]
            logits(idx, base, heads_z, d_z, hm4, n_res, False)
            softmax(idx, heads_z, d_z, n_res, True)
            upds = [mm(o, w_so[...], TN) for o in mixed(idx, base, heads_z, d_z, n_res)]
            zs = [(zw[c, i].astype(F32) + upd[:n_res]).astype(BF16).astype(F32) for i, upd in zip(idx, upds)]
            send_rows(zs, snd_z, c, g)
            start(piece_copies(10, c, g, snd_z, rcv_z))
            rcv_z[c, g, me] = snd_z[c, g, me]
            put_bias(stack([layer_norm(z) for z in zs]), 2, heads_z, idx)
        loop(pieces, group)
        ag_e[c, me] = stg_b[:heads_z].astype(BF16)
        start(gather_copies(5, c, ag_e))

    loop(crops, tri_start)

    def tri_end(c):
        base = c * slots
        take_columns(10, c, rcv_z)

        def prep(idx):
            keep(mm(wt_e[...], stack([layer_norm(xs[j]) for j in idx]), NT), c_z, [base + j for j in idx], n_res)
        grouped(res, 4, prep)
        gather_wait(5, c, ag_e)
        gathered_bias(ag_e, c, heads_z, d_z, False, res_bias(c))

        def step(g):
            idx = [g * part_rows + t for t in range(part_rows)]
            logits(idx, base, heads_z, d_z, hm4, n_res, False)
            softmax(idx, heads_z, d_z, n_res, True)
            upds = [mm(o, w_eo[...], TN) for o in mixed(idx, base, heads_z, d_z, n_res)]
            send_rows([xs[j] + upd[:n_res] for j, upd in zip(idx, upds)], snd_y, c, g)
            start(piece_copies(7, c, g, snd_y, zback))
            zback[c, g, me] = snd_y[c, g, me]
        loop(pieces, step)

    loop(crops, tri_end)

    def put_m(c):
        arrivals(3, c, lambda sender: rcv_b.at[c, sender])
        stg_m[...] = rcv_b[c].astype(F32).reshape(n * res * half, LANES)

        def step(idx):
            for s in idx:
                x2 = stg_m[pl.ds(s, n_res, stride=half), :].T
                m_out[c, s] = x2[:c_m].astype(BF16)
                m_out[c, s + half] = x2[c_m:].astype(BF16)
        grouped(half, 4, step)

    loop(crops, put_m)

    def put_z(c):
        take_columns(7, c, zback)

        def step(i):
            z_out[c, i] = xs[i].astype(BF16)
        for i in range(res):
            step(i)

    loop(crops, put_z)

    def drain(c):
        finish(gather_copies(0, c, ag_r))
        finish(swap_copies(1, c, snd_m, rcv_m))
        for g in range(pieces):
            for slot in range(n - 1):
                block_copy(c * pieces + g, me, device(1), slot).wait_send()
            finish(piece_copies(7, c, g, snd_y, zback))
            finish(piece_copies(10, c, g, snd_z, rcv_z))
        finish(swap_copies(3, c, snd_b, rcv_b))
        finish(gather_copies(4, c, ag_s))
        finish(gather_copies(5, c, ag_e))

    loop(crops, drain)


def solution(mesh):
    n = mesh.shape[GROUP_AXIS]
    rows_spec = P(PART_AXIS, GROUP_AXIS, None, None)
    in_specs = (rows_spec, rows_spec, P(PART_AXIS, None, None), P(PART_AXIS, None)) + (P(),) * N_WEIGHTS

    def local_block(m, z, msa_mask, res_mask, w_rb, w_rq, w_ro, w_cq, w_co, w_ac, w_oo, w_sb, w_sq, w_so,
                    w_eb, w_eq, w_eo):
        crops, seqs, n_res, c_m = m.shape
        res, c_z = z.shape[1], z.shape[3]
        heads_m, heads_z = w_rq.shape[2], w_sq.shape[2]
        o_w = w_ac.shape[2]
        half = seqs // 2
        assert n == 8 and crops == 2 and res % 3 == 0 and n * SLOT == LANES and res <= SLOT and n * seqs == LANES and 2 * c_m == LANES and c_z == LANES
        flat = lambda w: jnp.moveaxis(w, 0, -1).reshape(-1, w.shape[0])
        tall = lambda w: w.reshape(-1, w.shape[-1])
        args = (m.swapaxes(2, 3), z, msa_mask.swapaxes(1, 2), res_mask, w_rb.T, flat(w_rq), tall(w_ro), flat(w_cq),
                tall(w_co), flat(w_ac), tall(w_oo), w_sb.T, flat(w_sq), tall(w_so), w_eb.T, flat(w_eq), tall(w_eo))
        vm = pltpu.VMEM
        slots = max(seqs, res)
        pieces = 3
        piece = res * res // pieces
        scratch = [
            vm((crops, n, heads_m, SLOT, LANES), BF16),
            vm((crops, pieces, n, res // pieces, o_w, LANES), BF16),
            vm((crops, n, heads_z, SLOT, LANES), BF16),
            vm((crops, n, heads_z, SLOT, LANES), BF16),
            vm((crops, n, res, half, LANES), BF16),
            vm((crops, n, res, half, LANES), BF16),
            vm((crops, n, res, half, LANES), BF16),
            vm((crops, n, res, half, LANES), BF16),
            vm((crops, pieces, n, piece, LANES), BF16),
            vm((crops, pieces, n, piece, LANES), BF16),
            vm((crops, pieces, n, piece, LANES), BF16),
            vm((crops, pieces, n, piece, LANES), BF16),
            pltpu.SemaphoreType.DMA((13, crops, n)),
            pltpu.SemaphoreType.DMA((13, crops, n)),
            pltpu.SemaphoreType.DMA((crops * pieces, n)),
            pltpu.SemaphoreType.DMA((crops * pieces, n)),
        ]
        local = [
            vm((crops, res, n_res, LANES), BF16),
            vm((crops * slots, c_m, LANES), F32),
            vm((crops * slots, LANES, LANES), BF16),
            vm((crops * slots, LANES, LANES), BF16),
            vm((crops * slots, LANES, LANES), BF16),
            vm((crops * slots, LANES, LANES), F32),
            vm((heads_m, n_res, LANES), F32),
            vm((res, o_w * o_w, LANES), BF16),
            vm((n * res * half, LANES), F32),
            vm((o_w * (n_res + 8), LANES), F32),
            vm((heads_m, SLOT, LANES), F32),
            vm((n_res * res, LANES), F32),
            vm((crops, res * o_w, LANES), BF16),
            vm((crops, LANES, LANES), F32),
            vm((crops, n * seqs, LANES), F32),
            vm((crops, LANES), F32),
            vm((slots, heads_m // 2, LANES, 2 * LANES), F32),
            vm((slots, heads_m // 2, LANES, 2 * LANES), BF16),
            vm((slots, heads_m, LANES), F32),
            vm((SLOT, LANES), F32),
            vm((heads_m, c_m, LANES), BF16),
            vm((heads_z, c_z, LANES), BF16),
            vm((c_m, c_m), BF16),
            vm((c_m, c_m), BF16),
            vm((LANES, o_w * o_w), BF16),
            vm((3, SLOT, LANES), BF16),
            vm((AUG, LANES), F32),
            vm((AUG, 2 * LANES), BF16),
            vm((res, n_res, LANES), F32),
            vm((crops, LANES, LANES), BF16),
        ]
        cfg = dict(n=n, heads_m=heads_m, heads_z=heads_z, slots=slots, pieces=pieces, local=local)
        spec = pl.BlockSpec(memory_space=pltpu.VMEM)
        m_new, z_new = pl.pallas_call(
            functools.partial(body, cfg),
            out_shape=(jax.ShapeDtypeStruct((crops, seqs, c_m, n_res), BF16), jax.ShapeDtypeStruct(z.shape, BF16)),
            in_specs=[spec] * len(args),
            out_specs=(spec, spec),
            scratch_shapes=scratch,
            compiler_params=pltpu.CompilerParams(collective_id=0, has_side_effects=True,
                                                 vmem_limit_bytes=60 * 1024 * 1024),
        )(*args)
        return m_new.swapaxes(2, 3), z_new

    return jax.shard_map(local_block, mesh=mesh, in_specs=in_specs, out_specs=(rows_spec, rows_spec),
                         check_vma=False)
```

```python
import functools
import math

import jax
import jax.numpy as jnp
import numpy as np
from jax import lax
from jax.experimental import pallas as pl
from jax.experimental.pallas import tpu as pltpu
from jax.sharding import PartitionSpec as P

MASK_SCALE = 10000.0
LN_EPS = 1e-5
OPM_EPS = 1e-3
N_WEIGHTS = 13
PART_AXIS = 'data'
GROUP_AXIS = 'dap'
LOG2E = math.log2(math.e)
AUG = 16
LANES = 128
SLOT = 16
F32 = jnp.float32
BF16 = jnp.bfloat16
NN = (((1,), (0,)), ((), ()))
NT = (((1,), (1,)), ((), ()))
TN = (((0,), (0,)), ((), ()))


def mm(lhs, rhs, dims=NN):
    return lax.dot_general(lhs, rhs, dims, preferred_element_type=F32)


def layer_norm(x_float):
    mean_val = jnp.mean(x_float, axis=-1, keepdims=True)
    centred = x_float - mean_val
    var_val = jnp.mean(centred * centred, axis=-1, keepdims=True)
    return (centred * lax.rsqrt(var_val + LN_EPS)).astype(BF16)


def layer_norm_t(x_float):
    mean_val = jnp.mean(x_float, axis=0, keepdims=True)
    centred = x_float - mean_val
    var_val = jnp.mean(centred * centred, axis=0, keepdims=True)
    return (centred * lax.rsqrt(var_val + LN_EPS)).astype(BF16)


def iota(shape, axis):
    return lax.broadcasted_iota(jnp.int32, shape, axis)


def body(cfg, *refs):
    pl.run_scoped(functools.partial(scoped_body, cfg, refs), *cfg['local'])


def scoped_body(cfg, refs, *local):
    n = cfg['n']
    (m_in, z_in, mask_in, res_in, w_rb, wt_r, w_ro, wt_c, w_co, w_ac, w_oo,
     w_sb, wt_s, w_so, w_eb, wt_e, w_eo, m_out, z_out,
     ag_r, ag_c, ag_s, ag_e, snd_m, rcv_m, snd_b, rcv_b, snd_z, rcv_z, snd_y, zback, send_sem, recv_sem,
     ring_send, ring_recv) = refs
    (zw, xw, kbuf, qbuf, vbuf, gbuf, bias, obuf, stg_m, stg_c, stg_b, stg_z, abuf,
     mask_t, mask_r, res_r, raw, prob, inv, norm, hm8, hm4, wt_ro, wt_co, w_oo_t, wt_b, aug, one_rows, xs, mask_n) = local
    crops, seqs, c_m, n_res = m_in.shape
    res = z_in.shape[1]
    c_z = z_in.shape[3]
    half = seqs // 2
    heads_m, heads_z = cfg['heads_m'], cfg['heads_z']
    d_m, d_z = c_m // heads_m, c_z // heads_z
    n_seq = n * seqs
    slots, pieces = cfg['slots'], cfg['pieces']
    part_rows, n_blocks = res // pieces, crops * pieces
    me = lax.axis_index(GROUP_AXIS)

    barrier = pltpu.get_barrier_semaphore()
    for r in range(1, n):
        pl.semaphore_signal(barrier, inc=1, device_id={GROUP_AXIS: lax.rem(me + r, n)},
                            device_id_type=pl.DeviceIdType.MESH)
    pl.semaphore_wait(barrier, n - 1)

    def copies(exch, c, src_of, dst):
        out = []
        for r in range(1, n):
            peer = lax.rem(me + r, n)
            out.append(pltpu.make_async_remote_copy(
                src_ref=src_of(peer), dst_ref=dst, send_sem=send_sem.at[exch, c, r], recv_sem=recv_sem.at[exch, c, r],
                device_id={GROUP_AXIS: peer}, device_id_type=pl.DeviceIdType.MESH))
        return out

    def arrivals(exch, c, slot_of):
        for r in range(1, n):
            sender = lax.rem(me + n - r, n)
            ref = slot_of(sender)
            pltpu.make_async_remote_copy(
                src_ref=ref, dst_ref=ref, send_sem=send_sem.at[exch, c, r], recv_sem=recv_sem.at[exch, c, r],
                device_id={GROUP_AXIS: sender}, device_id_type=pl.DeviceIdType.MESH).wait_recv()

    def gather_copies(exch, c, buf):
        return copies(exch, c, lambda peer: buf.at[c, me], buf.at[c, me])

    def gather_wait(exch, c, buf):
        arrivals(exch, c, lambda sender: buf.at[c, sender])

    def swap_copies(exch, c, snd, rcv):
        return copies(exch, c, lambda peer: snd.at[c, peer], rcv.at[c, me])

    chips, core, chip = n // 2, lax.rem(me, 2), me // 2
    ahead = 1 - 2 * core

    def device(offset, other=False):
        return lax.rem(chip + offset + chips, chips) * 2 + ((1 - core) if other else core)

    def block_copy(k, block, peer, slot):
        c, g = k // pieces, lax.rem(k, pieces)
        return pltpu.make_async_remote_copy(
            src_ref=ag_c.at[c, g, block], dst_ref=ag_c.at[c, g, block], send_sem=ring_send.at[k, slot],
            recv_sem=ring_recv.at[k, block], device_id={GROUP_AXIS: peer}, device_id_type=pl.DeviceIdType.MESH)

    def block_wait(k, block):
        block_copy(k, block, block, 0).wait_recv()

    def relay_own(k):
        for slot, peer in enumerate((device(1), device(-1), device(0, True))):
            block_copy(k, me, peer, slot).start()

    def relay_near(k):
        block_wait(k, device(-1))
        block_wait(k, device(1))
        block_copy(k, device(-ahead), device(ahead), 3).start()
        block_copy(k, device(-1), device(0, True), 4).start()
        block_copy(k, device(1), device(0, True), 5).start()

    def relay_far(k):
        block_wait(k, device(2))
        block_copy(k, device(2), device(0, True), 6).start()

    def relay_done(k):
        for offset in range(chips):
            block_wait(k, device(offset, True))

    def start(descs):
        for d in descs:
            d.start()

    def finish(descs):
        for d in descs:
            d.wait_send()

    def loop(count, fn):
        def step(i, carry):
            fn(i)
            return carry
        lax.fori_loop(0, count, step, 0)

    def pad_matrix():
        row, col = iota((LANES, n_res), 0), iota((LANES, n_res), 1)
        hit = (col == (row // SLOT) * res + row % SLOT) & (row % SLOT < res)
        return jnp.where(hit, 1.0, 0.0).astype(BF16)

    def head_rows(heads, width, ref):
        for h in range(heads):
            row = iota((heads * width, LANES), 0)
            ref[h] = jnp.where((row >= h * width) & (row < (h + 1) * width), 1.0, 0.0).astype(BF16)

    pad = pad_matrix()
    tail = jnp.where(iota((n_res, LANES), 0) == iota((n_res, LANES), 1), 1.0, 0.0).astype(BF16)
    head_rows(heads_m, d_m, hm8)
    head_rows(heads_z, d_z, hm4)
    row, col = iota((LANES, LANES), 0), iota((LANES, LANES), 1)
    seq_of = ((col % (n_seq // 2)) // half) * seqs + (col // (n_seq // 2)) * half + col % half
    seq_perm = jnp.where(row == seq_of, 1.0, 0.0).astype(BF16)
    for c in range(crops):
        mask_bf = mask_in[c].astype(F32).astype(BF16)
        mask_t[c] = mm(mm(pad, mask_bf).astype(BF16), seq_perm)
        mask_n[c, :n_res] = mm(mask_bf, seq_perm).astype(BF16)
        mask_n[c, n_res:] = jnp.zeros((LANES - n_res, LANES), BF16)
        mask_r[c] = mm(mask_bf, tail, TN)
    res_r[...] = mm(res_in[...].astype(F32).astype(BF16), tail)
    term = MASK_SCALE * d_m ** 0.5
    aug[...] = jnp.zeros(aug.shape, F32)
    ones = jnp.zeros((AUG, 2 * LANES), F32)
    for k in range(3):
        piece = float(np.array(term, dtype=BF16))
        term = term - piece
        aug[k:k + 1, :] = jnp.full((1, LANES), piece, F32)
        ones = jnp.where(iota(ones.shape, 0) == k, 1.0, ones)
    one_rows[...] = ones.astype(BF16)
    for k, w in enumerate((w_rb, w_sb, w_eb)):
        wt_b[k] = jnp.zeros(wt_b.shape[1:], BF16)
        wt_b[k, :w.shape[0], :] = w[...]
    wt_ro[...] = w_ro[...].astype(F32).T.astype(BF16)
    wt_co[...] = w_co[...].astype(F32).T.astype(BF16)
    o_w = w_ac.shape[0] // 2
    stg_z[:o_w * o_w, :] = w_oo[...].astype(F32)
    for k in range(0, o_w, LANES // o_w):
        rows = [stg_z[pl.ds(f, o_w, stride=o_w), :] for f in range(k, k + LANES // o_w)]
        w_oo_t[:, k * o_w:k * o_w + LANES] = jnp.concatenate(rows, axis=0).T.astype(BF16)

    stg_b[...] = jnp.zeros(stg_b.shape, F32)

    def grouped(count, size, fn):
        while count % size:
            size -= 1

        def step(b, carry):
            fn([b * size + t for t in range(size)])
            return carry
        lax.fori_loop(0, count // size, step, 0)

    def put_bias(y, k, heads, rows):
        b = mm(wt_b[k], y, NT)
        for t, i in enumerate(rows):
            for h in range(heads):
                stg_b[pl.ds(h * res + i, 1), :] = b[h:h + 1, t * LANES:(t + 1) * LANES]

    def stack(ys):
        fill = jnp.zeros((LANES - n_res, ys[0].shape[1]), BF16)
        return jnp.concatenate([part for y in ys for part in (y, fill)], axis=0)

    def keep(p, width, slots, length, mask_rows=None):
        for t, slot in enumerate(slots):
            part = slice(t * LANES, (t + 1) * LANES)
            keys = p[width:2 * width, part]
            if mask_rows is not None:
                keys = jnp.concatenate([keys, (mask_rows[t] - 1.0) * aug[...]], axis=0)
            qbuf[slot, :width] = p[:width, part].astype(BF16)
            kbuf[slot, :length, :keys.shape[0]] = keys.T[:length].astype(BF16)
            vbuf[slot, :width] = p[2 * width:3 * width, part].astype(BF16)
            gbuf[slot, :width] = jax.nn.sigmoid(p[3 * width:, part])

    def column(rowvec):
        return jnp.broadcast_to(rowvec, (LANES, LANES)).T[:n_res]

    def gathered_bias(buf, c, heads, width, flip, add):
        parts = [buf[c, p].astype(F32) for p in range(n)]
        for h in range(heads):
            b = jnp.concatenate([part[h * res:(h + 1) * res] for part in parts], axis=0)
            if flip:
                b = jnp.concatenate([b, jnp.zeros((LANES - n_res, LANES), F32)], axis=0).T[:n_res]
            b = b * width ** 0.5
            bias[h] = b if add is None else b + add

    def logits(idx, base, heads, width, head_mask, length, masked):
        c = heads * width
        for i in idx:
            q_t, keys = qbuf[base + i, :c], kbuf[base + i, :length, :c + (AUG if masked else 0)]
            for pair in range(heads // 2):
                rhs = jnp.concatenate([q_t * head_mask[2 * pair], q_t * head_mask[2 * pair + 1]], axis=1)
                if masked:
                    rhs = jnp.concatenate([rhs, one_rows[...]], axis=0)
                raw[i, pair, :length] = mm(keys, rhs)

    def softmax(idx, heads, width, length, biased):
        scale2 = LOG2E * width ** -0.5
        for i in idx:
            for h in range(heads):
                part = slice((h % 2) * LANES, (h % 2 + 1) * LANES)
                x = raw[i, h // 2, :length, part]
                if biased:
                    x = x + bias[h]
                e = jnp.exp2((x - jnp.max(x, axis=0, keepdims=True)) * scale2)
                inv[i, h:h + 1, :] = 1.0 / jnp.sum(e, axis=0, keepdims=True)
                prob[i, h // 2, :length, part] = e.astype(BF16)

    def mixed(idx, base, heads, width, length):
        c = heads * width
        raws = [[mm(vbuf[base + i, 2 * p * width:2 * (p + 1) * width, :length], prob[i, p, :length])
                 for p in range(heads // 2)] for i in idx]
        outs = []
        for i, r in zip(idx, raws):
            parts = []
            for p in range(heads // 2):
                parts.append(r[p][:width, :LANES] * inv[i, 2 * p:2 * p + 1, :])
                parts.append(r[p][width:, LANES:] * inv[i, 2 * p + 1:2 * p + 2, :])
            outs.append((jnp.concatenate(parts, axis=0) * gbuf[base + i, :c]).astype(BF16))
        return outs

    def row_bias(c):
        def step(idx):
            put_bias(stack([layer_norm(z_in[c, i].astype(F32)) for i in idx]), 0, heads_m, idx)
        grouped(res, 6, step)
        ag_r[c, me] = stg_b[...].astype(BF16)
        start(gather_copies(0, c, ag_r))

    loop(crops, row_bias)

    def row_prep(c):
        def prep(idx):
            fill = jnp.zeros((c_m, LANES - n_res), F32)
            ms = [jnp.concatenate([m_in[c, s].astype(F32), fill], axis=1) for s in idx]
            keep(mm(wt_r[...], jnp.concatenate([layer_norm_t(x) for x in ms], axis=1)), c_m,
                 [c * slots + s for s in idx], n_res, [mask_r[c, pl.ds(me * seqs + s, 1), :] for s in idx])
            for s, x in zip(idx, ms):
                xw[c * slots + s] = x
        grouped(seqs, 4, prep)

    loop(crops, row_prep)

    def row_attention(c):
        base = c * slots
        grouped(seqs, 4, lambda idx: logits(idx, base, heads_m, d_m, hm8, n_res, True))
        gather_wait(0, c, ag_r)
        gathered_bias(ag_r, c, heads_m, d_m, True, None)
        grouped(seqs, 2, lambda idx: softmax(idx, heads_m, d_m, n_res, True))

        def step(idx):
            both = [s + t * half for s in idx for t in range(2)]
            upd = mm(wt_ro[...], jnp.concatenate(mixed(both, base, heads_m, d_m, n_res), axis=1))
            new = [xw[base + s] + upd[:, t * LANES:(t + 1) * LANES] for t, s in enumerate(both)]
            for k, s in enumerate(idx):
                x2 = jnp.concatenate(new[2 * k:2 * k + 2], axis=0).T
                stg_m[pl.ds(s, n_res, stride=half), :] = x2[:n_res]
        grouped(half, 4, step)
        for p in range(n):
            snd_m[c, p] = stg_m[p * res * half:(p + 1) * res * half, :].reshape(res, half, LANES).astype(BF16)
        rcv_m[c, me] = snd_m[c, me]
        start(swap_copies(1, c, snd_m, rcv_m))

    loop(crops, row_attention)

    def col_attention(c):
        base = c * slots
        arrivals(1, c, lambda sender: rcv_m.at[c, sender])
        hs = n_seq // 2

        def mask_row(i):
            return mask_t[c, pl.ds(me * SLOT + i, 1), :]

        def prep(idx):
            ys = []
            for k in range(0, len(idx), 2):
                x2 = jnp.concatenate([rcv_m[c, q, i].astype(F32) for i in idx[k:k + 2] for q in range(n)], axis=0).T
                for t, i in enumerate(idx[k:k + 2]):
                    x = jnp.concatenate([x2[:c_m, t * hs:(t + 1) * hs], x2[c_m:, t * hs:(t + 1) * hs]], axis=1)
                    xw[base + i] = x
                    ys.append(layer_norm_t(x))
            keep(mm(wt_c[...], jnp.concatenate(ys, axis=1)), c_m, [base + i for i in idx], LANES,
                 [mask_row(i) for i in idx])
        grouped(res, 4, prep)

        def group(g):
            idx = [g * part_rows + t for t in range(part_rows)]
            logits(idx, base, heads_m, d_m, hm8, LANES, True)
            softmax(idx, heads_m, d_m, LANES, False)
            upd = mm(wt_co[...], jnp.concatenate(mixed(idx, base, heads_m, d_m, LANES), axis=1))
            new = [(xw[base + i] + upd[:, t * LANES:(t + 1) * LANES]).astype(BF16).astype(F32)
                   for t, i in enumerate(idx)]
            ac = mm(w_ac[...], jnp.concatenate([layer_norm_t(x) for x in new], axis=1)).astype(BF16).astype(F32)
            for t, i in enumerate(idx):
                part = ac[:, t * LANES:(t + 1) * LANES] * mask_row(i)
                ag_c[c, g, me, t] = part[o_w:].astype(BF16)
                abuf[c, pl.ds(pl.multiple_of(i * o_w, o_w), o_w), :] = part[:o_w].astype(BF16)
            k = c * pieces + g
            relay_own(k)

            @pl.when(k >= 2)
            def _():
                relay_near(k - 2)

            @pl.when(k >= 4)
            def _():
                relay_far(k - 4)

            for t in range(0, part_rows, 2):
                two = jnp.concatenate([
                    jnp.concatenate([x[:, :hs] for x in new[t:t + 2]], axis=1),
                    jnp.concatenate([x[:, hs:] for x in new[t:t + 2]], axis=1)], axis=0).T
                for u, i in enumerate(idx[t:t + 2]):
                    for q in range(n):
                        snd_b[c, q, i] = two[u * hs + q * half:u * hs + (q + 1) * half].astype(BF16)
        loop(pieces, group)
        rcv_b[c, me] = snd_b[c, me]

    loop(crops, col_attention)

    def outer_product(c):
        base = c * slots
        @pl.when(c == 0)
        def _():
            relay_far(n_blocks - 4)

        mloc = mask_t[c, pl.ds(pl.multiple_of(me * SLOT, SLOT), SLOT), :].astype(BF16)
        norm[...] = 1.0 / (mm(mloc, mask_n[c], NT) + OPM_EPS)
        pitch = n_res + 8

        for g in range(pieces):
            relay_done(c * pieces + g)

            def spread(p):
                for t in range(part_rows):
                    stg_c[pl.ds(p * res + g * part_rows + t, o_w, stride=pitch), :] = ag_c[c, g, p, t].astype(F32)
            loop(n, spread)

        @pl.when(c == 0)
        def _():
            relay_near(n_blocks - 2)

        def outer(fs):
            rows = [stg_c[pl.ds(pl.multiple_of(f * pitch, 8), n_res), :].astype(BF16) for f in fs]
            outs = [mm(abuf[c], stack(rows[k:k + 2]), NT) for k in range(0, len(fs), 2)]
            for k, f in enumerate(fs):
                out = outs[k // 2][:, (k % 2) * LANES:(k % 2 + 1) * LANES]
                for i in range(res):
                    obuf[i, pl.ds(pl.multiple_of(f * o_w, o_w), o_w), :] = (
                        out[i * o_w:(i + 1) * o_w] * norm[i:i + 1, :]).astype(BF16)
        grouped(o_w, 8, outer)

        @pl.when(c == 0)
        def _():
            relay_near(n_blocks - 1)
            relay_far(n_blocks - 3)

        start(swap_copies(3, c, snd_b, rcv_b))

        def update(idx):
            rhs = [jnp.concatenate([obuf[i] for i in idx[k:k + 2]], axis=1) for k in range(0, len(idx), 2)]
            upds = [mm(w_oo_t[...], r) for r in rhs]
            for k, i in enumerate(idx):
                upd = upds[k // 2][:, (k % 2) * LANES:(k % 2 + 1) * LANES].T
                zw[c, i] = (z_in[c, i].astype(F32) + upd[:n_res]).astype(BF16)
        grouped(res, 4, update)

        @pl.when(c == 0)
        def _():
            relay_far(n_blocks - 2)

        def prep(idx):
            y = stack([layer_norm(zw[c, i].astype(F32)) for i in idx])
            put_bias(y, 1, heads_z, idx)
            keep(mm(wt_s[...], y, NT), c_z, [base + i for i in idx], n_res)
        grouped(res, 6, prep)

        @pl.when(c == 0)
        def _():
            relay_far(n_blocks - 1)

        ag_s[c, me] = stg_b[:heads_z * res, :].astype(BF16)
        start(gather_copies(4, c, ag_s))

    loop(crops, outer_product)

    def res_bias(c):
        return column((res_r[pl.ds(c, 1), :] - 1.0) * (MASK_SCALE * d_z ** 0.5))

    def piece_copies(first, c, g, snd, rcv):
        return copies(first + g, c, lambda peer: snd.at[c, g, peer], rcv.at[c, g, me])

    def send_rows(zs, snd, c, g):
        for t, z in enumerate(zs):
            stg_m[pl.ds(t, n_res, stride=part_rows), :] = z
        size = res * part_rows
        for q in range(n):
            snd[c, g, q] = stg_m[q * size:(q + 1) * size, :].astype(BF16)

    def take_columns(first, c, rcv):
        for g in range(pieces):
            arrivals(first + g, c, lambda sender: rcv.at[c, g, sender])
        for p in range(n):
            for g in range(pieces):
                block = rcv[c, g, p].astype(F32)
                row0 = p * res + g * part_rows
                for j in range(res):
                    xs[j, row0:row0 + part_rows, :] = block[j * part_rows:(j + 1) * part_rows]

    def tri_start(c):
        base = c * slots
        gather_wait(4, c, ag_s)
        gathered_bias(ag_s, c, heads_z, d_z, True, res_bias(c))
        stg_b[...] = jnp.zeros(stg_b.shape, F32)

        def group(g):
            idx = [g * part_rows + t for t in range(part_rows)]
            logits(idx, base, heads_z, d_z, hm4, n_res, False)
            softmax(idx, heads_z, d_z, n_res, True)
            upds = [mm(o, w_so[...], TN) for o in mixed(idx, base, heads_z, d_z, n_res)]
            zs = [(zw[c, i].astype(F32) + upd[:n_res]).astype(BF16).astype(F32) for i, upd in zip(idx, upds)]
            send_rows(zs, snd_z, c, g)
            start(piece_copies(10, c, g, snd_z, rcv_z))
            rcv_z[c, g, me] = snd_z[c, g, me]
            put_bias(stack([layer_norm(z) for z in zs]), 2, heads_z, idx)
        loop(pieces, group)
        ag_e[c, me] = stg_b[:heads_z * res, :].astype(BF16)
        start(gather_copies(5, c, ag_e))

    loop(crops, tri_start)

    def tri_end(c):
        base = c * slots
        take_columns(10, c, rcv_z)

        def prep(idx):
            keep(mm(wt_e[...], stack([layer_norm(xs[j]) for j in idx]), NT), c_z, [base + j for j in idx], n_res)
        grouped(res, 6, prep)
        gather_wait(5, c, ag_e)
        gathered_bias(ag_e, c, heads_z, d_z, False, res_bias(c))

        def step(g):
            idx = [g * part_rows + t for t in range(part_rows)]
            logits(idx, base, heads_z, d_z, hm4, n_res, False)
            softmax(idx, heads_z, d_z, n_res, True)
            upds = [mm(o, w_eo[...], TN) for o in mixed(idx, base, heads_z, d_z, n_res)]
            send_rows([xs[j] + upd[:n_res] for j, upd in zip(idx, upds)], snd_y, c, g)
            start(piece_copies(7, c, g, snd_y, zback))
            zback[c, g, me] = snd_y[c, g, me]
        loop(pieces, step)

    loop(crops, tri_end)

    def put_m(c):
        arrivals(3, c, lambda sender: rcv_b.at[c, sender])
        stg_m[...] = rcv_b[c].astype(F32).reshape(n * res * half, LANES)

        def step(idx):
            for s in idx:
                x2 = stg_m[pl.ds(s, n_res, stride=half), :].T
                m_out[c, s] = x2[:c_m].astype(BF16)
                m_out[c, s + half] = x2[c_m:].astype(BF16)
        grouped(half, 4, step)

    loop(crops, put_m)

    def put_z(c):
        take_columns(7, c, zback)

        def step(i):
            z_out[c, i] = xs[i].astype(BF16)
        for i in range(res):
            step(i)

    loop(crops, put_z)

    def drain(c):
        finish(gather_copies(0, c, ag_r))
        finish(swap_copies(1, c, snd_m, rcv_m))
        for g in range(pieces):
            for slot in range(n - 1):
                block_copy(c * pieces + g, me, device(1), slot).wait_send()
            finish(piece_copies(7, c, g, snd_y, zback))
            finish(piece_copies(10, c, g, snd_z, rcv_z))
        finish(swap_copies(3, c, snd_b, rcv_b))
        finish(gather_copies(4, c, ag_s))
        finish(gather_copies(5, c, ag_e))

    loop(crops, drain)


def solution(mesh):
    n = mesh.shape[GROUP_AXIS]
    rows_spec = P(PART_AXIS, GROUP_AXIS, None, None)
    in_specs = (rows_spec, rows_spec, P(PART_AXIS, None, None), P(PART_AXIS, None)) + (P(),) * N_WEIGHTS

    def local_block(m, z, msa_mask, res_mask, w_rb, w_rq, w_ro, w_cq, w_co, w_ac, w_oo, w_sb, w_sq, w_so,
                    w_eb, w_eq, w_eo):
        crops, seqs, n_res, c_m = m.shape
        res, c_z = z.shape[1], z.shape[3]
        heads_m, heads_z = w_rq.shape[2], w_sq.shape[2]
        o_w = w_ac.shape[2]
        half = seqs // 2
        assert n == 8 and crops == 2 and res % 3 == 0 and n * SLOT == LANES and res <= SLOT and n * seqs == LANES and 2 * c_m == LANES and c_z == LANES
        flat = lambda w: jnp.moveaxis(w, 0, -1).reshape(-1, w.shape[0])
        tall = lambda w: w.reshape(-1, w.shape[-1])
        args = (m.swapaxes(2, 3), z, msa_mask.swapaxes(1, 2), res_mask, w_rb.T, flat(w_rq), tall(w_ro), flat(w_cq),
                tall(w_co), flat(w_ac), tall(w_oo), w_sb.T, flat(w_sq), tall(w_so), w_eb.T, flat(w_eq), tall(w_eo))
        vm = pltpu.VMEM
        slots = max(seqs, res)
        pieces = 3
        piece = res * res // pieces
        scratch = [
            vm((crops, n, heads_m * res, LANES), BF16),
            vm((crops, pieces, n, res // pieces, o_w, LANES), BF16),
            vm((crops, n, heads_z * res, LANES), BF16),
            vm((crops, n, heads_z * res, LANES), BF16),
            vm((crops, n, res, half, LANES), BF16),
            vm((crops, n, res, half, LANES), BF16),
            vm((crops, n, res, half, LANES), BF16),
            vm((crops, n, res, half, LANES), BF16),
            vm((crops, pieces, n, piece, LANES), BF16),
            vm((crops, pieces, n, piece, LANES), BF16),
            vm((crops, pieces, n, piece, LANES), BF16),
            vm((crops, pieces, n, piece, LANES), BF16),
            pltpu.SemaphoreType.DMA((13, crops, n)),
            pltpu.SemaphoreType.DMA((13, crops, n)),
            pltpu.SemaphoreType.DMA((crops * pieces, n)),
            pltpu.SemaphoreType.DMA((crops * pieces, n)),
        ]
        local = [
            vm((crops, res, n_res, LANES), BF16),
            vm((crops * slots, c_m, LANES), F32),
            vm((crops * slots, LANES, LANES), BF16),
            vm((crops * slots, LANES, LANES), BF16),
            vm((crops * slots, LANES, LANES), BF16),
            vm((crops * slots, LANES, LANES), F32),
            vm((heads_m, n_res, LANES), F32),
            vm((res, o_w * o_w, LANES), BF16),
            vm((n * res * half, LANES), F32),
            vm((o_w * (n_res + 8), LANES), F32),
            vm((heads_m * res, LANES), F32),
            vm((n_res * res, LANES), F32),
            vm((crops, res * o_w, LANES), BF16),
            vm((crops, LANES, LANES), F32),
            vm((crops, n * seqs, LANES), F32),
            vm((crops, LANES), F32),
            vm((slots, heads_m // 2, LANES, 2 * LANES), F32),
            vm((slots, heads_m // 2, LANES, 2 * LANES), BF16),
            vm((slots, heads_m, LANES), F32),
            vm((SLOT, LANES), F32),
            vm((heads_m, c_m, LANES), BF16),
            vm((heads_z, c_z, LANES), BF16),
            vm((c_m, c_m), BF16),
            vm((c_m, c_m), BF16),
            vm((LANES, o_w * o_w), BF16),
            vm((3, SLOT, LANES), BF16),
            vm((AUG, LANES), F32),
            vm((AUG, 2 * LANES), BF16),
            vm((res, n_res, LANES), F32),
            vm((crops, LANES, LANES), BF16),
        ]
        cfg = dict(n=n, heads_m=heads_m, heads_z=heads_z, slots=slots, pieces=pieces, local=local)
        spec = pl.BlockSpec(memory_space=pltpu.VMEM)
        m_new, z_new = pl.pallas_call(
            functools.partial(body, cfg),
            out_shape=(jax.ShapeDtypeStruct((crops, seqs, c_m, n_res), BF16), jax.ShapeDtypeStruct(z.shape, BF16)),
            in_specs=[spec] * len(args),
            out_specs=(spec, spec),
            scratch_shapes=scratch,
            compiler_params=pltpu.CompilerParams(collective_id=0, has_side_effects=True,
                                                 vmem_limit_bytes=60 * 1024 * 1024),
        )(*args)
        return m_new.swapaxes(2, 3), z_new

    return jax.shard_map(local_block, mesh=mesh, in_specs=in_specs, out_specs=(rows_spec, rows_spec),
                         check_vma=False)
```

```python
import functools
import math

import jax
import jax.numpy as jnp
import numpy as np
from jax import lax
from jax.experimental import pallas as pl
from jax.experimental.pallas import tpu as pltpu
from jax.sharding import PartitionSpec as P

MASK_SCALE = 10000.0
LN_EPS = 1e-5
OPM_EPS = 1e-3
N_WEIGHTS = 13
PART_AXIS = 'data'
GROUP_AXIS = 'dap'
LOG2E = math.log2(math.e)
AUG = 16
LANES = 128
SLOT = 16
F32 = jnp.float32
BF16 = jnp.bfloat16
NN = (((1,), (0,)), ((), ()))
NT = (((1,), (1,)), ((), ()))
TN = (((0,), (0,)), ((), ()))


def mm(lhs, rhs, dims=NN):
    return lax.dot_general(lhs, rhs, dims, preferred_element_type=F32)


def layer_norm(x_float):
    mean_val = jnp.mean(x_float, axis=-1, keepdims=True)
    centred = x_float - mean_val
    var_val = jnp.mean(centred * centred, axis=-1, keepdims=True)
    return (centred * lax.rsqrt(var_val + LN_EPS)).astype(BF16)


def layer_norm_t(x_float):
    mean_val = jnp.mean(x_float, axis=0, keepdims=True)
    centred = x_float - mean_val
    var_val = jnp.mean(centred * centred, axis=0, keepdims=True)
    return (centred * lax.rsqrt(var_val + LN_EPS)).astype(BF16)


def iota(shape, axis):
    return lax.broadcasted_iota(jnp.int32, shape, axis)


def body(cfg, *refs):
    pl.run_scoped(functools.partial(scoped_body, cfg, refs), *cfg['local'])


def scoped_body(cfg, refs, *local):
    n = cfg['n']
    (m_in, z_in, mask_in, res_in, w_rb, wt_r, w_ro, wt_c, w_co, w_ac, w_oo,
     w_sb, wt_s, w_so, w_eb, wt_e, w_eo, m_out, z_out,
     ag_r, ag_c, ag_s, ag_e, snd_m, rcv_m, snd_b, rcv_b, snd_z, rcv_z, snd_y, zback, send_sem, recv_sem,
     ring_send, ring_recv) = refs
    (zw, xw, kbuf, qbuf, vbuf, gbuf, bias, obuf, stg_m, stg_c, stg_b, stg_z, abuf,
     mask_t, mask_r, res_r, raw, prob, inv, norm, hm8, hm4, wt_ro, wt_co, w_oo_t, wt_b, aug, one_rows, xs, mask_n) = local
    crops, seqs, c_m, n_res = m_in.shape
    res = z_in.shape[1]
    c_z = z_in.shape[3]
    half = seqs // 2
    heads_m, heads_z = cfg['heads_m'], cfg['heads_z']
    d_m, d_z = c_m // heads_m, c_z // heads_z
    n_seq = n * seqs
    slots, pieces = cfg['slots'], cfg['pieces']
    part_rows, n_blocks = res // pieces, crops * pieces
    me = lax.axis_index(GROUP_AXIS)

    barrier = pltpu.get_barrier_semaphore()
    for r in range(1, n):
        pl.semaphore_signal(barrier, inc=1, device_id={GROUP_AXIS: lax.rem(me + r, n)},
                            device_id_type=pl.DeviceIdType.MESH)
    pl.semaphore_wait(barrier, n - 1)

    def copies(exch, c, src_of, dst):
        out = []
        for r in range(1, n):
            peer = lax.rem(me + r, n)
            out.append(pltpu.make_async_remote_copy(
                src_ref=src_of(peer), dst_ref=dst, send_sem=send_sem.at[exch, c, r], recv_sem=recv_sem.at[exch, c, r],
                device_id={GROUP_AXIS: peer}, device_id_type=pl.DeviceIdType.MESH))
        return out

    def arrivals(exch, c, slot_of):
        for r in range(1, n):
            sender = lax.rem(me + n - r, n)
            ref = slot_of(sender)
            pltpu.make_async_remote_copy(
                src_ref=ref, dst_ref=ref, send_sem=send_sem.at[exch, c, r], recv_sem=recv_sem.at[exch, c, r],
                device_id={GROUP_AXIS: sender}, device_id_type=pl.DeviceIdType.MESH).wait_recv()

    def gather_copies(exch, c, buf):
        return copies(exch, c, lambda peer: buf.at[c, me], buf.at[c, me])

    def gather_wait(exch, c, buf):
        arrivals(exch, c, lambda sender: buf.at[c, sender])

    def swap_copies(exch, c, snd, rcv):
        return copies(exch, c, lambda peer: snd.at[c, peer], rcv.at[c, me])

    chips, core, chip = n // 2, lax.rem(me, 2), me // 2
    ahead = 1 - 2 * core

    def device(offset, other=False):
        return lax.rem(chip + offset + chips, chips) * 2 + ((1 - core) if other else core)

    def block_copy(k, block, peer, slot):
        c, g = k // pieces, lax.rem(k, pieces)
        return pltpu.make_async_remote_copy(
            src_ref=ag_c.at[c, g, block], dst_ref=ag_c.at[c, g, block], send_sem=ring_send.at[k, slot],
            recv_sem=ring_recv.at[k, block], device_id={GROUP_AXIS: peer}, device_id_type=pl.DeviceIdType.MESH)

    def block_wait(k, block):
        block_copy(k, block, block, 0).wait_recv()

    def relay_own(k):
        for slot, peer in enumerate((device(1), device(-1), device(0, True))):
            block_copy(k, me, peer, slot).start()

    def relay_near(k):
        block_wait(k, device(-1))
        block_wait(k, device(1))
        block_copy(k, device(-ahead), device(ahead), 3).start()
        block_copy(k, device(-1), device(0, True), 4).start()
        block_copy(k, device(1), device(0, True), 5).start()

    def relay_far(k):
        block_wait(k, device(2))
        block_copy(k, device(2), device(0, True), 6).start()

    def relay_done(k):
        for offset in range(chips):
            block_wait(k, device(offset, True))

    def start(descs):
        for d in descs:
            d.start()

    def finish(descs):
        for d in descs:
            d.wait_send()

    def loop(count, fn):
        def step(i, carry):
            fn(i)
            return carry
        lax.fori_loop(0, count, step, 0)

    def pad_matrix():
        row, col = iota((LANES, n_res), 0), iota((LANES, n_res), 1)
        hit = (col == (row // SLOT) * res + row % SLOT) & (row % SLOT < res)
        return jnp.where(hit, 1.0, 0.0).astype(BF16)

    def head_rows(heads, width, ref):
        for h in range(heads):
            row = iota((heads * width, LANES), 0)
            ref[h] = jnp.where((row >= h * width) & (row < (h + 1) * width), 1.0, 0.0).astype(BF16)

    pad = pad_matrix()
    tail = jnp.where(iota((n_res, LANES), 0) == iota((n_res, LANES), 1), 1.0, 0.0).astype(BF16)
    head_rows(heads_m, d_m, hm8)
    head_rows(heads_z, d_z, hm4)
    row, col = iota((LANES, LANES), 0), iota((LANES, LANES), 1)
    seq_of = ((col % (n_seq // 2)) // half) * seqs + (col // (n_seq // 2)) * half + col % half
    seq_perm = jnp.where(row == seq_of, 1.0, 0.0).astype(BF16)
    for c in range(crops):
        mask_bf = mask_in[c].astype(F32).astype(BF16)
        mask_t[c] = mm(mm(pad, mask_bf).astype(BF16), seq_perm)
        mask_n[c, :n_res] = mm(mask_bf, seq_perm).astype(BF16)
        mask_n[c, n_res:] = jnp.zeros((LANES - n_res, LANES), BF16)
        mask_r[c] = mm(mask_bf, tail, TN)
    res_r[...] = mm(res_in[...].astype(F32).astype(BF16), tail)
    term = MASK_SCALE * d_m ** 0.5
    aug[...] = jnp.zeros(aug.shape, F32)
    ones = jnp.zeros((AUG, 2 * LANES), F32)
    for k in range(3):
        piece = float(np.array(term, dtype=BF16))
        term = term - piece
        aug[k:k + 1, :] = jnp.full((1, LANES), piece, F32)
        ones = jnp.where(iota(ones.shape, 0) == k, 1.0, ones)
    one_rows[...] = ones.astype(BF16)
    for k, w in enumerate((w_rb, w_sb, w_eb)):
        wt_b[k] = jnp.zeros(wt_b.shape[1:], BF16)
        wt_b[k, :w.shape[0], :] = w[...]
    wt_ro[...] = w_ro[...].astype(F32).T.astype(BF16)
    wt_co[...] = w_co[...].astype(F32).T.astype(BF16)
    o_w = w_ac.shape[0] // 2
    stg_z[:o_w * o_w, :] = w_oo[...].astype(F32)
    for k in range(0, o_w, LANES // o_w):
        rows = [stg_z[pl.ds(f, o_w, stride=o_w), :] for f in range(k, k + LANES // o_w)]
        w_oo_t[:, k * o_w:k * o_w + LANES] = jnp.concatenate(rows, axis=0).T.astype(BF16)

    stg_b[...] = jnp.zeros(stg_b.shape, F32)

    def grouped(count, size, fn):
        while count % size:
            size -= 1

        def step(b, carry):
            fn([b * size + t for t in range(size)])
            return carry
        lax.fori_loop(0, count // size, step, 0)

    def put_bias(y, k, heads, rows):
        b = mm(wt_b[k], y, NT)
        for t, i in enumerate(rows):
            for h in range(heads):
                stg_b[pl.ds(h * res + i, 1), :] = b[h:h + 1, t * LANES:(t + 1) * LANES]

    def stack(ys):
        fill = jnp.zeros((LANES - n_res, ys[0].shape[1]), BF16)
        return jnp.concatenate([part for y in ys for part in (y, fill)], axis=0)

    def keep(p, width, slots, length, mask_rows=None):
        for t, slot in enumerate(slots):
            part = slice(t * LANES, (t + 1) * LANES)
            keys = p[width:2 * width, part]
            if mask_rows is not None:
                keys = jnp.concatenate([keys, (mask_rows[t] - 1.0) * aug[...]], axis=0)
            qbuf[slot, :width] = p[:width, part].astype(BF16)
            kbuf[slot, :length, :keys.shape[0]] = keys.T[:length].astype(BF16)
            vbuf[slot, :width] = p[2 * width:3 * width, part].astype(BF16)
            gbuf[slot, :width] = jax.nn.sigmoid(p[3 * width:, part])

    def column(rowvec):
        return jnp.broadcast_to(rowvec, (LANES, LANES)).T[:n_res]

    def gathered_bias(buf, c, heads, width, flip, add):
        parts = [buf[c, p].astype(F32) for p in range(n)]
        for h in range(heads):
            b = jnp.concatenate([part[h * res:(h + 1) * res] for part in parts], axis=0)
            if flip:
                b = jnp.concatenate([b, jnp.zeros((LANES - n_res, LANES), F32)], axis=0).T[:n_res]
            b = b * width ** 0.5
            bias[h] = b if add is None else b + add

    def logits(idx, base, heads, width, head_mask, length, masked):
        c = heads * width
        for i in idx:
            q_t, keys = qbuf[base + i, :c], kbuf[base + i, :length, :c + (AUG if masked else 0)]
            for pair in range(heads // 2):
                rhs = jnp.concatenate([q_t * head_mask[2 * pair], q_t * head_mask[2 * pair + 1]], axis=1)
                if masked:
                    rhs = jnp.concatenate([rhs, one_rows[...]], axis=0)
                raw[i, pair, :length] = mm(keys, rhs)

    def softmax(idx, heads, width, length, biased):
        scale2 = LOG2E * width ** -0.5
        for i in idx:
            for h in range(heads):
                part = slice((h % 2) * LANES, (h % 2 + 1) * LANES)
                x = raw[i, h // 2, :length, part]
                if biased:
                    x = x + bias[h]
                e = jnp.exp2((x - jnp.max(x, axis=0, keepdims=True)) * scale2)
                inv[i, h:h + 1, :] = 1.0 / jnp.sum(e, axis=0, keepdims=True)
                prob[i, h // 2, :length, part] = e.astype(BF16)

    def mixed(idx, base, heads, width, length):
        c = heads * width
        raws = [[mm(vbuf[base + i, 2 * p * width:2 * (p + 1) * width, :length], prob[i, p, :length])
                 for p in range(heads // 2)] for i in idx]
        outs = []
        for i, r in zip(idx, raws):
            parts = []
            for p in range(heads // 2):
                parts.append(r[p][:width, :LANES] * inv[i, 2 * p:2 * p + 1, :])
                parts.append(r[p][width:, LANES:] * inv[i, 2 * p + 1:2 * p + 2, :])
            outs.append((jnp.concatenate(parts, axis=0) * gbuf[base + i, :c]).astype(BF16))
        return outs

    def row_bias(c):
        def step(idx):
            put_bias(stack([layer_norm(z_in[c, i].astype(F32)) for i in idx]), 0, heads_m, idx)
        grouped(res, 6, step)
        ag_r[c, me] = stg_b[...].astype(BF16)
        start(gather_copies(0, c, ag_r))

    loop(crops, row_bias)

    def row_prep(c):
        def prep(idx):
            fill = jnp.zeros((c_m, LANES - n_res), F32)
            ms = [jnp.concatenate([m_in[c, s].astype(F32), fill], axis=1) for s in idx]
            keep(mm(wt_r[...], jnp.concatenate([layer_norm_t(x) for x in ms], axis=1)), c_m,
                 [c * slots + s for s in idx], n_res, [mask_r[c, pl.ds(me * seqs + s, 1), :] for s in idx])
            for s, x in zip(idx, ms):
                xw[c * slots + s] = x
        grouped(seqs, 4, prep)

    loop(crops, row_prep)

    def row_attention(c):
        base = c * slots
        grouped(seqs, 4, lambda idx: logits(idx, base, heads_m, d_m, hm8, n_res, True))
        gather_wait(0, c, ag_r)
        gathered_bias(ag_r, c, heads_m, d_m, True, None)
        grouped(seqs, 2, lambda idx: softmax(idx, heads_m, d_m, n_res, True))

        def step(idx):
            both = [s + t * half for s in idx for t in range(2)]
            upd = mm(wt_ro[...], jnp.concatenate(mixed(both, base, heads_m, d_m, n_res), axis=1))
            new = [xw[base + s] + upd[:, t * LANES:(t + 1) * LANES] for t, s in enumerate(both)]
            for k, s in enumerate(idx):
                x2 = jnp.concatenate(new[2 * k:2 * k + 2], axis=0).T
                stg_m[pl.ds(s, n_res, stride=half), :] = x2[:n_res]
        grouped(half, 4, step)
        for p in range(n):
            snd_m[c, p] = stg_m[p * res * half:(p + 1) * res * half, :].reshape(res, half, LANES).astype(BF16)
        rcv_m[c, me] = snd_m[c, me]
        start(swap_copies(1, c, snd_m, rcv_m))

    loop(crops, row_attention)

    def col_attention(c):
        base = c * slots
        arrivals(1, c, lambda sender: rcv_m.at[c, sender])
        hs = n_seq // 2

        def mask_row(i):
            return mask_t[c, pl.ds(me * SLOT + i, 1), :]

        def prep(idx):
            ys = []
            for k in range(0, len(idx), 2):
                x2 = jnp.concatenate([rcv_m[c, q, i].astype(F32) for i in idx[k:k + 2] for q in range(n)], axis=0).T
                for t, i in enumerate(idx[k:k + 2]):
                    x = jnp.concatenate([x2[:c_m, t * hs:(t + 1) * hs], x2[c_m:, t * hs:(t + 1) * hs]], axis=1)
                    xw[base + i] = x
                    ys.append(layer_norm_t(x))
            keep(mm(wt_c[...], jnp.concatenate(ys, axis=1)), c_m, [base + i for i in idx], LANES,
                 [mask_row(i) for i in idx])
        grouped(res, 4, prep)

        def group(g):
            idx = [g * part_rows + t for t in range(part_rows)]
            logits(idx, base, heads_m, d_m, hm8, LANES, True)
            softmax(idx, heads_m, d_m, LANES, False)
            upd = mm(wt_co[...], jnp.concatenate(mixed(idx, base, heads_m, d_m, LANES), axis=1))
            new = [(xw[base + i] + upd[:, t * LANES:(t + 1) * LANES]).astype(BF16).astype(F32)
                   for t, i in enumerate(idx)]
            ac = mm(w_ac[...], jnp.concatenate([layer_norm_t(x) for x in new], axis=1)).astype(BF16).astype(F32)
            for t, i in enumerate(idx):
                part = ac[:, t * LANES:(t + 1) * LANES] * mask_row(i)
                ag_c[c, g, me, t] = part[o_w:].astype(BF16)
                abuf[c, pl.ds(pl.multiple_of(i * o_w, o_w), o_w), :] = part[:o_w].astype(BF16)
            k = c * pieces + g
            relay_own(k)

            @pl.when(k >= 1)
            def _():
                relay_near(k - 1)

            @pl.when(k >= 2)
            def _():
                relay_far(k - 2)

            for t in range(0, part_rows, 2):
                two = jnp.concatenate([
                    jnp.concatenate([x[:, :hs] for x in new[t:t + 2]], axis=1),
                    jnp.concatenate([x[:, hs:] for x in new[t:t + 2]], axis=1)], axis=0).T
                for u, i in enumerate(idx[t:t + 2]):
                    for q in range(n):
                        snd_b[c, q, i] = two[u * hs + q * half:u * hs + (q + 1) * half].astype(BF16)
        loop(pieces, group)
        rcv_b[c, me] = snd_b[c, me]

    loop(crops, col_attention)

    def outer_product(c):
        base = c * slots
        mloc = mask_t[c, pl.ds(pl.multiple_of(me * SLOT, SLOT), SLOT), :].astype(BF16)
        norm[...] = 1.0 / (mm(mloc, mask_n[c], NT) + OPM_EPS)
        pitch = n_res + 8

        for g in range(pieces):
            relay_done(c * pieces + g)

            def spread(p):
                for t in range(part_rows):
                    stg_c[pl.ds(p * res + g * part_rows + t, o_w, stride=pitch), :] = ag_c[c, g, p, t].astype(F32)
            loop(n, spread)

        @pl.when(c == 0)
        def _():
            relay_near(n_blocks - 1)

        def outer(fs):
            rows = [stg_c[pl.ds(pl.multiple_of(f * pitch, 8), n_res), :].astype(BF16) for f in fs]
            outs = [mm(abuf[c], stack(rows[k:k + 2]), NT) for k in range(0, len(fs), 2)]
            for k, f in enumerate(fs):
                out = outs[k // 2][:, (k % 2) * LANES:(k % 2 + 1) * LANES]
                for i in range(res):
                    obuf[i, pl.ds(pl.multiple_of(f * o_w, o_w), o_w), :] = (
                        out[i * o_w:(i + 1) * o_w] * norm[i:i + 1, :]).astype(BF16)
        grouped(o_w, 8, outer)

        @pl.when(c == 0)
        def _():
            relay_far(n_blocks - 2)

        start(swap_copies(3, c, snd_b, rcv_b))

        def update(idx):
            rhs = [jnp.concatenate([obuf[i] for i in idx[k:k + 2]], axis=1) for k in range(0, len(idx), 2)]
            upds = [mm(w_oo_t[...], r) for r in rhs]
            for k, i in enumerate(idx):
                upd = upds[k // 2][:, (k % 2) * LANES:(k % 2 + 1) * LANES].T
                zw[c, i] = (z_in[c, i].astype(F32) + upd[:n_res]).astype(BF16)
        grouped(res, 4, update)

        @pl.when(c == 0)
        def _():
            relay_far(n_blocks - 1)

        def prep(idx):
            y = stack([layer_norm(zw[c, i].astype(F32)) for i in idx])
            put_bias(y, 1, heads_z, idx)
            keep(mm(wt_s[...], y, NT), c_z, [base + i for i in idx], n_res)
        grouped(res, 6, prep)
        ag_s[c, me] = stg_b[:heads_z * res, :].astype(BF16)
        start(gather_copies(4, c, ag_s))

    loop(crops, outer_product)

    def res_bias(c):
        return column((res_r[pl.ds(c, 1), :] - 1.0) * (MASK_SCALE * d_z ** 0.5))

    def piece_copies(first, c, g, snd, rcv):
        return copies(first + g, c, lambda peer: snd.at[c, g, peer], rcv.at[c, g, me])

    def send_rows(zs, snd, c, g):
        for t, z in enumerate(zs):
            stg_m[pl.ds(t, n_res, stride=part_rows), :] = z
        size = res * part_rows
        for q in range(n):
            snd[c, g, q] = stg_m[q * size:(q + 1) * size, :].astype(BF16)

    def take_columns(first, c, rcv):
        for g in range(pieces):
            arrivals(first + g, c, lambda sender: rcv.at[c, g, sender])
        for p in range(n):
            for g in range(pieces):
                block = rcv[c, g, p].astype(F32)
                row0 = p * res + g * part_rows
                for j in range(res):
                    xs[j, row0:row0 + part_rows, :] = block[j * part_rows:(j + 1) * part_rows]

    def tri_start(c):
        base = c * slots
        gather_wait(4, c, ag_s)
        gathered_bias(ag_s, c, heads_z, d_z, True, res_bias(c))
        stg_b[...] = jnp.zeros(stg_b.shape, F32)

        def group(g):
            idx = [g * part_rows + t for t in range(part_rows)]
            logits(idx, base, heads_z, d_z, hm4, n_res, False)
            softmax(idx, heads_z, d_z, n_res, True)
            upds = [mm(o, w_so[...], TN) for o in mixed(idx, base, heads_z, d_z, n_res)]
            zs = [(zw[c, i].astype(F32) + upd[:n_res]).astype(BF16).astype(F32) for i, upd in zip(idx, upds)]
            send_rows(zs, snd_z, c, g)
            start(piece_copies(10, c, g, snd_z, rcv_z))
            rcv_z[c, g, me] = snd_z[c, g, me]
            put_bias(stack([layer_norm(z) for z in zs]), 2, heads_z, idx)
        loop(pieces, group)
        ag_e[c, me] = stg_b[:heads_z * res, :].astype(BF16)
        start(gather_copies(5, c, ag_e))

    loop(crops, tri_start)

    def tri_end(c):
        base = c * slots
        take_columns(10, c, rcv_z)

        def prep(idx):
            keep(mm(wt_e[...], stack([layer_norm(xs[j]) for j in idx]), NT), c_z, [base + j for j in idx], n_res)
        grouped(res, 6, prep)
        gather_wait(5, c, ag_e)
        gathered_bias(ag_e, c, heads_z, d_z, False, res_bias(c))

        def step(g):
            idx = [g * part_rows + t for t in range(part_rows)]
            logits(idx, base, heads_z, d_z, hm4, n_res, False)
            softmax(idx, heads_z, d_z, n_res, True)
            upds = [mm(o, w_eo[...], TN) for o in mixed(idx, base, heads_z, d_z, n_res)]
            send_rows([xs[j] + upd[:n_res] for j, upd in zip(idx, upds)], snd_y, c, g)
            start(piece_copies(7, c, g, snd_y, zback))
            zback[c, g, me] = snd_y[c, g, me]
        loop(pieces, step)

    loop(crops, tri_end)

    def put_m(c):
        arrivals(3, c, lambda sender: rcv_b.at[c, sender])
        stg_m[...] = rcv_b[c].astype(F32).reshape(n * res * half, LANES)

        def step(idx):
            for s in idx:
                x2 = stg_m[pl.ds(s, n_res, stride=half), :].T
                m_out[c, s] = x2[:c_m].astype(BF16)
                m_out[c, s + half] = x2[c_m:].astype(BF16)
        grouped(half, 4, step)

    loop(crops, put_m)

    def put_z(c):
        take_columns(7, c, zback)

        def step(i):
            z_out[c, i] = xs[i].astype(BF16)
        for i in range(res):
            step(i)

    loop(crops, put_z)

    def drain(c):
        finish(gather_copies(0, c, ag_r))
        finish(swap_copies(1, c, snd_m, rcv_m))
        for g in range(pieces):
            for slot in range(n - 1):
                block_copy(c * pieces + g, me, device(1), slot).wait_send()
            finish(piece_copies(7, c, g, snd_y, zback))
            finish(piece_copies(10, c, g, snd_z, rcv_z))
        finish(swap_copies(3, c, snd_b, rcv_b))
        finish(gather_copies(4, c, ag_s))
        finish(gather_copies(5, c, ag_e))

    loop(crops, drain)


def solution(mesh):
    n = mesh.shape[GROUP_AXIS]
    rows_spec = P(PART_AXIS, GROUP_AXIS, None, None)
    in_specs = (rows_spec, rows_spec, P(PART_AXIS, None, None), P(PART_AXIS, None)) + (P(),) * N_WEIGHTS

    def local_block(m, z, msa_mask, res_mask, w_rb, w_rq, w_ro, w_cq, w_co, w_ac, w_oo, w_sb, w_sq, w_so,
                    w_eb, w_eq, w_eo):
        crops, seqs, n_res, c_m = m.shape
        res, c_z = z.shape[1], z.shape[3]
        heads_m, heads_z = w_rq.shape[2], w_sq.shape[2]
        o_w = w_ac.shape[2]
        half = seqs // 2
        assert n == 8 and crops == 2 and res % 3 == 0 and n * SLOT == LANES and res <= SLOT and n * seqs == LANES and 2 * c_m == LANES and c_z == LANES
        flat = lambda w: jnp.moveaxis(w, 0, -1).reshape(-1, w.shape[0])
        tall = lambda w: w.reshape(-1, w.shape[-1])
        args = (m.swapaxes(2, 3), z, msa_mask.swapaxes(1, 2), res_mask, w_rb.T, flat(w_rq), tall(w_ro), flat(w_cq),
                tall(w_co), flat(w_ac), tall(w_oo), w_sb.T, flat(w_sq), tall(w_so), w_eb.T, flat(w_eq), tall(w_eo))
        vm = pltpu.VMEM
        slots = max(seqs, res)
        pieces = 2
        piece = res * res // pieces
        scratch = [
            vm((crops, n, heads_m * res, LANES), BF16),
            vm((crops, pieces, n, res // pieces, o_w, LANES), BF16),
            vm((crops, n, heads_z * res, LANES), BF16),
            vm((crops, n, heads_z * res, LANES), BF16),
            vm((crops, n, res, half, LANES), BF16),
            vm((crops, n, res, half, LANES), BF16),
            vm((crops, n, res, half, LANES), BF16),
            vm((crops, n, res, half, LANES), BF16),
            vm((crops, pieces, n, piece, LANES), BF16),
            vm((crops, pieces, n, piece, LANES), BF16),
            vm((crops, pieces, n, piece, LANES), BF16),
            vm((crops, pieces, n, piece, LANES), BF16),
            pltpu.SemaphoreType.DMA((13, crops, n)),
            pltpu.SemaphoreType.DMA((13, crops, n)),
            pltpu.SemaphoreType.DMA((crops * pieces, n)),
            pltpu.SemaphoreType.DMA((crops * pieces, n)),
        ]
        local = [
            vm((crops, res, n_res, LANES), BF16),
            vm((crops * slots, c_m, LANES), F32),
            vm((crops * slots, LANES, LANES), BF16),
            vm((crops * slots, LANES, LANES), BF16),
            vm((crops * slots, LANES, LANES), BF16),
            vm((crops * slots, LANES, LANES), F32),
            vm((heads_m, n_res, LANES), F32),
            vm((res, o_w * o_w, LANES), BF16),
            vm((n * res * half, LANES), F32),
            vm((o_w * (n_res + 8), LANES), F32),
            vm((heads_m * res, LANES), F32),
            vm((n_res * res, LANES), F32),
            vm((crops, res * o_w, LANES), BF16),
            vm((crops, LANES, LANES), F32),
            vm((crops, n * seqs, LANES), F32),
            vm((crops, LANES), F32),
            vm((slots, heads_m // 2, LANES, 2 * LANES), F32),
            vm((slots, heads_m // 2, LANES, 2 * LANES), BF16),
            vm((slots, heads_m, LANES), F32),
            vm((SLOT, LANES), F32),
            vm((heads_m, c_m, LANES), BF16),
            vm((heads_z, c_z, LANES), BF16),
            vm((c_m, c_m), BF16),
            vm((c_m, c_m), BF16),
            vm((LANES, o_w * o_w), BF16),
            vm((3, SLOT, LANES), BF16),
            vm((AUG, LANES), F32),
            vm((AUG, 2 * LANES), BF16),
            vm((res, n_res, LANES), F32),
            vm((crops, LANES, LANES), BF16),
        ]
        cfg = dict(n=n, heads_m=heads_m, heads_z=heads_z, slots=slots, pieces=pieces, local=local)
        spec = pl.BlockSpec(memory_space=pltpu.VMEM)
        m_new, z_new = pl.pallas_call(
            functools.partial(body, cfg),
            out_shape=(jax.ShapeDtypeStruct((crops, seqs, c_m, n_res), BF16), jax.ShapeDtypeStruct(z.shape, BF16)),
            in_specs=[spec] * len(args),
            out_specs=(spec, spec),
            scratch_shapes=scratch,
            compiler_params=pltpu.CompilerParams(collective_id=0, has_side_effects=True,
                                                 vmem_limit_bytes=60 * 1024 * 1024),
        )(*args)
        return m_new.swapaxes(2, 3), z_new

    return jax.shard_map(local_block, mesh=mesh, in_specs=in_specs, out_specs=(rows_spec, rows_spec),
                         check_vma=False)
```

```python
import functools
import math

import jax
import jax.numpy as jnp
import numpy as np
from jax import lax
from jax.experimental import pallas as pl
from jax.experimental.pallas import tpu as pltpu
from jax.sharding import PartitionSpec as P

MASK_SCALE = 10000.0
LN_EPS = 1e-5
OPM_EPS = 1e-3
N_WEIGHTS = 13
PART_AXIS = 'data'
GROUP_AXIS = 'dap'
LOG2E = math.log2(math.e)
AUG = 16
LANES = 128
SLOT = 16
F32 = jnp.float32
BF16 = jnp.bfloat16
NN = (((1,), (0,)), ((), ()))
NT = (((1,), (1,)), ((), ()))
TN = (((0,), (0,)), ((), ()))


def mm(lhs, rhs, dims=NN):
    return lax.dot_general(lhs, rhs, dims, preferred_element_type=F32)


def layer_norm(x_float):
    mean_val = jnp.mean(x_float, axis=-1, keepdims=True)
    centred = x_float - mean_val
    var_val = jnp.mean(centred * centred, axis=-1, keepdims=True)
    return (centred * lax.rsqrt(var_val + LN_EPS)).astype(BF16)


def layer_norm_t(x_float):
    mean_val = jnp.mean(x_float, axis=0, keepdims=True)
    centred = x_float - mean_val
    var_val = jnp.mean(centred * centred, axis=0, keepdims=True)
    return (centred * lax.rsqrt(var_val + LN_EPS)).astype(BF16)


def iota(shape, axis):
    return lax.broadcasted_iota(jnp.int32, shape, axis)


def body(cfg, *refs):
    pl.run_scoped(functools.partial(scoped_body, cfg, refs), *cfg['local'])


def scoped_body(cfg, refs, *local):
    n = cfg['n']
    (m_in, z_in, mask_in, res_in, w_rb, wt_r, w_ro, wt_c, w_co, w_ac, w_oo,
     w_sb, wt_s, w_so, w_eb, wt_e, w_eo, m_out, z_out,
     ag_r, ag_c, ag_s, ag_e, snd_m, rcv_m, snd_b, rcv_b, snd_z, rcv_z, snd_y, zback, send_sem, recv_sem,
     ring_send, ring_recv) = refs
    (zw, xw, kbuf, qbuf, vbuf, gbuf, bias, obuf, stg_m, stg_c, stg_b, stg_z, abuf,
     mask_t, mask_r, res_r, raw, prob, inv, norm, hm8, hm4, wt_ro, wt_co, w_oo_t, wt_b, aug, one_rows, xs, mask_n) = local
    crops, seqs, c_m, n_res = m_in.shape
    res = z_in.shape[1]
    c_z = z_in.shape[3]
    half = seqs // 2
    heads_m, heads_z = cfg['heads_m'], cfg['heads_z']
    d_m, d_z = c_m // heads_m, c_z // heads_z
    n_seq = n * seqs
    slots, pieces = cfg['slots'], cfg['pieces']
    part_rows, n_blocks = res // pieces, crops * pieces
    me = lax.axis_index(GROUP_AXIS)

    barrier = pltpu.get_barrier_semaphore()
    for r in range(1, n):
        pl.semaphore_signal(barrier, inc=1, device_id={GROUP_AXIS: lax.rem(me + r, n)},
                            device_id_type=pl.DeviceIdType.MESH)
    pl.semaphore_wait(barrier, n - 1)

    def copies(exch, c, src_of, dst):
        out = []
        for r in range(1, n):
            peer = lax.rem(me + r, n)
            out.append(pltpu.make_async_remote_copy(
                src_ref=src_of(peer), dst_ref=dst, send_sem=send_sem.at[exch, c, r], recv_sem=recv_sem.at[exch, c, r],
                device_id={GROUP_AXIS: peer}, device_id_type=pl.DeviceIdType.MESH))
        return out

    def arrivals(exch, c, slot_of):
        for r in range(1, n):
            sender = lax.rem(me + n - r, n)
            ref = slot_of(sender)
            pltpu.make_async_remote_copy(
                src_ref=ref, dst_ref=ref, send_sem=send_sem.at[exch, c, r], recv_sem=recv_sem.at[exch, c, r],
                device_id={GROUP_AXIS: sender}, device_id_type=pl.DeviceIdType.MESH).wait_recv()

    def gather_copies(exch, c, buf):
        return copies(exch, c, lambda peer: buf.at[c, me], buf.at[c, me])

    def gather_wait(exch, c, buf):
        arrivals(exch, c, lambda sender: buf.at[c, sender])

    def swap_copies(exch, c, snd, rcv):
        return copies(exch, c, lambda peer: snd.at[c, peer], rcv.at[c, me])

    chips, core, chip = n // 2, lax.rem(me, 2), me // 2

    def device(offset, other=False):
        return lax.rem(chip + offset + chips, chips) * 2 + ((1 - core) if other else core)

    def block_copy(k, block, peer, slot):
        c, g = k // pieces, lax.rem(k, pieces)
        return pltpu.make_async_remote_copy(
            src_ref=ag_c.at[c, g, block], dst_ref=ag_c.at[c, g, block], send_sem=ring_send.at[k, slot],
            recv_sem=ring_recv.at[k, block], device_id={GROUP_AXIS: peer}, device_id_type=pl.DeviceIdType.MESH)

    def block_wait(k, block):
        block_copy(k, block, block, 0).wait_recv()

    def relay_own(k):
        for slot in range(chips):
            block_copy(k, me, device(slot, slot == 0), slot).start()

    def relay(k):
        for offset in range(1, chips):
            block_wait(k, device(offset))
        for offset in range(1, chips):
            block_copy(k, device(offset), device(0, True), chips - 1 + offset).start()

    def relay_done(k):
        for offset in range(chips):
            block_wait(k, device(offset, True))

    def start(descs):
        for d in descs:
            d.start()

    def finish(descs):
        for d in descs:
            d.wait_send()

    def loop(count, fn):
        def step(i, carry):
            fn(i)
            return carry
        lax.fori_loop(0, count, step, 0)

    def pad_matrix():
        row, col = iota((LANES, n_res), 0), iota((LANES, n_res), 1)
        hit = (col == (row // SLOT) * res + row % SLOT) & (row % SLOT < res)
        return jnp.where(hit, 1.0, 0.0).astype(BF16)

    def head_rows(heads, width, ref):
        for h in range(heads):
            row = iota((heads * width, LANES), 0)
            ref[h] = jnp.where((row >= h * width) & (row < (h + 1) * width), 1.0, 0.0).astype(BF16)

    pad = pad_matrix()
    tail = jnp.where(iota((n_res, LANES), 0) == iota((n_res, LANES), 1), 1.0, 0.0).astype(BF16)
    head_rows(heads_m, d_m, hm8)
    head_rows(heads_z, d_z, hm4)
    row, col = iota((LANES, LANES), 0), iota((LANES, LANES), 1)
    seq_of = ((col % (n_seq // 2)) // half) * seqs + (col // (n_seq // 2)) * half + col % half
    seq_perm = jnp.where(row == seq_of, 1.0, 0.0).astype(BF16)
    for c in range(crops):
        mask_bf = mask_in[c].astype(F32).astype(BF16)
        mask_t[c] = mm(mm(pad, mask_bf).astype(BF16), seq_perm)
        mask_n[c, :n_res] = mm(mask_bf, seq_perm).astype(BF16)
        mask_n[c, n_res:] = jnp.zeros((LANES - n_res, LANES), BF16)
        mask_r[c] = mm(mask_bf, tail, TN)
    res_r[...] = mm(res_in[...].astype(F32).astype(BF16), tail)
    term = MASK_SCALE * d_m ** 0.5
    aug[...] = jnp.zeros(aug.shape, F32)
    ones = jnp.zeros((AUG, 2 * LANES), F32)
    for k in range(3):
        piece = float(np.array(term, dtype=BF16))
        term = term - piece
        aug[k:k + 1, :] = jnp.full((1, LANES), piece, F32)
        ones = jnp.where(iota(ones.shape, 0) == k, 1.0, ones)
    one_rows[...] = ones.astype(BF16)
    for k, w in enumerate((w_rb, w_sb, w_eb)):
        wt_b[k] = jnp.zeros(wt_b.shape[1:], BF16)
        wt_b[k, :w.shape[0], :] = w[...]
    wt_ro[...] = w_ro[...].astype(F32).T.astype(BF16)
    wt_co[...] = w_co[...].astype(F32).T.astype(BF16)
    o_w = w_ac.shape[0] // 2
    stg_z[:o_w * o_w, :] = w_oo[...].astype(F32)
    for k in range(0, o_w, LANES // o_w):
        rows = [stg_z[pl.ds(f, o_w, stride=o_w), :] for f in range(k, k + LANES // o_w)]
        w_oo_t[:, k * o_w:k * o_w + LANES] = jnp.concatenate(rows, axis=0).T.astype(BF16)

    stg_b[...] = jnp.zeros(stg_b.shape, F32)

    def grouped(count, size, fn):
        while count % size:
            size -= 1

        def step(b, carry):
            fn([b * size + t for t in range(size)])
            return carry
        lax.fori_loop(0, count // size, step, 0)

    def put_bias(y, k, heads, rows):
        b = mm(wt_b[k], y, NT)
        for t, i in enumerate(rows):
            for h in range(heads):
                stg_b[pl.ds(h * res + i, 1), :] = b[h:h + 1, t * LANES:(t + 1) * LANES]

    def stack(ys):
        fill = jnp.zeros((LANES - n_res, ys[0].shape[1]), BF16)
        return jnp.concatenate([part for y in ys for part in (y, fill)], axis=0)

    def keep(p, width, slots, length, mask_rows=None):
        for t, slot in enumerate(slots):
            part = slice(t * LANES, (t + 1) * LANES)
            keys = p[width:2 * width, part]
            if mask_rows is not None:
                keys = jnp.concatenate([keys, (mask_rows[t] - 1.0) * aug[...]], axis=0)
            qbuf[slot, :width] = p[:width, part].astype(BF16)
            kbuf[slot, :length, :keys.shape[0]] = keys.T[:length].astype(BF16)
            vbuf[slot, :width] = p[2 * width:3 * width, part].astype(BF16)
            gbuf[slot, :width] = jax.nn.sigmoid(p[3 * width:, part])

    def column(rowvec):
        return jnp.broadcast_to(rowvec, (LANES, LANES)).T[:n_res]

    def gathered_bias(buf, c, heads, width, flip, add):
        parts = [buf[c, p].astype(F32) for p in range(n)]
        for h in range(heads):
            b = jnp.concatenate([part[h * res:(h + 1) * res] for part in parts], axis=0)
            if flip:
                b = jnp.concatenate([b, jnp.zeros((LANES - n_res, LANES), F32)], axis=0).T[:n_res]
            b = b * width ** 0.5
            bias[h] = b if add is None else b + add

    def logits(idx, base, heads, width, head_mask, length, masked):
        c = heads * width
        for i in idx:
            q_t, keys = qbuf[base + i, :c], kbuf[base + i, :length, :c + (AUG if masked else 0)]
            for pair in range(heads // 2):
                rhs = jnp.concatenate([q_t * head_mask[2 * pair], q_t * head_mask[2 * pair + 1]], axis=1)
                if masked:
                    rhs = jnp.concatenate([rhs, one_rows[...]], axis=0)
                raw[i, pair, :length] = mm(keys, rhs)

    def softmax(idx, heads, width, length, biased):
        scale2 = LOG2E * width ** -0.5
        for i in idx:
            for h in range(heads):
                part = slice((h % 2) * LANES, (h % 2 + 1) * LANES)
                x = raw[i, h // 2, :length, part]
                if biased:
                    x = x + bias[h]
                e = jnp.exp2((x - jnp.max(x, axis=0, keepdims=True)) * scale2)
                inv[i, h:h + 1, :] = 1.0 / jnp.sum(e, axis=0, keepdims=True)
                prob[i, h // 2, :length, part] = e.astype(BF16)

    def mixed(idx, base, heads, width, length):
        c = heads * width
        raws = [[mm(vbuf[base + i, 2 * p * width:2 * (p + 1) * width, :length], prob[i, p, :length])
                 for p in range(heads // 2)] for i in idx]
        outs = []
        for i, r in zip(idx, raws):
            parts = []
            for p in range(heads // 2):
                parts.append(r[p][:width, :LANES] * inv[i, 2 * p:2 * p + 1, :])
                parts.append(r[p][width:, LANES:] * inv[i, 2 * p + 1:2 * p + 2, :])
            outs.append((jnp.concatenate(parts, axis=0) * gbuf[base + i, :c]).astype(BF16))
        return outs

    def row_bias(c):
        def step(idx):
            put_bias(stack([layer_norm(z_in[c, i].astype(F32)) for i in idx]), 0, heads_m, idx)
        grouped(res, 6, step)
        ag_r[c, me] = stg_b[...].astype(BF16)
        start(gather_copies(0, c, ag_r))

    loop(crops, row_bias)

    def row_prep(c):
        def prep(idx):
            fill = jnp.zeros((c_m, LANES - n_res), F32)
            ms = [jnp.concatenate([m_in[c, s].astype(F32), fill], axis=1) for s in idx]
            keep(mm(wt_r[...], jnp.concatenate([layer_norm_t(x) for x in ms], axis=1)), c_m,
                 [c * slots + s for s in idx], n_res, [mask_r[c, pl.ds(me * seqs + s, 1), :] for s in idx])
            for s, x in zip(idx, ms):
                xw[c * slots + s] = x
        grouped(seqs, 4, prep)

    loop(crops, row_prep)

    def row_attention(c):
        base = c * slots
        grouped(seqs, 4, lambda idx: logits(idx, base, heads_m, d_m, hm8, n_res, True))
        gather_wait(0, c, ag_r)
        gathered_bias(ag_r, c, heads_m, d_m, True, None)
        grouped(seqs, 2, lambda idx: softmax(idx, heads_m, d_m, n_res, True))

        def step(idx):
            both = [s + t * half for s in idx for t in range(2)]
            upd = mm(wt_ro[...], jnp.concatenate(mixed(both, base, heads_m, d_m, n_res), axis=1))
            new = [xw[base + s] + upd[:, t * LANES:(t + 1) * LANES] for t, s in enumerate(both)]
            for k, s in enumerate(idx):
                x2 = jnp.concatenate(new[2 * k:2 * k + 2], axis=0).T
                stg_m[pl.ds(s, n_res, stride=half), :] = x2[:n_res]
        grouped(half, 4, step)
        for p in range(n):
            snd_m[c, p] = stg_m[p * res * half:(p + 1) * res * half, :].reshape(res, half, LANES).astype(BF16)
        rcv_m[c, me] = snd_m[c, me]
        start(swap_copies(1, c, snd_m, rcv_m))

    loop(crops, row_attention)

    def col_attention(c):
        base = c * slots
        arrivals(1, c, lambda sender: rcv_m.at[c, sender])
        hs = n_seq // 2

        def mask_row(i):
            return mask_t[c, pl.ds(me * SLOT + i, 1), :]

        def prep(idx):
            ys = []
            for k in range(0, len(idx), 2):
                x2 = jnp.concatenate([rcv_m[c, q, i].astype(F32) for i in idx[k:k + 2] for q in range(n)], axis=0).T
                for t, i in enumerate(idx[k:k + 2]):
                    x = jnp.concatenate([x2[:c_m, t * hs:(t + 1) * hs], x2[c_m:, t * hs:(t + 1) * hs]], axis=1)
                    xw[base + i] = x
                    ys.append(layer_norm_t(x))
            keep(mm(wt_c[...], jnp.concatenate(ys, axis=1)), c_m, [base + i for i in idx], LANES,
                 [mask_row(i) for i in idx])
        grouped(res, 4, prep)

        def group(g):
            idx = [g * part_rows + t for t in range(part_rows)]
            logits(idx, base, heads_m, d_m, hm8, LANES, True)
            softmax(idx, heads_m, d_m, LANES, False)
            upd = mm(wt_co[...], jnp.concatenate(mixed(idx, base, heads_m, d_m, LANES), axis=1))
            new = [(xw[base + i] + upd[:, t * LANES:(t + 1) * LANES]).astype(BF16).astype(F32)
                   for t, i in enumerate(idx)]
            ac = mm(w_ac[...], jnp.concatenate([layer_norm_t(x) for x in new], axis=1)).astype(BF16).astype(F32)
            for t, i in enumerate(idx):
                part = ac[:, t * LANES:(t + 1) * LANES] * mask_row(i)
                ag_c[c, g, me, t] = part[o_w:].astype(BF16)
                abuf[c, pl.ds(pl.multiple_of(i * o_w, o_w), o_w), :] = part[:o_w].astype(BF16)
            k = c * pieces + g
            relay_own(k)

            @pl.when(k >= 2)
            def _():
                relay(k - 2)

            for t in range(0, part_rows, 2):
                two = jnp.concatenate([
                    jnp.concatenate([x[:, :hs] for x in new[t:t + 2]], axis=1),
                    jnp.concatenate([x[:, hs:] for x in new[t:t + 2]], axis=1)], axis=0).T
                for u, i in enumerate(idx[t:t + 2]):
                    for q in range(n):
                        snd_b[c, q, i] = two[u * hs + q * half:u * hs + (q + 1) * half].astype(BF16)
        loop(pieces, group)
        rcv_b[c, me] = snd_b[c, me]

    loop(crops, col_attention)

    def outer_product(c):
        base = c * slots
        mloc = mask_t[c, pl.ds(pl.multiple_of(me * SLOT, SLOT), SLOT), :].astype(BF16)
        norm[...] = 1.0 / (mm(mloc, mask_n[c], NT) + OPM_EPS)
        pitch = n_res + 8

        for g in range(pieces):
            relay_done(c * pieces + g)

            def spread(p):
                for t in range(part_rows):
                    stg_c[pl.ds(p * res + g * part_rows + t, o_w, stride=pitch), :] = ag_c[c, g, p, t].astype(F32)
            loop(n, spread)


        def outer(fs):
            rows = [stg_c[pl.ds(pl.multiple_of(f * pitch, 8), n_res), :].astype(BF16) for f in fs]
            outs = [mm(abuf[c], stack(rows[k:k + 2]), NT) for k in range(0, len(fs), 2)]
            for k, f in enumerate(fs):
                out = outs[k // 2][:, (k % 2) * LANES:(k % 2 + 1) * LANES]
                for i in range(res):
                    obuf[i, pl.ds(pl.multiple_of(f * o_w, o_w), o_w), :] = (
                        out[i * o_w:(i + 1) * o_w] * norm[i:i + 1, :]).astype(BF16)
        grouped(o_w, 8, outer)

        @pl.when(c == 0)
        def _():
            relay(n_blocks - 2)

        start(swap_copies(3, c, snd_b, rcv_b))

        def update(idx):
            rhs = [jnp.concatenate([obuf[i] for i in idx[k:k + 2]], axis=1) for k in range(0, len(idx), 2)]
            upds = [mm(w_oo_t[...], r) for r in rhs]
            for k, i in enumerate(idx):
                upd = upds[k // 2][:, (k % 2) * LANES:(k % 2 + 1) * LANES].T
                zw[c, i] = (z_in[c, i].astype(F32) + upd[:n_res]).astype(BF16)
        grouped(res, 4, update)

        def prep(idx):
            y = stack([layer_norm(zw[c, i].astype(F32)) for i in idx])
            put_bias(y, 1, heads_z, idx)
            keep(mm(wt_s[...], y, NT), c_z, [base + i for i in idx], n_res)
        grouped(res, 6, prep)
        @pl.when(c == 0)
        def _():
            relay(n_blocks - 1)

        ag_s[c, me] = stg_b[:heads_z * res, :].astype(BF16)
        start(gather_copies(4, c, ag_s))

    loop(crops, outer_product)

    def res_bias(c):
        return column((res_r[pl.ds(c, 1), :] - 1.0) * (MASK_SCALE * d_z ** 0.5))

    def piece_copies(first, c, g, snd, rcv):
        return copies(first + g, c, lambda peer: snd.at[c, g, peer], rcv.at[c, g, me])

    def send_rows(zs, snd, c, g):
        for t, z in enumerate(zs):
            stg_m[pl.ds(t, n_res, stride=part_rows), :] = z
        size = res * part_rows
        for q in range(n):
            snd[c, g, q] = stg_m[q * size:(q + 1) * size, :].astype(BF16)

    def take_columns(first, c, rcv):
        for g in range(pieces):
            arrivals(first + g, c, lambda sender: rcv.at[c, g, sender])
        for p in range(n):
            for g in range(pieces):
                block = rcv[c, g, p].astype(F32)
                row0 = p * res + g * part_rows
                for j in range(res):
                    xs[j, row0:row0 + part_rows, :] = block[j * part_rows:(j + 1) * part_rows]

    def tri_start(c):
        base = c * slots
        gather_wait(4, c, ag_s)
        gathered_bias(ag_s, c, heads_z, d_z, True, res_bias(c))
        stg_b[...] = jnp.zeros(stg_b.shape, F32)

        def group(g):
            idx = [g * part_rows + t for t in range(part_rows)]
            logits(idx, base, heads_z, d_z, hm4, n_res, False)
            softmax(idx, heads_z, d_z, n_res, True)
            upds = [mm(o, w_so[...], TN) for o in mixed(idx, base, heads_z, d_z, n_res)]
            zs = [(zw[c, i].astype(F32) + upd[:n_res]).astype(BF16).astype(F32) for i, upd in zip(idx, upds)]
            send_rows(zs, snd_z, c, g)
            start(piece_copies(10, c, g, snd_z, rcv_z))
            rcv_z[c, g, me] = snd_z[c, g, me]
            put_bias(stack([layer_norm(z) for z in zs]), 2, heads_z, idx)
        loop(pieces, group)
        ag_e[c, me] = stg_b[:heads_z * res, :].astype(BF16)
        start(gather_copies(5, c, ag_e))

    loop(crops, tri_start)

    def tri_end(c):
        base = c * slots
        take_columns(10, c, rcv_z)

        def prep(idx):
            keep(mm(wt_e[...], stack([layer_norm(xs[j]) for j in idx]), NT), c_z, [base + j for j in idx], n_res)
        grouped(res, 6, prep)
        gather_wait(5, c, ag_e)
        gathered_bias(ag_e, c, heads_z, d_z, False, res_bias(c))

        def step(g):
            idx = [g * part_rows + t for t in range(part_rows)]
            logits(idx, base, heads_z, d_z, hm4, n_res, False)
            softmax(idx, heads_z, d_z, n_res, True)
            upds = [mm(o, w_eo[...], TN) for o in mixed(idx, base, heads_z, d_z, n_res)]
            send_rows([xs[j] + upd[:n_res] for j, upd in zip(idx, upds)], snd_y, c, g)
            start(piece_copies(7, c, g, snd_y, zback))
            zback[c, g, me] = snd_y[c, g, me]
        loop(pieces, step)

    loop(crops, tri_end)

    def put_m(c):
        arrivals(3, c, lambda sender: rcv_b.at[c, sender])
        stg_m[...] = rcv_b[c].astype(F32).reshape(n * res * half, LANES)

        def step(idx):
            for s in idx:
                x2 = stg_m[pl.ds(s, n_res, stride=half), :].T
                m_out[c, s] = x2[:c_m].astype(BF16)
                m_out[c, s + half] = x2[c_m:].astype(BF16)
        grouped(half, 4, step)

    loop(crops, put_m)

    def put_z(c):
        take_columns(7, c, zback)

        def step(i):
            z_out[c, i] = xs[i].astype(BF16)
        for i in range(res):
            step(i)

    loop(crops, put_z)

    def drain(c):
        finish(gather_copies(0, c, ag_r))
        finish(swap_copies(1, c, snd_m, rcv_m))
        for g in range(pieces):
            for slot in range(n - 1):
                block_copy(c * pieces + g, me, device(1), slot).wait_send()
            finish(piece_copies(7, c, g, snd_y, zback))
            finish(piece_copies(10, c, g, snd_z, rcv_z))
        finish(swap_copies(3, c, snd_b, rcv_b))
        finish(gather_copies(4, c, ag_s))
        finish(gather_copies(5, c, ag_e))

    loop(crops, drain)


def solution(mesh):
    n = mesh.shape[GROUP_AXIS]
    rows_spec = P(PART_AXIS, GROUP_AXIS, None, None)
    in_specs = (rows_spec, rows_spec, P(PART_AXIS, None, None), P(PART_AXIS, None)) + (P(),) * N_WEIGHTS

    def local_block(m, z, msa_mask, res_mask, w_rb, w_rq, w_ro, w_cq, w_co, w_ac, w_oo, w_sb, w_sq, w_so,
                    w_eb, w_eq, w_eo):
        crops, seqs, n_res, c_m = m.shape
        res, c_z = z.shape[1], z.shape[3]
        heads_m, heads_z = w_rq.shape[2], w_sq.shape[2]
        o_w = w_ac.shape[2]
        half = seqs // 2
        assert n == 8 and crops == 2 and res % 3 == 0 and n * SLOT == LANES and res <= SLOT and n * seqs == LANES and 2 * c_m == LANES and c_z == LANES
        flat = lambda w: jnp.moveaxis(w, 0, -1).reshape(-1, w.shape[0])
        tall = lambda w: w.reshape(-1, w.shape[-1])
        args = (m.swapaxes(2, 3), z, msa_mask.swapaxes(1, 2), res_mask, w_rb.T, flat(w_rq), tall(w_ro), flat(w_cq),
                tall(w_co), flat(w_ac), tall(w_oo), w_sb.T, flat(w_sq), tall(w_so), w_eb.T, flat(w_eq), tall(w_eo))
        vm = pltpu.VMEM
        slots = max(seqs, res)
        pieces = 2
        piece = res * res // pieces
        scratch = [
            vm((crops, n, heads_m * res, LANES), BF16),
            vm((crops, pieces, n, res // pieces, o_w, LANES), BF16),
            vm((crops, n, heads_z * res, LANES), BF16),
            vm((crops, n, heads_z * res, LANES), BF16),
            vm((crops, n, res, half, LANES), BF16),
            vm((crops, n, res, half, LANES), BF16),
            vm((crops, n, res, half, LANES), BF16),
            vm((crops, n, res, half, LANES), BF16),
            vm((crops, pieces, n, piece, LANES), BF16),
            vm((crops, pieces, n, piece, LANES), BF16),
            vm((crops, pieces, n, piece, LANES), BF16),
            vm((crops, pieces, n, piece, LANES), BF16),
            pltpu.SemaphoreType.DMA((13, crops, n)),
            pltpu.SemaphoreType.DMA((13, crops, n)),
            pltpu.SemaphoreType.DMA((crops * pieces, n)),
            pltpu.SemaphoreType.DMA((crops * pieces, n)),
        ]
        local = [
            vm((crops, res, n_res, LANES), BF16),
            vm((crops * slots, c_m, LANES), F32),
            vm((crops * slots, LANES, LANES), BF16),
            vm((crops * slots, LANES, LANES), BF16),
            vm((crops * slots, LANES, LANES), BF16),
            vm((crops * slots, LANES, LANES), F32),
            vm((heads_m, n_res, LANES), F32),
            vm((res, o_w * o_w, LANES), BF16),
            vm((n * res * half, LANES), F32),
            vm((o_w * (n_res + 8), LANES), F32),
            vm((heads_m * res, LANES), F32),
            vm((n_res * res, LANES), F32),
            vm((crops, res * o_w, LANES), BF16),
            vm((crops, LANES, LANES), F32),
            vm((crops, n * seqs, LANES), F32),
            vm((crops, LANES), F32),
            vm((slots, heads_m // 2, LANES, 2 * LANES), F32),
            vm((slots, heads_m // 2, LANES, 2 * LANES), BF16),
            vm((slots, heads_m, LANES), F32),
            vm((SLOT, LANES), F32),
            vm((heads_m, c_m, LANES), BF16),
            vm((heads_z, c_z, LANES), BF16),
            vm((c_m, c_m), BF16),
            vm((c_m, c_m), BF16),
            vm((LANES, o_w * o_w), BF16),
            vm((3, SLOT, LANES), BF16),
            vm((AUG, LANES), F32),
            vm((AUG, 2 * LANES), BF16),
            vm((res, n_res, LANES), F32),
            vm((crops, LANES, LANES), BF16),
        ]
        cfg = dict(n=n, heads_m=heads_m, heads_z=heads_z, slots=slots, pieces=pieces, local=local)
        spec = pl.BlockSpec(memory_space=pltpu.VMEM)
        m_new, z_new = pl.pallas_call(
            functools.partial(body, cfg),
            out_shape=(jax.ShapeDtypeStruct((crops, seqs, c_m, n_res), BF16), jax.ShapeDtypeStruct(z.shape, BF16)),
            in_specs=[spec] * len(args),
            out_specs=(spec, spec),
            scratch_shapes=scratch,
            compiler_params=pltpu.CompilerParams(collective_id=0, has_side_effects=True,
                                                 vmem_limit_bytes=60 * 1024 * 1024),
        )(*args)
        return m_new.swapaxes(2, 3), z_new

    return jax.shard_map(local_block, mesh=mesh, in_specs=in_specs, out_specs=(rows_spec, rows_spec),
                         check_vma=False)
```

```python
import functools
import math

import jax
import jax.numpy as jnp
import numpy as np
from jax import lax
from jax.experimental import pallas as pl
from jax.experimental.pallas import tpu as pltpu
from jax.sharding import PartitionSpec as P

MASK_SCALE = 10000.0
LN_EPS = 1e-5
OPM_EPS = 1e-3
N_WEIGHTS = 13
PART_AXIS = 'data'
GROUP_AXIS = 'dap'
LOG2E = math.log2(math.e)
AUG = 16
LANES = 128
SLOT = 16
F32 = jnp.float32
BF16 = jnp.bfloat16
NN = (((1,), (0,)), ((), ()))
NT = (((1,), (1,)), ((), ()))
TN = (((0,), (0,)), ((), ()))


def mm(lhs, rhs, dims=NN):
    return lax.dot_general(lhs, rhs, dims, preferred_element_type=F32)


def layer_norm(x_float):
    mean_val = jnp.mean(x_float, axis=-1, keepdims=True)
    centred = x_float - mean_val
    var_val = jnp.mean(centred * centred, axis=-1, keepdims=True)
    return (centred * lax.rsqrt(var_val + LN_EPS)).astype(BF16)


def layer_norm_t(x_float):
    mean_val = jnp.mean(x_float, axis=0, keepdims=True)
    centred = x_float - mean_val
    var_val = jnp.mean(centred * centred, axis=0, keepdims=True)
    return (centred * lax.rsqrt(var_val + LN_EPS)).astype(BF16)


def iota(shape, axis):
    return lax.broadcasted_iota(jnp.int32, shape, axis)


def body(cfg, *refs):
    pl.run_scoped(functools.partial(scoped_body, cfg, refs), *cfg['local'])


def scoped_body(cfg, refs, *local):
    n = cfg['n']
    (m_in, z_in, mask_in, res_in, w_rb, wt_r, w_ro, wt_c, w_co, w_ac, w_oo,
     w_sb, wt_s, w_so, w_eb, wt_e, w_eo, m_out, z_out,
     ag_r, ag_c, ag_s, ag_e, snd_m, rcv_m, snd_b, rcv_b, snd_z, rcv_z, snd_y, zback, send_sem, recv_sem,
     ring_send, ring_recv) = refs
    (zw, xw, kbuf, qbuf, vbuf, gbuf, bias, obuf, stg_m, stg_c, stg_b, stg_z, abuf,
     mask_t, mask_r, res_r, raw, prob, inv, norm, hm8, hm4, wt_ro, wt_co, w_oo_t, wt_b, aug, one_rows, xs, mask_n) = local
    crops, seqs, c_m, n_res = m_in.shape
    res = z_in.shape[1]
    c_z = z_in.shape[3]
    half = seqs // 2
    heads_m, heads_z = cfg['heads_m'], cfg['heads_z']
    d_m, d_z = c_m // heads_m, c_z // heads_z
    n_seq = n * seqs
    slots, pieces = cfg['slots'], cfg['pieces']
    part_rows, n_blocks = res // pieces, crops * pieces
    me = lax.axis_index(GROUP_AXIS)

    barrier = pltpu.get_barrier_semaphore()
    for r in range(1, n):
        pl.semaphore_signal(barrier, inc=1, device_id={GROUP_AXIS: lax.rem(me + r, n)},
                            device_id_type=pl.DeviceIdType.MESH)
    pl.semaphore_wait(barrier, n - 1)

    def copies(exch, c, src_of, dst):
        out = []
        for r in range(1, n):
            peer = lax.rem(me + r, n)
            out.append(pltpu.make_async_remote_copy(
                src_ref=src_of(peer), dst_ref=dst, send_sem=send_sem.at[exch, c, r], recv_sem=recv_sem.at[exch, c, r],
                device_id={GROUP_AXIS: peer}, device_id_type=pl.DeviceIdType.MESH))
        return out

    def arrivals(exch, c, slot_of):
        for r in range(1, n):
            sender = lax.rem(me + n - r, n)
            ref = slot_of(sender)
            pltpu.make_async_remote_copy(
                src_ref=ref, dst_ref=ref, send_sem=send_sem.at[exch, c, r], recv_sem=recv_sem.at[exch, c, r],
                device_id={GROUP_AXIS: sender}, device_id_type=pl.DeviceIdType.MESH).wait_recv()

    def gather_copies(exch, c, buf):
        return copies(exch, c, lambda peer: buf.at[c, me], buf.at[c, me])

    def gather_wait(exch, c, buf):
        arrivals(exch, c, lambda sender: buf.at[c, sender])

    def swap_copies(exch, c, snd, rcv):
        return copies(exch, c, lambda peer: snd.at[c, peer], rcv.at[c, me])

    chips, core, chip = n // 2, lax.rem(me, 2), me // 2

    def device(offset, other=False):
        return lax.rem(chip + offset + chips, chips) * 2 + ((1 - core) if other else core)

    def block_copy(k, block, peer, slot):
        c, g = k // pieces, lax.rem(k, pieces)
        return pltpu.make_async_remote_copy(
            src_ref=ag_c.at[c, g, block], dst_ref=ag_c.at[c, g, block], send_sem=ring_send.at[k, slot],
            recv_sem=ring_recv.at[k, block], device_id={GROUP_AXIS: peer}, device_id_type=pl.DeviceIdType.MESH)

    def block_wait(k, block):
        block_copy(k, block, block, 0).wait_recv()

    def relay_own(k):
        for slot in range(chips):
            block_copy(k, me, device(slot, slot == 0), slot).start()

    def relay(k):
        for offset in range(1, chips):
            block_wait(k, device(offset))
        for offset in range(1, chips):
            block_copy(k, device(offset), device(0, True), chips - 1 + offset).start()

    def relay_done(k):
        for offset in range(chips):
            block_wait(k, device(offset, True))

    def start(descs):
        for d in descs:
            d.start()

    def finish(descs):
        for d in descs:
            d.wait_send()

    def loop(count, fn):
        def step(i, carry):
            fn(i)
            return carry
        lax.fori_loop(0, count, step, 0)

    def pad_matrix():
        row, col = iota((LANES, n_res), 0), iota((LANES, n_res), 1)
        hit = (col == (row // SLOT) * res + row % SLOT) & (row % SLOT < res)
        return jnp.where(hit, 1.0, 0.0).astype(BF16)

    def head_rows(heads, width, ref):
        for h in range(heads):
            row = iota((heads * width, LANES), 0)
            ref[h] = jnp.where((row >= h * width) & (row < (h + 1) * width), 1.0, 0.0).astype(BF16)

    pad = pad_matrix()
    tail = jnp.where(iota((n_res, LANES), 0) == iota((n_res, LANES), 1), 1.0, 0.0).astype(BF16)
    head_rows(heads_m, d_m, hm8)
    head_rows(heads_z, d_z, hm4)
    row, col = iota((LANES, LANES), 0), iota((LANES, LANES), 1)
    seq_of = ((col % (n_seq // 2)) // half) * seqs + (col // (n_seq // 2)) * half + col % half
    seq_perm = jnp.where(row == seq_of, 1.0, 0.0).astype(BF16)
    for c in range(crops):
        mask_bf = mask_in[c].astype(F32).astype(BF16)
        mask_t[c] = mm(mm(pad, mask_bf).astype(BF16), seq_perm)
        mask_n[c, :n_res] = mm(mask_bf, seq_perm).astype(BF16)
        mask_n[c, n_res:] = jnp.zeros((LANES - n_res, LANES), BF16)
        mask_r[c] = mm(mask_bf, tail, TN)
    res_r[...] = mm(res_in[...].astype(F32).astype(BF16), tail)
    term = MASK_SCALE * d_m ** 0.5
    aug[...] = jnp.zeros(aug.shape, F32)
    ones = jnp.zeros((AUG, 2 * LANES), F32)
    for k in range(3):
        piece = float(np.array(term, dtype=BF16))
        term = term - piece
        aug[k:k + 1, :] = jnp.full((1, LANES), piece, F32)
        ones = jnp.where(iota(ones.shape, 0) == k, 1.0, ones)
    one_rows[...] = ones.astype(BF16)
    for k, w in enumerate((w_rb, w_sb, w_eb)):
        wt_b[k] = jnp.zeros(wt_b.shape[1:], BF16)
        wt_b[k, :w.shape[0], :] = w[...]
    wt_ro[...] = w_ro[...].astype(F32).T.astype(BF16)
    wt_co[...] = w_co[...].astype(F32).T.astype(BF16)
    o_w = w_ac.shape[0] // 2
    stg_z[:o_w * o_w, :] = w_oo[...].astype(F32)
    for k in range(0, o_w, LANES // o_w):
        rows = [stg_z[pl.ds(f, o_w, stride=o_w), :] for f in range(k, k + LANES // o_w)]
        w_oo_t[:, k * o_w:k * o_w + LANES] = jnp.concatenate(rows, axis=0).T.astype(BF16)

    stg_b[...] = jnp.zeros(stg_b.shape, F32)

    def grouped(count, size, fn):
        while count % size:
            size -= 1

        def step(b, carry):
            fn([b * size + t for t in range(size)])
            return carry
        lax.fori_loop(0, count // size, step, 0)

    def put_bias(y, k, heads, rows):
        b = mm(wt_b[k], y, NT)
        for t, i in enumerate(rows):
            for h in range(heads):
                stg_b[pl.ds(h * res + i, 1), :] = b[h:h + 1, t * LANES:(t + 1) * LANES]

    def stack(ys):
        fill = jnp.zeros((LANES - n_res, ys[0].shape[1]), BF16)
        return jnp.concatenate([part for y in ys for part in (y, fill)], axis=0)

    def keep(p, width, slots, length, mask_rows=None):
        for t, slot in enumerate(slots):
            part = slice(t * LANES, (t + 1) * LANES)
            keys = p[width:2 * width, part]
            if mask_rows is not None:
                keys = jnp.concatenate([keys, (mask_rows[t] - 1.0) * aug[...]], axis=0)
            qbuf[slot, :width] = p[:width, part].astype(BF16)
            kbuf[slot, :length, :keys.shape[0]] = keys.T[:length].astype(BF16)
            vbuf[slot, :width] = p[2 * width:3 * width, part].astype(BF16)
            gbuf[slot, :width] = jax.nn.sigmoid(p[3 * width:, part])

    def column(rowvec):
        return jnp.broadcast_to(rowvec, (LANES, LANES)).T[:n_res]

    def gathered_bias(buf, c, heads, width, flip, add):
        parts = [buf[c, p].astype(F32) for p in range(n)]
        for h in range(heads):
            b = jnp.concatenate([part[h * res:(h + 1) * res] for part in parts], axis=0)
            if flip:
                b = jnp.concatenate([b, jnp.zeros((LANES - n_res, LANES), F32)], axis=0).T[:n_res]
            b = b * width ** 0.5
            bias[h] = b if add is None else b + add

    def logits(idx, base, heads, width, head_mask, length, masked):
        c = heads * width
        for i in idx:
            q_t, keys = qbuf[base + i, :c], kbuf[base + i, :length, :c + (AUG if masked else 0)]
            for pair in range(heads // 2):
                rhs = jnp.concatenate([q_t * head_mask[2 * pair], q_t * head_mask[2 * pair + 1]], axis=1)
                if masked:
                    rhs = jnp.concatenate([rhs, one_rows[...]], axis=0)
                raw[i, pair, :length] = mm(keys, rhs)

    def softmax(idx, heads, width, length, biased):
        scale2 = LOG2E * width ** -0.5
        for i in idx:
            for h in range(heads):
                part = slice((h % 2) * LANES, (h % 2 + 1) * LANES)
                x = raw[i, h // 2, :length, part]
                if biased:
                    x = x + bias[h]
                e = jnp.exp2((x - jnp.max(x, axis=0, keepdims=True)) * scale2)
                inv[i, h:h + 1, :] = 1.0 / jnp.sum(e, axis=0, keepdims=True)
                prob[i, h // 2, :length, part] = e.astype(BF16)

    def mixed(idx, base, heads, width, length):
        c = heads * width
        raws = [[mm(vbuf[base + i, 2 * p * width:2 * (p + 1) * width, :length], prob[i, p, :length])
                 for p in range(heads // 2)] for i in idx]
        outs = []
        for i, r in zip(idx, raws):
            parts = []
            for p in range(heads // 2):
                parts.append(r[p][:width, :LANES] * inv[i, 2 * p:2 * p + 1, :])
                parts.append(r[p][width:, LANES:] * inv[i, 2 * p + 1:2 * p + 2, :])
            outs.append((jnp.concatenate(parts, axis=0) * gbuf[base + i, :c]).astype(BF16))
        return outs

    def row_bias(c):
        def step(idx):
            put_bias(stack([layer_norm(z_in[c, i].astype(F32)) for i in idx]), 0, heads_m, idx)
        grouped(res, 12, step)
        ag_r[c, me] = stg_b[...].astype(BF16)
        start(gather_copies(0, c, ag_r))

    loop(crops, row_bias)

    def row_prep(c):
        def prep(idx):
            fill = jnp.zeros((c_m, LANES - n_res), F32)
            ms = [jnp.concatenate([m_in[c, s].astype(F32), fill], axis=1) for s in idx]
            keep(mm(wt_r[...], jnp.concatenate([layer_norm_t(x) for x in ms], axis=1)), c_m,
                 [c * slots + s for s in idx], n_res, [mask_r[c, pl.ds(me * seqs + s, 1), :] for s in idx])
            for s, x in zip(idx, ms):
                xw[c * slots + s] = x
        grouped(seqs, 8, prep)

    loop(crops, row_prep)

    def row_attention(c):
        base = c * slots
        grouped(seqs, 8, lambda idx: logits(idx, base, heads_m, d_m, hm8, n_res, True))
        gather_wait(0, c, ag_r)
        gathered_bias(ag_r, c, heads_m, d_m, True, None)
        grouped(seqs, 2, lambda idx: softmax(idx, heads_m, d_m, n_res, True))

        def step(idx):
            both = [s + t * half for s in idx for t in range(2)]
            upd = mm(wt_ro[...], jnp.concatenate(mixed(both, base, heads_m, d_m, n_res), axis=1))
            new = [xw[base + s] + upd[:, t * LANES:(t + 1) * LANES] for t, s in enumerate(both)]
            for k, s in enumerate(idx):
                x2 = jnp.concatenate(new[2 * k:2 * k + 2], axis=0).T
                stg_m[pl.ds(s, n_res, stride=half), :] = x2[:n_res]
        grouped(half, 4, step)
        for p in range(n):
            snd_m[c, p] = stg_m[p * res * half:(p + 1) * res * half, :].reshape(res, half, LANES).astype(BF16)
        rcv_m[c, me] = snd_m[c, me]
        start(swap_copies(1, c, snd_m, rcv_m))

    loop(crops, row_attention)

    def col_attention(c):
        base = c * slots
        arrivals(1, c, lambda sender: rcv_m.at[c, sender])
        hs = n_seq // 2

        def mask_row(i):
            return mask_t[c, pl.ds(me * SLOT + i, 1), :]

        def prep(idx):
            ys = []
            for k in range(0, len(idx), 2):
                x2 = jnp.concatenate([rcv_m[c, q, i].astype(F32) for i in idx[k:k + 2] for q in range(n)], axis=0).T
                for t, i in enumerate(idx[k:k + 2]):
                    x = jnp.concatenate([x2[:c_m, t * hs:(t + 1) * hs], x2[c_m:, t * hs:(t + 1) * hs]], axis=1)
                    xw[base + i] = x
                    ys.append(layer_norm_t(x))
            keep(mm(wt_c[...], jnp.concatenate(ys, axis=1)), c_m, [base + i for i in idx], LANES,
                 [mask_row(i) for i in idx])
        grouped(res, 6, prep)

        def group(g):
            idx = [g * part_rows + t for t in range(part_rows)]
            logits(idx, base, heads_m, d_m, hm8, LANES, True)
            softmax(idx, heads_m, d_m, LANES, False)
            upd = mm(wt_co[...], jnp.concatenate(mixed(idx, base, heads_m, d_m, LANES), axis=1))
            new = [(xw[base + i] + upd[:, t * LANES:(t + 1) * LANES]).astype(BF16).astype(F32)
                   for t, i in enumerate(idx)]
            ac = mm(w_ac[...], jnp.concatenate([layer_norm_t(x) for x in new], axis=1)).astype(BF16).astype(F32)
            for t, i in enumerate(idx):
                part = ac[:, t * LANES:(t + 1) * LANES] * mask_row(i)
                ag_c[c, g, me, t] = part[o_w:].astype(BF16)
                abuf[c, pl.ds(pl.multiple_of(i * o_w, o_w), o_w), :] = part[:o_w].astype(BF16)
            k = c * pieces + g
            relay_own(k)

            @pl.when(k >= 2)
            def _():
                relay(k - 2)

            for t in range(0, part_rows, 2):
                two = jnp.concatenate([
                    jnp.concatenate([x[:, :hs] for x in new[t:t + 2]], axis=1),
                    jnp.concatenate([x[:, hs:] for x in new[t:t + 2]], axis=1)], axis=0).T
                for u, i in enumerate(idx[t:t + 2]):
                    for q in range(n):
                        snd_b[c, q, i] = two[u * hs + q * half:u * hs + (q + 1) * half].astype(BF16)
        loop(pieces, group)
        rcv_b[c, me] = snd_b[c, me]

    loop(crops, col_attention)

    def outer_product(c):
        base = c * slots
        mloc = mask_t[c, pl.ds(pl.multiple_of(me * SLOT, SLOT), SLOT), :].astype(BF16)
        norm[...] = 1.0 / (mm(mloc, mask_n[c], NT) + OPM_EPS)
        pitch = n_res + 8

        for g in range(pieces):
            relay_done(c * pieces + g)

            def spread(p):
                for t in range(part_rows):
                    stg_c[pl.ds(p * res + g * part_rows + t, o_w, stride=pitch), :] = ag_c[c, g, p, t].astype(F32)
            loop(n, spread)


        def outer(fs):
            rows = [stg_c[pl.ds(pl.multiple_of(f * pitch, 8), n_res), :].astype(BF16) for f in fs]
            outs = [mm(abuf[c], stack(rows[k:k + 2]), NT) for k in range(0, len(fs), 2)]
            for k, f in enumerate(fs):
                out = outs[k // 2][:, (k % 2) * LANES:(k % 2 + 1) * LANES]
                for i in range(res):
                    obuf[i, pl.ds(pl.multiple_of(f * o_w, o_w), o_w), :] = (
                        out[i * o_w:(i + 1) * o_w] * norm[i:i + 1, :]).astype(BF16)
        grouped(o_w, 8, outer)

        @pl.when(c == 0)
        def _():
            relay(n_blocks - 2)

        start(swap_copies(3, c, snd_b, rcv_b))

        def update(idx):
            rhs = [jnp.concatenate([obuf[i] for i in idx[k:k + 2]], axis=1) for k in range(0, len(idx), 2)]
            upds = [mm(w_oo_t[...], r) for r in rhs]
            for k, i in enumerate(idx):
                upd = upds[k // 2][:, (k % 2) * LANES:(k % 2 + 1) * LANES].T
                zw[c, i] = (z_in[c, i].astype(F32) + upd[:n_res]).astype(BF16)
        grouped(res, 6, update)

        def prep(idx):
            y = stack([layer_norm(zw[c, i].astype(F32)) for i in idx])
            put_bias(y, 1, heads_z, idx)
            keep(mm(wt_s[...], y, NT), c_z, [base + i for i in idx], n_res)
        grouped(res, 12, prep)
        @pl.when(c == 0)
        def _():
            relay(n_blocks - 1)

        ag_s[c, me] = stg_b[:heads_z * res, :].astype(BF16)
        start(gather_copies(4, c, ag_s))

    loop(crops, outer_product)

    def res_bias(c):
        return column((res_r[pl.ds(c, 1), :] - 1.0) * (MASK_SCALE * d_z ** 0.5))

    def piece_copies(first, c, g, snd, rcv):
        return copies(first + g, c, lambda peer: snd.at[c, g, peer], rcv.at[c, g, me])

    def send_rows(zs, snd, c, g):
        for t, z in enumerate(zs):
            stg_m[pl.ds(t, n_res, stride=part_rows), :] = z
        size = res * part_rows
        for q in range(n):
            snd[c, g, q] = stg_m[q * size:(q + 1) * size, :].astype(BF16)

    def take_columns(first, c, rcv):
        for g in range(pieces):
            arrivals(first + g, c, lambda sender: rcv.at[c, g, sender])
        for p in range(n):
            for g in range(pieces):
                block = rcv[c, g, p].astype(F32)
                row0 = p * res + g * part_rows
                for j in range(res):
                    xs[j, row0:row0 + part_rows, :] = block[j * part_rows:(j + 1) * part_rows]

    def tri_start(c):
        base = c * slots
        gather_wait(4, c, ag_s)
        gathered_bias(ag_s, c, heads_z, d_z, True, res_bias(c))
        stg_b[...] = jnp.zeros(stg_b.shape, F32)

        def group(g):
            idx = [g * part_rows + t for t in range(part_rows)]
            logits(idx, base, heads_z, d_z, hm4, n_res, False)
            softmax(idx, heads_z, d_z, n_res, True)
            upds = [mm(o, w_so[...], TN) for o in mixed(idx, base, heads_z, d_z, n_res)]
            zs = [(zw[c, i].astype(F32) + upd[:n_res]).astype(BF16).astype(F32) for i, upd in zip(idx, upds)]
            send_rows(zs, snd_z, c, g)
            start(piece_copies(10, c, g, snd_z, rcv_z))
            rcv_z[c, g, me] = snd_z[c, g, me]
            put_bias(stack([layer_norm(z) for z in zs]), 2, heads_z, idx)
        loop(pieces, group)
        ag_e[c, me] = stg_b[:heads_z * res, :].astype(BF16)
        start(gather_copies(5, c, ag_e))

    loop(crops, tri_start)

    def tri_end(c):
        base = c * slots
        take_columns(10, c, rcv_z)

        def prep(idx):
            keep(mm(wt_e[...], stack([layer_norm(xs[j]) for j in idx]), NT), c_z, [base + j for j in idx], n_res)
        grouped(res, 12, prep)
        gather_wait(5, c, ag_e)
        gathered_bias(ag_e, c, heads_z, d_z, False, res_bias(c))

        def step(g):
            idx = [g * part_rows + t for t in range(part_rows)]
            logits(idx, base, heads_z, d_z, hm4, n_res, False)
            softmax(idx, heads_z, d_z, n_res, True)
            upds = [mm(o, w_eo[...], TN) for o in mixed(idx, base, heads_z, d_z, n_res)]
            send_rows([xs[j] + upd[:n_res] for j, upd in zip(idx, upds)], snd_y, c, g)
            start(piece_copies(7, c, g, snd_y, zback))
            zback[c, g, me] = snd_y[c, g, me]
        loop(pieces, step)

    loop(crops, tri_end)

    def put_m(c):
        arrivals(3, c, lambda sender: rcv_b.at[c, sender])
        stg_m[...] = rcv_b[c].astype(F32).reshape(n * res * half, LANES)

        def step(idx):
            for s in idx:
                x2 = stg_m[pl.ds(s, n_res, stride=half), :].T
                m_out[c, s] = x2[:c_m].astype(BF16)
                m_out[c, s + half] = x2[c_m:].astype(BF16)
        grouped(half, 4, step)

    loop(crops, put_m)

    def put_z(c):
        take_columns(7, c, zback)

        def step(i):
            z_out[c, i] = xs[i].astype(BF16)
        for i in range(res):
            step(i)

    loop(crops, put_z)

    def drain(c):
        finish(gather_copies(0, c, ag_r))
        finish(swap_copies(1, c, snd_m, rcv_m))
        for g in range(pieces):
            for slot in range(n - 1):
                block_copy(c * pieces + g, me, device(1), slot).wait_send()
            finish(piece_copies(7, c, g, snd_y, zback))
            finish(piece_copies(10, c, g, snd_z, rcv_z))
        finish(swap_copies(3, c, snd_b, rcv_b))
        finish(gather_copies(4, c, ag_s))
        finish(gather_copies(5, c, ag_e))

    loop(crops, drain)


def solution(mesh):
    n = mesh.shape[GROUP_AXIS]
    rows_spec = P(PART_AXIS, GROUP_AXIS, None, None)
    in_specs = (rows_spec, rows_spec, P(PART_AXIS, None, None), P(PART_AXIS, None)) + (P(),) * N_WEIGHTS

    def local_block(m, z, msa_mask, res_mask, w_rb, w_rq, w_ro, w_cq, w_co, w_ac, w_oo, w_sb, w_sq, w_so,
                    w_eb, w_eq, w_eo):
        crops, seqs, n_res, c_m = m.shape
        res, c_z = z.shape[1], z.shape[3]
        heads_m, heads_z = w_rq.shape[2], w_sq.shape[2]
        o_w = w_ac.shape[2]
        half = seqs // 2
        assert n == 8 and crops == 2 and res % 3 == 0 and n * SLOT == LANES and res <= SLOT and n * seqs == LANES and 2 * c_m == LANES and c_z == LANES
        flat = lambda w: jnp.moveaxis(w, 0, -1).reshape(-1, w.shape[0])
        tall = lambda w: w.reshape(-1, w.shape[-1])
        args = (m.swapaxes(2, 3), z, msa_mask.swapaxes(1, 2), res_mask, w_rb.T, flat(w_rq), tall(w_ro), flat(w_cq),
                tall(w_co), flat(w_ac), tall(w_oo), w_sb.T, flat(w_sq), tall(w_so), w_eb.T, flat(w_eq), tall(w_eo))
        vm = pltpu.VMEM
        slots = max(seqs, res)
        pieces = 2
        piece = res * res // pieces
        scratch = [
            vm((crops, n, heads_m * res, LANES), BF16),
            vm((crops, pieces, n, res // pieces, o_w, LANES), BF16),
            vm((crops, n, heads_z * res, LANES), BF16),
            vm((crops, n, heads_z * res, LANES), BF16),
            vm((crops, n, res, half, LANES), BF16),
            vm((crops, n, res, half, LANES), BF16),
            vm((crops, n, res, half, LANES), BF16),
            vm((crops, n, res, half, LANES), BF16),
            vm((crops, pieces, n, piece, LANES), BF16),
            vm((crops, pieces, n, piece, LANES), BF16),
            vm((crops, pieces, n, piece, LANES), BF16),
            vm((crops, pieces, n, piece, LANES), BF16),
            pltpu.SemaphoreType.DMA((13, crops, n)),
            pltpu.SemaphoreType.DMA((13, crops, n)),
            pltpu.SemaphoreType.DMA((crops * pieces, n)),
            pltpu.SemaphoreType.DMA((crops * pieces, n)),
        ]
        local = [
            vm((crops, res, n_res, LANES), BF16),
            vm((crops * slots, c_m, LANES), F32),
            vm((crops * slots, LANES, LANES), BF16),
            vm((crops * slots, LANES, LANES), BF16),
            vm((crops * slots, LANES, LANES), BF16),
            vm((crops * slots, LANES, LANES), F32),
            vm((heads_m, n_res, LANES), F32),
            vm((res, o_w * o_w, LANES), BF16),
            vm((n * res * half, LANES), F32),
            vm((o_w * (n_res + 8), LANES), F32),
            vm((heads_m * res, LANES), F32),
            vm((n_res * res, LANES), F32),
            vm((crops, res * o_w, LANES), BF16),
            vm((crops, LANES, LANES), F32),
            vm((crops, n * seqs, LANES), F32),
            vm((crops, LANES), F32),
            vm((slots, heads_m // 2, LANES, 2 * LANES), F32),
            vm((slots, heads_m // 2, LANES, 2 * LANES), BF16),
            vm((slots, heads_m, LANES), F32),
            vm((SLOT, LANES), F32),
            vm((heads_m, c_m, LANES), BF16),
            vm((heads_z, c_z, LANES), BF16),
            vm((c_m, c_m), BF16),
            vm((c_m, c_m), BF16),
            vm((LANES, o_w * o_w), BF16),
            vm((3, SLOT, LANES), BF16),
            vm((AUG, LANES), F32),
            vm((AUG, 2 * LANES), BF16),
            vm((res, n_res, LANES), F32),
            vm((crops, LANES, LANES), BF16),
        ]
        cfg = dict(n=n, heads_m=heads_m, heads_z=heads_z, slots=slots, pieces=pieces, local=local)
        spec = pl.BlockSpec(memory_space=pltpu.VMEM)
        m_new, z_new = pl.pallas_call(
            functools.partial(body, cfg),
            out_shape=(jax.ShapeDtypeStruct((crops, seqs, c_m, n_res), BF16), jax.ShapeDtypeStruct(z.shape, BF16)),
            in_specs=[spec] * len(args),
            out_specs=(spec, spec),
            scratch_shapes=scratch,
            compiler_params=pltpu.CompilerParams(collective_id=0, has_side_effects=True,
                                                 vmem_limit_bytes=60 * 1024 * 1024),
        )(*args)
        return m_new.swapaxes(2, 3), z_new

    return jax.shard_map(local_block, mesh=mesh, in_specs=in_specs, out_specs=(rows_spec, rows_spec),
                         check_vma=False)
```

```python
import functools
import math

import jax
import jax.numpy as jnp
import numpy as np
from jax import lax
from jax.experimental import pallas as pl
from jax.experimental.pallas import tpu as pltpu
from jax.sharding import PartitionSpec as P

MASK_SCALE = 10000.0
LN_EPS = 1e-5
OPM_EPS = 1e-3
N_WEIGHTS = 13
PART_AXIS = 'data'
GROUP_AXIS = 'dap'
LOG2E = math.log2(math.e)
AUG = 16
LANES = 128
SLOT = 16
F32 = jnp.float32
BF16 = jnp.bfloat16
NN = (((1,), (0,)), ((), ()))
NT = (((1,), (1,)), ((), ()))
TN = (((0,), (0,)), ((), ()))


def mm(lhs, rhs, dims=NN):
    return lax.dot_general(lhs, rhs, dims, preferred_element_type=F32)


def layer_norm(x_float):
    mean_val = jnp.mean(x_float, axis=-1, keepdims=True)
    centred = x_float - mean_val
    var_val = jnp.mean(centred * centred, axis=-1, keepdims=True)
    return (centred * lax.rsqrt(var_val + LN_EPS)).astype(BF16)


def layer_norm_t(x_float):
    mean_val = jnp.mean(x_float, axis=0, keepdims=True)
    centred = x_float - mean_val
    var_val = jnp.mean(centred * centred, axis=0, keepdims=True)
    return (centred * lax.rsqrt(var_val + LN_EPS)).astype(BF16)


def iota(shape, axis):
    return lax.broadcasted_iota(jnp.int32, shape, axis)


def body(cfg, *refs):
    pl.run_scoped(functools.partial(scoped_body, cfg, refs), *cfg['local'])


def scoped_body(cfg, refs, *local):
    n = cfg['n']
    (m_in, z_in, mask_in, res_in, w_rb, wt_r, w_ro, wt_c, w_co, w_ac, w_oo,
     w_sb, wt_s, w_so, w_eb, wt_e, w_eo, m_out, z_out,
     ag_r, ag_c, ag_s, ag_e, snd_m, rcv_m, snd_b, rcv_b, snd_z, rcv_z, snd_y, zback, send_sem, recv_sem,
     ring_send, ring_recv) = refs
    (zw, xw, kbuf, qbuf, vbuf, gbuf, bias, obuf, stg_m, stg_c, stg_b, stg_z, abuf,
     mask_t, mask_r, res_r, raw, prob, inv, norm, hm8, hm4, wt_ro, wt_co, w_oo_t, wt_b, aug, one_rows, xs, mask_n) = local
    crops, seqs, c_m, n_res = m_in.shape
    res = z_in.shape[1]
    c_z = z_in.shape[3]
    half = seqs // 2
    heads_m, heads_z = cfg['heads_m'], cfg['heads_z']
    d_m, d_z = c_m // heads_m, c_z // heads_z
    n_seq = n * seqs
    slots, pieces = cfg['slots'], cfg['pieces']
    part_rows, n_blocks = res // pieces, crops * pieces
    me = lax.axis_index(GROUP_AXIS)

    barrier = pltpu.get_barrier_semaphore()
    for r in range(1, n):
        pl.semaphore_signal(barrier, inc=1, device_id={GROUP_AXIS: lax.rem(me + r, n)},
                            device_id_type=pl.DeviceIdType.MESH)

    def copies(exch, c, src_of, dst):
        out = []
        for r in range(1, n):
            peer = lax.rem(me + r, n)
            out.append(pltpu.make_async_remote_copy(
                src_ref=src_of(peer), dst_ref=dst, send_sem=send_sem.at[exch, c, r], recv_sem=recv_sem.at[exch, c, r],
                device_id={GROUP_AXIS: peer}, device_id_type=pl.DeviceIdType.MESH))
        return out

    def arrivals(exch, c, slot_of):
        for r in range(1, n):
            sender = lax.rem(me + n - r, n)
            ref = slot_of(sender)
            pltpu.make_async_remote_copy(
                src_ref=ref, dst_ref=ref, send_sem=send_sem.at[exch, c, r], recv_sem=recv_sem.at[exch, c, r],
                device_id={GROUP_AXIS: sender}, device_id_type=pl.DeviceIdType.MESH).wait_recv()

    def gather_copies(exch, c, buf):
        return copies(exch, c, lambda peer: buf.at[c, me], buf.at[c, me])

    def gather_wait(exch, c, buf):
        arrivals(exch, c, lambda sender: buf.at[c, sender])

    def swap_copies(exch, c, snd, rcv):
        return copies(exch, c, lambda peer: snd.at[c, peer], rcv.at[c, me])

    chips, core, chip = n // 2, lax.rem(me, 2), me // 2

    def device(offset, other=False):
        return lax.rem(chip + offset + chips, chips) * 2 + ((1 - core) if other else core)

    def block_copy(k, block, peer, slot):
        c, g = k // pieces, lax.rem(k, pieces)
        return pltpu.make_async_remote_copy(
            src_ref=ag_c.at[c, g, block], dst_ref=ag_c.at[c, g, block], send_sem=ring_send.at[k, slot],
            recv_sem=ring_recv.at[k, block], device_id={GROUP_AXIS: peer}, device_id_type=pl.DeviceIdType.MESH)

    def block_wait(k, block):
        block_copy(k, block, block, 0).wait_recv()

    def relay_own(k):
        for slot in range(chips):
            block_copy(k, me, device(slot, slot == 0), slot).start()

    def relay(k):
        for offset in range(1, chips):
            block_wait(k, device(offset))
        for offset in range(1, chips):
            block_copy(k, device(offset), device(0, True), chips - 1 + offset).start()

    def relay_done(k):
        for offset in range(chips):
            block_wait(k, device(offset, True))

    def start(descs):
        for d in descs:
            d.start()

    def finish(descs):
        for d in descs:
            d.wait_send()

    def loop(count, fn):
        def step(i, carry):
            fn(i)
            return carry
        lax.fori_loop(0, count, step, 0)

    def pad_matrix():
        row, col = iota((LANES, n_res), 0), iota((LANES, n_res), 1)
        hit = (col == (row // SLOT) * res + row % SLOT) & (row % SLOT < res)
        return jnp.where(hit, 1.0, 0.0).astype(BF16)

    def head_rows(heads, width, ref):
        for h in range(heads):
            row = iota((heads * width, LANES), 0)
            ref[h] = jnp.where((row >= h * width) & (row < (h + 1) * width), 1.0, 0.0).astype(BF16)

    pad = pad_matrix()
    tail = jnp.where(iota((n_res, LANES), 0) == iota((n_res, LANES), 1), 1.0, 0.0).astype(BF16)
    head_rows(heads_m, d_m, hm8)
    head_rows(heads_z, d_z, hm4)
    row, col = iota((LANES, LANES), 0), iota((LANES, LANES), 1)
    seq_of = ((col % (n_seq // 2)) // half) * seqs + (col // (n_seq // 2)) * half + col % half
    seq_perm = jnp.where(row == seq_of, 1.0, 0.0).astype(BF16)
    for c in range(crops):
        mask_bf = mask_in[c].astype(F32).astype(BF16)
        mask_t[c] = mm(mm(pad, mask_bf).astype(BF16), seq_perm)
        mask_n[c, :n_res] = mm(mask_bf, seq_perm).astype(BF16)
        mask_n[c, n_res:] = jnp.zeros((LANES - n_res, LANES), BF16)
        mask_r[c] = mm(mask_bf, tail, TN)
    res_r[...] = mm(res_in[...].astype(F32).astype(BF16), tail)
    term = MASK_SCALE * d_m ** 0.5
    aug[...] = jnp.zeros(aug.shape, F32)
    ones = jnp.zeros((AUG, 2 * LANES), F32)
    for k in range(3):
        piece = float(np.array(term, dtype=BF16))
        term = term - piece
        aug[k:k + 1, :] = jnp.full((1, LANES), piece, F32)
        ones = jnp.where(iota(ones.shape, 0) == k, 1.0, ones)
    one_rows[...] = ones.astype(BF16)
    for k, w in enumerate((w_rb, w_sb, w_eb)):
        wt_b[k] = jnp.zeros(wt_b.shape[1:], BF16)
        wt_b[k, :w.shape[0], :] = w[...]
    wt_ro[...] = w_ro[...].astype(F32).T.astype(BF16)
    wt_co[...] = w_co[...].astype(F32).T.astype(BF16)
    o_w = w_ac.shape[0] // 2
    stg_z[:o_w * o_w, :] = w_oo[...].astype(F32)
    for k in range(0, o_w, LANES // o_w):
        rows = [stg_z[pl.ds(f, o_w, stride=o_w), :] for f in range(k, k + LANES // o_w)]
        w_oo_t[:, k * o_w:k * o_w + LANES] = jnp.concatenate(rows, axis=0).T.astype(BF16)

    stg_b[...] = jnp.zeros(stg_b.shape, F32)

    def grouped(count, size, fn):
        while count % size:
            size -= 1

        def step(b, carry):
            fn([b * size + t for t in range(size)])
            return carry
        lax.fori_loop(0, count // size, step, 0)

    def put_bias(y, k, heads, rows):
        b = mm(wt_b[k], y, NT)
        for t, i in enumerate(rows):
            for h in range(heads):
                stg_b[pl.ds(h * res + i, 1), :] = b[h:h + 1, t * LANES:(t + 1) * LANES]

    def stack(ys):
        fill = jnp.zeros((LANES - n_res, ys[0].shape[1]), BF16)
        return jnp.concatenate([part for y in ys for part in (y, fill)], axis=0)

    def keep(p, width, slots, length, mask_rows=None):
        for t, slot in enumerate(slots):
            part = slice(t * LANES, (t + 1) * LANES)
            keys = p[width:2 * width, part]
            if mask_rows is not None:
                keys = jnp.concatenate([keys, (mask_rows[t] - 1.0) * aug[...]], axis=0)
            qbuf[slot, :width] = p[:width, part].astype(BF16)
            kbuf[slot, :length, :keys.shape[0]] = keys.T[:length].astype(BF16)
            vbuf[slot, :width] = p[2 * width:3 * width, part].astype(BF16)
            gbuf[slot, :width] = jax.nn.sigmoid(p[3 * width:, part])

    def column(rowvec):
        return jnp.broadcast_to(rowvec, (LANES, LANES)).T[:n_res]

    def gathered_bias(buf, c, heads, width, flip, add):
        parts = [buf[c, p].astype(F32) for p in range(n)]
        for h in range(heads):
            b = jnp.concatenate([part[h * res:(h + 1) * res] for part in parts], axis=0)
            if flip:
                b = jnp.concatenate([b, jnp.zeros((LANES - n_res, LANES), F32)], axis=0).T[:n_res]
            b = b * width ** 0.5
            bias[h] = b if add is None else b + add

    def logits(idx, base, heads, width, head_mask, length, masked):
        c = heads * width
        for i in idx:
            q_t, keys = qbuf[base + i, :c], kbuf[base + i, :length, :c + (AUG if masked else 0)]
            for pair in range(heads // 2):
                rhs = jnp.concatenate([q_t * head_mask[2 * pair], q_t * head_mask[2 * pair + 1]], axis=1)
                if masked:
                    rhs = jnp.concatenate([rhs, one_rows[...]], axis=0)
                raw[i, pair, :length] = mm(keys, rhs)

    def softmax(idx, heads, width, length, biased):
        scale2 = LOG2E * width ** -0.5
        for i in idx:
            for h in range(heads):
                part = slice((h % 2) * LANES, (h % 2 + 1) * LANES)
                x = raw[i, h // 2, :length, part]
                if biased:
                    x = x + bias[h]
                e = jnp.exp2((x - jnp.max(x, axis=0, keepdims=True)) * scale2)
                inv[i, h:h + 1, :] = 1.0 / jnp.sum(e, axis=0, keepdims=True)
                prob[i, h // 2, :length, part] = e.astype(BF16)

    def mixed(idx, base, heads, width, length):
        c = heads * width
        raws = [[mm(vbuf[base + i, 2 * p * width:2 * (p + 1) * width, :length], prob[i, p, :length])
                 for p in range(heads // 2)] for i in idx]
        outs = []
        for i, r in zip(idx, raws):
            parts = []
            for p in range(heads // 2):
                parts.append(r[p][:width, :LANES] * inv[i, 2 * p:2 * p + 1, :])
                parts.append(r[p][width:, LANES:] * inv[i, 2 * p + 1:2 * p + 2, :])
            outs.append((jnp.concatenate(parts, axis=0) * gbuf[base + i, :c]).astype(BF16))
        return outs

    pl.semaphore_wait(barrier, n - 1)

    def row_bias(c):
        def step(idx):
            put_bias(stack([layer_norm(z_in[c, i].astype(F32)) for i in idx]), 0, heads_m, idx)
        grouped(res, 12, step)
        ag_r[c, me] = stg_b[...].astype(BF16)
        start(gather_copies(0, c, ag_r))

    loop(crops, row_bias)

    def row_prep(c):
        def prep(idx):
            fill = jnp.zeros((c_m, LANES - n_res), F32)
            ms = [jnp.concatenate([m_in[c, s].astype(F32), fill], axis=1) for s in idx]
            keep(mm(wt_r[...], jnp.concatenate([layer_norm_t(x) for x in ms], axis=1)), c_m,
                 [c * slots + s for s in idx], n_res, [mask_r[c, pl.ds(me * seqs + s, 1), :] for s in idx])
            for s, x in zip(idx, ms):
                xw[c * slots + s] = x
        grouped(seqs, 8, prep)

    loop(crops, row_prep)

    def row_attention(c):
        base = c * slots
        grouped(seqs, 8, lambda idx: logits(idx, base, heads_m, d_m, hm8, n_res, True))
        gather_wait(0, c, ag_r)
        gathered_bias(ag_r, c, heads_m, d_m, True, None)
        grouped(seqs, 4, lambda idx: softmax(idx, heads_m, d_m, n_res, True))

        def step(idx):
            both = [s + t * half for s in idx for t in range(2)]
            upd = mm(wt_ro[...], jnp.concatenate(mixed(both, base, heads_m, d_m, n_res), axis=1))
            new = [xw[base + s] + upd[:, t * LANES:(t + 1) * LANES] for t, s in enumerate(both)]
            for k, s in enumerate(idx):
                x2 = jnp.concatenate(new[2 * k:2 * k + 2], axis=0).T
                stg_m[pl.ds(s, n_res, stride=half), :] = x2[:n_res]
        grouped(half, 8, step)
        for p in range(n):
            snd_m[c, p] = stg_m[p * res * half:(p + 1) * res * half, :].reshape(res, half, LANES).astype(BF16)
        rcv_m[c, me] = snd_m[c, me]
        start(swap_copies(1, c, snd_m, rcv_m))

    loop(crops, row_attention)

    def col_attention(c):
        base = c * slots
        arrivals(1, c, lambda sender: rcv_m.at[c, sender])
        hs = n_seq // 2

        def mask_row(i):
            return mask_t[c, pl.ds(me * SLOT + i, 1), :]

        def prep(idx):
            ys = []
            for k in range(0, len(idx), 2):
                x2 = jnp.concatenate([rcv_m[c, q, i].astype(F32) for i in idx[k:k + 2] for q in range(n)], axis=0).T
                for t, i in enumerate(idx[k:k + 2]):
                    x = jnp.concatenate([x2[:c_m, t * hs:(t + 1) * hs], x2[c_m:, t * hs:(t + 1) * hs]], axis=1)
                    xw[base + i] = x
                    ys.append(layer_norm_t(x))
            keep(mm(wt_c[...], jnp.concatenate(ys, axis=1)), c_m, [base + i for i in idx], LANES,
                 [mask_row(i) for i in idx])
        grouped(res, 6, prep)

        def group(g):
            idx = [g * part_rows + t for t in range(part_rows)]
            logits(idx, base, heads_m, d_m, hm8, LANES, True)
            softmax(idx, heads_m, d_m, LANES, False)
            upd = mm(wt_co[...], jnp.concatenate(mixed(idx, base, heads_m, d_m, LANES), axis=1))
            new = [(xw[base + i] + upd[:, t * LANES:(t + 1) * LANES]).astype(BF16).astype(F32)
                   for t, i in enumerate(idx)]
            ac = mm(w_ac[...], jnp.concatenate([layer_norm_t(x) for x in new], axis=1)).astype(BF16).astype(F32)
            for t, i in enumerate(idx):
                part = ac[:, t * LANES:(t + 1) * LANES] * mask_row(i)
                ag_c[c, g, me, t] = part[o_w:].astype(BF16)
                abuf[c, pl.ds(pl.multiple_of(i * o_w, o_w), o_w), :] = part[:o_w].astype(BF16)
            k = c * pieces + g
            relay_own(k)

            @pl.when(k >= 2)
            def _():
                relay(k - 2)

            for t in range(0, part_rows, 2):
                two = jnp.concatenate([
                    jnp.concatenate([x[:, :hs] for x in new[t:t + 2]], axis=1),
                    jnp.concatenate([x[:, hs:] for x in new[t:t + 2]], axis=1)], axis=0).T
                for u, i in enumerate(idx[t:t + 2]):
                    for q in range(n):
                        snd_b[c, q, i] = two[u * hs + q * half:u * hs + (q + 1) * half].astype(BF16)
        loop(pieces, group)
        rcv_b[c, me] = snd_b[c, me]

    loop(crops, col_attention)

    def outer_product(c):
        base = c * slots
        mloc = mask_t[c, pl.ds(pl.multiple_of(me * SLOT, SLOT), SLOT), :].astype(BF16)
        norm[...] = 1.0 / (mm(mloc, mask_n[c], NT) + OPM_EPS)
        pitch = n_res + 8

        for g in range(pieces):
            relay_done(c * pieces + g)

            def spread(p):
                for t in range(part_rows):
                    stg_c[pl.ds(p * res + g * part_rows + t, o_w, stride=pitch), :] = ag_c[c, g, p, t].astype(F32)
            loop(n, spread)


        def outer(fs):
            rows = [stg_c[pl.ds(pl.multiple_of(f * pitch, 8), n_res), :].astype(BF16) for f in fs]
            outs = [mm(abuf[c], stack(rows[k:k + 2]), NT) for k in range(0, len(fs), 2)]
            for k, f in enumerate(fs):
                out = outs[k // 2][:, (k % 2) * LANES:(k % 2 + 1) * LANES]
                for i in range(res):
                    obuf[i, pl.ds(pl.multiple_of(f * o_w, o_w), o_w), :] = (
                        out[i * o_w:(i + 1) * o_w] * norm[i:i + 1, :]).astype(BF16)
        grouped(o_w, 16, outer)

        @pl.when(c == 0)
        def _():
            relay(n_blocks - 2)

        start(swap_copies(3, c, snd_b, rcv_b))

        def update(idx):
            rhs = [jnp.concatenate([obuf[i] for i in idx[k:k + 2]], axis=1) for k in range(0, len(idx), 2)]
            upds = [mm(w_oo_t[...], r) for r in rhs]
            for k, i in enumerate(idx):
                upd = upds[k // 2][:, (k % 2) * LANES:(k % 2 + 1) * LANES].T
                zw[c, i] = (z_in[c, i].astype(F32) + upd[:n_res]).astype(BF16)
        grouped(res, 12, update)

        def prep(idx):
            y = stack([layer_norm(zw[c, i].astype(F32)) for i in idx])
            put_bias(y, 1, heads_z, idx)
            keep(mm(wt_s[...], y, NT), c_z, [base + i for i in idx], n_res)
        grouped(res, 12, prep)
        @pl.when(c == 0)
        def _():
            relay(n_blocks - 1)

        ag_s[c, me] = stg_b[:heads_z * res, :].astype(BF16)
        start(gather_copies(4, c, ag_s))

    loop(crops, outer_product)

    def res_bias(c):
        return column((res_r[pl.ds(c, 1), :] - 1.0) * (MASK_SCALE * d_z ** 0.5))

    def piece_copies(first, c, g, snd, rcv):
        return copies(first + g, c, lambda peer: snd.at[c, g, peer], rcv.at[c, g, me])

    def send_rows(zs, snd, c, g):
        for t, z in enumerate(zs):
            stg_m[pl.ds(t, n_res, stride=part_rows), :] = z
        size = res * part_rows
        for q in range(n):
            snd[c, g, q] = stg_m[q * size:(q + 1) * size, :].astype(BF16)

    def take_columns(first, c, rcv):
        for g in range(pieces):
            arrivals(first + g, c, lambda sender: rcv.at[c, g, sender])
        for p in range(n):
            for g in range(pieces):
                block = rcv[c, g, p].astype(F32)
                row0 = p * res + g * part_rows
                for j in range(res):
                    xs[j, row0:row0 + part_rows, :] = block[j * part_rows:(j + 1) * part_rows]

    def tri_start(c):
        base = c * slots
        gather_wait(4, c, ag_s)
        gathered_bias(ag_s, c, heads_z, d_z, True, res_bias(c))
        stg_b[...] = jnp.zeros(stg_b.shape, F32)

        def group(g):
            idx = [g * part_rows + t for t in range(part_rows)]
            logits(idx, base, heads_z, d_z, hm4, n_res, False)
            softmax(idx, heads_z, d_z, n_res, True)
            upds = [mm(o, w_so[...], TN) for o in mixed(idx, base, heads_z, d_z, n_res)]
            zs = [(zw[c, i].astype(F32) + upd[:n_res]).astype(BF16).astype(F32) for i, upd in zip(idx, upds)]
            send_rows(zs, snd_z, c, g)
            start(piece_copies(10, c, g, snd_z, rcv_z))
            rcv_z[c, g, me] = snd_z[c, g, me]
            put_bias(stack([layer_norm(z) for z in zs]), 2, heads_z, idx)
        loop(pieces, group)
        ag_e[c, me] = stg_b[:heads_z * res, :].astype(BF16)
        start(gather_copies(5, c, ag_e))

    loop(crops, tri_start)

    def tri_end(c):
        base = c * slots
        take_columns(10, c, rcv_z)

        def prep(idx):
            keep(mm(wt_e[...], stack([layer_norm(xs[j]) for j in idx]), NT), c_z, [base + j for j in idx], n_res)
        grouped(res, 12, prep)
        gather_wait(5, c, ag_e)
        gathered_bias(ag_e, c, heads_z, d_z, False, res_bias(c))

        def step(g):
            idx = [g * part_rows + t for t in range(part_rows)]
            logits(idx, base, heads_z, d_z, hm4, n_res, False)
            softmax(idx, heads_z, d_z, n_res, True)
            upds = [mm(o, w_eo[...], TN) for o in mixed(idx, base, heads_z, d_z, n_res)]
            send_rows([xs[j] + upd[:n_res] for j, upd in zip(idx, upds)], snd_y, c, g)
            start(piece_copies(7, c, g, snd_y, zback))
            zback[c, g, me] = snd_y[c, g, me]
        loop(pieces, step)

    loop(crops, tri_end)

    def put_m(c):
        arrivals(3, c, lambda sender: rcv_b.at[c, sender])
        stg_m[...] = rcv_b[c].astype(F32).reshape(n * res * half, LANES)

        def step(idx):
            for s in idx:
                x2 = stg_m[pl.ds(s, n_res, stride=half), :].T
                m_out[c, s] = x2[:c_m].astype(BF16)
                m_out[c, s + half] = x2[c_m:].astype(BF16)
        grouped(half, 4, step)

    loop(crops, put_m)

    def put_z(c):
        take_columns(7, c, zback)

        def step(i):
            z_out[c, i] = xs[i].astype(BF16)
        for i in range(res):
            step(i)

    loop(crops, put_z)

    def drain(c):
        finish(gather_copies(0, c, ag_r))
        finish(swap_copies(1, c, snd_m, rcv_m))
        for g in range(pieces):
            for slot in range(n - 1):
                block_copy(c * pieces + g, me, device(1), slot).wait_send()
            finish(piece_copies(7, c, g, snd_y, zback))
            finish(piece_copies(10, c, g, snd_z, rcv_z))
        finish(swap_copies(3, c, snd_b, rcv_b))
        finish(gather_copies(4, c, ag_s))
        finish(gather_copies(5, c, ag_e))

    loop(crops, drain)


def solution(mesh):
    n = mesh.shape[GROUP_AXIS]
    rows_spec = P(PART_AXIS, GROUP_AXIS, None, None)
    in_specs = (rows_spec, rows_spec, P(PART_AXIS, None, None), P(PART_AXIS, None)) + (P(),) * N_WEIGHTS

    def local_block(m, z, msa_mask, res_mask, w_rb, w_rq, w_ro, w_cq, w_co, w_ac, w_oo, w_sb, w_sq, w_so,
                    w_eb, w_eq, w_eo):
        crops, seqs, n_res, c_m = m.shape
        res, c_z = z.shape[1], z.shape[3]
        heads_m, heads_z = w_rq.shape[2], w_sq.shape[2]
        o_w = w_ac.shape[2]
        half = seqs // 2
        assert n == 8 and crops == 2 and res % 3 == 0 and n * SLOT == LANES and res <= SLOT and n * seqs == LANES and 2 * c_m == LANES and c_z == LANES
        flat = lambda w: jnp.moveaxis(w, 0, -1).reshape(-1, w.shape[0])
        tall = lambda w: w.reshape(-1, w.shape[-1])
        args = (m.swapaxes(2, 3), z, msa_mask.swapaxes(1, 2), res_mask, w_rb.T, flat(w_rq), tall(w_ro), flat(w_cq),
                tall(w_co), flat(w_ac), tall(w_oo), w_sb.T, flat(w_sq), tall(w_so), w_eb.T, flat(w_eq), tall(w_eo))
        vm = pltpu.VMEM
        slots = max(seqs, res)
        pieces = 2
        piece = res * res // pieces
        scratch = [
            vm((crops, n, heads_m * res, LANES), BF16),
            vm((crops, pieces, n, res // pieces, o_w, LANES), BF16),
            vm((crops, n, heads_z * res, LANES), BF16),
            vm((crops, n, heads_z * res, LANES), BF16),
            vm((crops, n, res, half, LANES), BF16),
            vm((crops, n, res, half, LANES), BF16),
            vm((crops, n, res, half, LANES), BF16),
            vm((crops, n, res, half, LANES), BF16),
            vm((crops, pieces, n, piece, LANES), BF16),
            vm((crops, pieces, n, piece, LANES), BF16),
            vm((crops, pieces, n, piece, LANES), BF16),
            vm((crops, pieces, n, piece, LANES), BF16),
            pltpu.SemaphoreType.DMA((13, crops, n)),
            pltpu.SemaphoreType.DMA((13, crops, n)),
            pltpu.SemaphoreType.DMA((crops * pieces, n)),
            pltpu.SemaphoreType.DMA((crops * pieces, n)),
        ]
        local = [
            vm((crops, res, n_res, LANES), BF16),
            vm((crops * slots, c_m, LANES), F32),
            vm((crops * slots, LANES, LANES), BF16),
            vm((crops * slots, LANES, LANES), BF16),
            vm((crops * slots, LANES, LANES), BF16),
            vm((crops * slots, LANES, LANES), F32),
            vm((heads_m, n_res, LANES), F32),
            vm((res, o_w * o_w, LANES), BF16),
            vm((n * res * half, LANES), F32),
            vm((o_w * (n_res + 8), LANES), F32),
            vm((heads_m * res, LANES), F32),
            vm((n_res * res, LANES), F32),
            vm((crops, res * o_w, LANES), BF16),
            vm((crops, LANES, LANES), F32),
            vm((crops, n * seqs, LANES), F32),
            vm((crops, LANES), F32),
            vm((slots, heads_m // 2, LANES, 2 * LANES), F32),
            vm((slots, heads_m // 2, LANES, 2 * LANES), BF16),
            vm((slots, heads_m, LANES), F32),
            vm((SLOT, LANES), F32),
            vm((heads_m, c_m, LANES), BF16),
            vm((heads_z, c_z, LANES), BF16),
            vm((c_m, c_m), BF16),
            vm((c_m, c_m), BF16),
            vm((LANES, o_w * o_w), BF16),
            vm((3, SLOT, LANES), BF16),
            vm((AUG, LANES), F32),
            vm((AUG, 2 * LANES), BF16),
            vm((res, n_res, LANES), F32),
            vm((crops, LANES, LANES), BF16),
        ]
        cfg = dict(n=n, heads_m=heads_m, heads_z=heads_z, slots=slots, pieces=pieces, local=local)
        spec = pl.BlockSpec(memory_space=pltpu.VMEM)
        m_new, z_new = pl.pallas_call(
            functools.partial(body, cfg),
            out_shape=(jax.ShapeDtypeStruct((crops, seqs, c_m, n_res), BF16), jax.ShapeDtypeStruct(z.shape, BF16)),
            in_specs=[spec] * len(args),
            out_specs=(spec, spec),
            scratch_shapes=scratch,
            compiler_params=pltpu.CompilerParams(collective_id=0, has_side_effects=True,
                                                 vmem_limit_bytes=60 * 1024 * 1024),
        )(*args)
        return m_new.swapaxes(2, 3), z_new

    return jax.shard_map(local_block, mesh=mesh, in_specs=in_specs, out_specs=(rows_spec, rows_spec),
                         check_vma=False)
```

```python
import functools
import math

import jax
import jax.numpy as jnp
import numpy as np
from jax import lax
from jax.experimental import pallas as pl
from jax.experimental.pallas import tpu as pltpu
from jax.sharding import PartitionSpec as P

MASK_SCALE = 10000.0
LN_EPS = 1e-5
OPM_EPS = 1e-3
N_WEIGHTS = 13
PART_AXIS = 'data'
GROUP_AXIS = 'dap'
LOG2E = math.log2(math.e)
AUG = 16
LANES = 128
SLOT = 16
F32 = jnp.float32
BF16 = jnp.bfloat16
NN = (((1,), (0,)), ((), ()))
NT = (((1,), (1,)), ((), ()))
TN = (((0,), (0,)), ((), ()))


def mm(lhs, rhs, dims=NN):
    return lax.dot_general(lhs, rhs, dims, preferred_element_type=F32)


def layer_norm(x_float):
    mean_val = jnp.mean(x_float, axis=-1, keepdims=True)
    centred = x_float - mean_val
    var_val = jnp.mean(centred * centred, axis=-1, keepdims=True)
    return (centred * lax.rsqrt(var_val + LN_EPS)).astype(BF16)


def layer_norm_t(x_float):
    mean_val = jnp.mean(x_float, axis=0, keepdims=True)
    centred = x_float - mean_val
    var_val = jnp.mean(centred * centred, axis=0, keepdims=True)
    return (centred * lax.rsqrt(var_val + LN_EPS)).astype(BF16)


def iota(shape, axis):
    return lax.broadcasted_iota(jnp.int32, shape, axis)


def body(cfg, *refs):
    pl.run_scoped(functools.partial(scoped_body, cfg, refs), *cfg['local'])


def scoped_body(cfg, refs, *local):
    n = cfg['n']
    (m_in, z_in, mask_in, res_in, w_rb, wt_r, w_ro, wt_c, w_co, w_ac, w_oo,
     w_sb, wt_s, w_so, w_eb, wt_e, w_eo, m_out, z_out,
     ag_r, ag_c, ag_s, ag_e, snd_m, rcv_m, snd_b, rcv_b, snd_z, rcv_z, snd_y, zback, send_sem, recv_sem,
     ring_send, ring_recv) = refs
    (zw, xw, kbuf, qbuf, vbuf, gbuf, bias, obuf, stg_m, stg_c, stg_b, stg_z, abuf,
     mask_t, mask_r, res_r, raw, prob, inv, norm, hm8, hm4, wt_ro, wt_co, w_oo_t, wt_b, aug, one_rows, xs, mask_n) = local
    crops, seqs, c_m, n_res = m_in.shape
    res = z_in.shape[1]
    c_z = z_in.shape[3]
    half = seqs // 2
    heads_m, heads_z = cfg['heads_m'], cfg['heads_z']
    d_m, d_z = c_m // heads_m, c_z // heads_z
    n_seq = n * seqs
    slots, pieces = cfg['slots'], cfg['pieces']
    part_rows, n_blocks = res // pieces, crops * pieces
    me = lax.axis_index(GROUP_AXIS)

    barrier = pltpu.get_barrier_semaphore()
    for r in range(1, n):
        pl.semaphore_signal(barrier, inc=1, device_id={GROUP_AXIS: lax.rem(me + r, n)},
                            device_id_type=pl.DeviceIdType.MESH)

    def copies(exch, c, src_of, dst):
        out = []
        for r in range(1, n):
            peer = lax.rem(me + r, n)
            out.append(pltpu.make_async_remote_copy(
                src_ref=src_of(peer), dst_ref=dst, send_sem=send_sem.at[exch, c, r], recv_sem=recv_sem.at[exch, c, r],
                device_id={GROUP_AXIS: peer}, device_id_type=pl.DeviceIdType.MESH))
        return out

    def arrivals(exch, c, slot_of):
        for r in range(1, n):
            sender = lax.rem(me + n - r, n)
            ref = slot_of(sender)
            pltpu.make_async_remote_copy(
                src_ref=ref, dst_ref=ref, send_sem=send_sem.at[exch, c, r], recv_sem=recv_sem.at[exch, c, r],
                device_id={GROUP_AXIS: sender}, device_id_type=pl.DeviceIdType.MESH).wait_recv()

    def gather_copies(exch, c, buf):
        return copies(exch, c, lambda peer: buf.at[c, me], buf.at[c, me])

    def gather_wait(exch, c, buf):
        arrivals(exch, c, lambda sender: buf.at[c, sender])

    def swap_copies(exch, c, snd, rcv):
        return copies(exch, c, lambda peer: snd.at[c, peer], rcv.at[c, me])

    chips, core, chip = n // 2, lax.rem(me, 2), me // 2

    def device(offset, other=False):
        return lax.rem(chip + offset + chips, chips) * 2 + ((1 - core) if other else core)

    def block_copy(k, block, peer, slot):
        c, g = k // pieces, lax.rem(k, pieces)
        return pltpu.make_async_remote_copy(
            src_ref=ag_c.at[c, g, block], dst_ref=ag_c.at[c, g, block], send_sem=ring_send.at[k, slot],
            recv_sem=ring_recv.at[k, block], device_id={GROUP_AXIS: peer}, device_id_type=pl.DeviceIdType.MESH)

    def block_wait(k, block):
        block_copy(k, block, block, 0).wait_recv()

    def relay_own(k):
        for slot in range(chips):
            block_copy(k, me, device(slot, slot == 0), slot).start()

    def relay(k):
        for offset in range(1, chips):
            block_wait(k, device(offset))
        for offset in range(1, chips):
            block_copy(k, device(offset), device(0, True), chips - 1 + offset).start()

    def relay_done(k):
        for offset in range(chips):
            block_wait(k, device(offset, True))

    def start(descs):
        for d in descs:
            d.start()

    def finish(descs):
        for d in descs:
            d.wait_send()

    def loop(count, fn):
        def step(i, carry):
            fn(i)
            return carry
        lax.fori_loop(0, count, step, 0)

    def pad_matrix():
        row, col = iota((LANES, n_res), 0), iota((LANES, n_res), 1)
        hit = (col == (row // SLOT) * res + row % SLOT) & (row % SLOT < res)
        return jnp.where(hit, 1.0, 0.0).astype(BF16)

    def head_rows(heads, width, ref):
        for h in range(heads):
            row = iota((heads * width, LANES), 0)
            ref[h] = jnp.where((row >= h * width) & (row < (h + 1) * width), 1.0, 0.0).astype(BF16)

    pad = pad_matrix()
    tail = jnp.where(iota((n_res, LANES), 0) == iota((n_res, LANES), 1), 1.0, 0.0).astype(BF16)
    head_rows(heads_m, d_m, hm8)
    head_rows(heads_z, d_z, hm4)
    row, col = iota((LANES, LANES), 0), iota((LANES, LANES), 1)
    seq_of = ((col % (n_seq // 2)) // half) * seqs + (col // (n_seq // 2)) * half + col % half
    seq_perm = jnp.where(row == seq_of, 1.0, 0.0).astype(BF16)
    for c in range(crops):
        mask_bf = mask_in[c].astype(F32).astype(BF16)
        mask_t[c] = mm(mm(pad, mask_bf).astype(BF16), seq_perm)
        mask_n[c, :n_res] = mm(mask_bf, seq_perm).astype(BF16)
        mask_n[c, n_res:] = jnp.zeros((LANES - n_res, LANES), BF16)
        mask_r[c] = mm(mask_bf, tail, TN)
    res_r[...] = mm(res_in[...].astype(F32).astype(BF16), tail)
    term = MASK_SCALE * d_m ** 0.5
    aug[...] = jnp.zeros(aug.shape, F32)
    ones = jnp.zeros((AUG, 2 * LANES), F32)
    for k in range(3):
        piece = float(np.array(term, dtype=BF16))
        term = term - piece
        aug[k:k + 1, :] = jnp.full((1, LANES), piece, F32)
        ones = jnp.where(iota(ones.shape, 0) == k, 1.0, ones)
    one_rows[...] = ones.astype(BF16)
    for k, w in enumerate((w_rb, w_sb, w_eb)):
        wt_b[k] = jnp.zeros(wt_b.shape[1:], BF16)
        wt_b[k, :w.shape[0], :] = w[...]
    wt_ro[...] = w_ro[...].astype(F32).T.astype(BF16)
    wt_co[...] = w_co[...].astype(F32).T.astype(BF16)
    o_w = w_ac.shape[0] // 2
    stg_z[:o_w * o_w, :] = w_oo[...].astype(F32)
    for k in range(0, o_w, LANES // o_w):
        rows = [stg_z[pl.ds(f, o_w, stride=o_w), :] for f in range(k, k + LANES // o_w)]
        w_oo_t[:, k * o_w:k * o_w + LANES] = jnp.concatenate(rows, axis=0).T.astype(BF16)

    stg_b[...] = jnp.zeros(stg_b.shape, F32)

    def grouped(count, size, fn):
        while count % size:
            size -= 1

        def step(b, carry):
            fn([b * size + t for t in range(size)])
            return carry
        lax.fori_loop(0, count // size, step, 0)

    def put_bias(y, k, heads, rows):
        b = mm(wt_b[k], y, NT)
        for t, i in enumerate(rows):
            for h in range(heads):
                stg_b[pl.ds(h * res + i, 1), :] = b[h:h + 1, t * LANES:(t + 1) * LANES]

    def stack(ys):
        fill = jnp.zeros((LANES - n_res, ys[0].shape[1]), BF16)
        return jnp.concatenate([part for y in ys for part in (y, fill)], axis=0)

    def keep(p, width, slots, length, mask_rows=None):
        for t, slot in enumerate(slots):
            part = slice(t * LANES, (t + 1) * LANES)
            keys = p[width:2 * width, part]
            if mask_rows is not None:
                keys = jnp.concatenate([keys, (mask_rows[t] - 1.0) * aug[...]], axis=0)
            qbuf[slot, :width] = p[:width, part].astype(BF16)
            kbuf[slot, :length, :keys.shape[0]] = keys.T[:length].astype(BF16)
            vbuf[slot, :width] = p[2 * width:3 * width, part].astype(BF16)
            gbuf[slot, :width] = jax.nn.sigmoid(p[3 * width:, part])

    def column(rowvec):
        return jnp.broadcast_to(rowvec, (LANES, LANES)).T[:n_res]

    def gathered_bias(buf, c, heads, width, flip, add):
        parts = [buf[c, p].astype(F32) for p in range(n)]
        for h in range(heads):
            b = jnp.concatenate([part[h * res:(h + 1) * res] for part in parts], axis=0)
            if flip:
                b = jnp.concatenate([b, jnp.zeros((LANES - n_res, LANES), F32)], axis=0).T[:n_res]
            b = b * width ** 0.5
            bias[h] = b if add is None else b + add

    def logits(idx, base, heads, width, head_mask, length, masked):
        c = heads * width
        for i in idx:
            q_t, keys = qbuf[base + i, :c], kbuf[base + i, :length, :c + (AUG if masked else 0)]
            for pair in range(heads // 2):
                rhs = jnp.concatenate([q_t * head_mask[2 * pair], q_t * head_mask[2 * pair + 1]], axis=1)
                if masked:
                    rhs = jnp.concatenate([rhs, one_rows[...]], axis=0)
                raw[i, pair, :length] = mm(keys, rhs)

    def softmax(idx, heads, width, length, biased):
        scale2 = LOG2E * width ** -0.5
        for i in idx:
            for h in range(heads):
                part = slice((h % 2) * LANES, (h % 2 + 1) * LANES)
                x = raw[i, h // 2, :length, part]
                if biased:
                    x = x + bias[h]
                e = jnp.exp2((x - jnp.max(x, axis=0, keepdims=True)) * scale2)
                inv[i, h:h + 1, :] = 1.0 / jnp.sum(e, axis=0, keepdims=True)
                prob[i, h // 2, :length, part] = e.astype(BF16)

    def mixed(idx, base, heads, width, length):
        c = heads * width
        raws = [[mm(vbuf[base + i, 2 * p * width:2 * (p + 1) * width, :length], prob[i, p, :length])
                 for p in range(heads // 2)] for i in idx]
        outs = []
        for i, r in zip(idx, raws):
            parts = []
            for p in range(heads // 2):
                parts.append(r[p][:width, :LANES] * inv[i, 2 * p:2 * p + 1, :])
                parts.append(r[p][width:, LANES:] * inv[i, 2 * p + 1:2 * p + 2, :])
            outs.append((jnp.concatenate(parts, axis=0) * gbuf[base + i, :c]).astype(BF16))
        return outs

    pl.semaphore_wait(barrier, n - 1)

    def row_bias(c):
        def step(idx):
            put_bias(stack([layer_norm(z_in[c, i].astype(F32)) for i in idx]), 0, heads_m, idx)
        grouped(res, 12, step)
        ag_r[c, me] = stg_b[...].astype(BF16)
        start(gather_copies(0, c, ag_r))

    loop(crops, row_bias)

    def row_prep(c):
        def prep(idx):
            fill = jnp.zeros((c_m, LANES - n_res), F32)
            ms = [jnp.concatenate([m_in[c, s].astype(F32), fill], axis=1) for s in idx]
            keep(mm(wt_r[...], jnp.concatenate([layer_norm_t(x) for x in ms], axis=1)), c_m,
                 [c * slots + s for s in idx], n_res, [mask_r[c, pl.ds(me * seqs + s, 1), :] for s in idx])
            for s, x in zip(idx, ms):
                xw[c * slots + s] = x
        grouped(seqs, 16, prep)

    loop(crops, row_prep)

    def row_attention(c):
        base = c * slots
        grouped(seqs, 16, lambda idx: logits(idx, base, heads_m, d_m, hm8, n_res, True))
        gather_wait(0, c, ag_r)
        gathered_bias(ag_r, c, heads_m, d_m, True, None)
        grouped(seqs, 4, lambda idx: softmax(idx, heads_m, d_m, n_res, True))

        def step(idx):
            both = [s + t * half for s in idx for t in range(2)]
            upd = mm(wt_ro[...], jnp.concatenate(mixed(both, base, heads_m, d_m, n_res), axis=1))
            new = [xw[base + s] + upd[:, t * LANES:(t + 1) * LANES] for t, s in enumerate(both)]
            for k, s in enumerate(idx):
                x2 = jnp.concatenate(new[2 * k:2 * k + 2], axis=0).T
                stg_m[pl.ds(s, n_res, stride=half), :] = x2[:n_res]
        grouped(half, 8, step)
        for p in range(n):
            snd_m[c, p] = stg_m[p * res * half:(p + 1) * res * half, :].reshape(res, half, LANES).astype(BF16)
        rcv_m[c, me] = snd_m[c, me]
        start(swap_copies(1, c, snd_m, rcv_m))

    loop(crops, row_attention)

    def col_attention(c):
        base = c * slots
        arrivals(1, c, lambda sender: rcv_m.at[c, sender])
        hs = n_seq // 2

        def mask_row(i):
            return mask_t[c, pl.ds(me * SLOT + i, 1), :]

        def prep(idx):
            ys = []
            for k in range(0, len(idx), 2):
                x2 = jnp.concatenate([rcv_m[c, q, i].astype(F32) for i in idx[k:k + 2] for q in range(n)], axis=0).T
                for t, i in enumerate(idx[k:k + 2]):
                    x = jnp.concatenate([x2[:c_m, t * hs:(t + 1) * hs], x2[c_m:, t * hs:(t + 1) * hs]], axis=1)
                    xw[base + i] = x
                    ys.append(layer_norm_t(x))
            keep(mm(wt_c[...], jnp.concatenate(ys, axis=1)), c_m, [base + i for i in idx], LANES,
                 [mask_row(i) for i in idx])
        grouped(res, 12, prep)

        def group(g):
            idx = [g * part_rows + t for t in range(part_rows)]
            logits(idx, base, heads_m, d_m, hm8, LANES, True)
            softmax(idx, heads_m, d_m, LANES, False)
            upd = mm(wt_co[...], jnp.concatenate(mixed(idx, base, heads_m, d_m, LANES), axis=1))
            new = [(xw[base + i] + upd[:, t * LANES:(t + 1) * LANES]).astype(BF16).astype(F32)
                   for t, i in enumerate(idx)]
            ac = mm(w_ac[...], jnp.concatenate([layer_norm_t(x) for x in new], axis=1)).astype(BF16).astype(F32)
            for t, i in enumerate(idx):
                part = ac[:, t * LANES:(t + 1) * LANES] * mask_row(i)
                ag_c[c, g, me, t] = part[o_w:].astype(BF16)
                abuf[c, pl.ds(pl.multiple_of(i * o_w, o_w), o_w), :] = part[:o_w].astype(BF16)
            k = c * pieces + g
            relay_own(k)

            @pl.when(k >= 2)
            def _():
                relay(k - 2)

            for t in range(0, part_rows, 2):
                two = jnp.concatenate([
                    jnp.concatenate([x[:, :hs] for x in new[t:t + 2]], axis=1),
                    jnp.concatenate([x[:, hs:] for x in new[t:t + 2]], axis=1)], axis=0).T
                for u, i in enumerate(idx[t:t + 2]):
                    for q in range(n):
                        snd_b[c, q, i] = two[u * hs + q * half:u * hs + (q + 1) * half].astype(BF16)
        loop(pieces, group)
        rcv_b[c, me] = snd_b[c, me]

    loop(crops, col_attention)

    def outer_product(c):
        base = c * slots
        mloc = mask_t[c, pl.ds(pl.multiple_of(me * SLOT, SLOT), SLOT), :].astype(BF16)
        norm[...] = 1.0 / (mm(mloc, mask_n[c], NT) + OPM_EPS)
        pitch = n_res + 8

        for g in range(pieces):
            relay_done(c * pieces + g)

            def spread(p):
                for t in range(part_rows):
                    stg_c[pl.ds(p * res + g * part_rows + t, o_w, stride=pitch), :] = ag_c[c, g, p, t].astype(F32)
            loop(n, spread)


        def outer(fs):
            rows = [stg_c[pl.ds(pl.multiple_of(f * pitch, 8), n_res), :].astype(BF16) for f in fs]
            outs = [mm(abuf[c], stack(rows[k:k + 2]), NT) for k in range(0, len(fs), 2)]
            for k, f in enumerate(fs):
                out = outs[k // 2][:, (k % 2) * LANES:(k % 2 + 1) * LANES]
                for i in range(res):
                    obuf[i, pl.ds(pl.multiple_of(f * o_w, o_w), o_w), :] = (
                        out[i * o_w:(i + 1) * o_w] * norm[i:i + 1, :]).astype(BF16)
        grouped(o_w, 16, outer)

        @pl.when(c == 0)
        def _():
            relay(n_blocks - 2)

        start(swap_copies(3, c, snd_b, rcv_b))

        def update(idx):
            rhs = [jnp.concatenate([obuf[i] for i in idx[k:k + 2]], axis=1) for k in range(0, len(idx), 2)]
            upds = [mm(w_oo_t[...], r) for r in rhs]
            for k, i in enumerate(idx):
                upd = upds[k // 2][:, (k % 2) * LANES:(k % 2 + 1) * LANES].T
                zw[c, i] = (z_in[c, i].astype(F32) + upd[:n_res]).astype(BF16)
        grouped(res, 12, update)

        def prep(idx):
            y = stack([layer_norm(zw[c, i].astype(F32)) for i in idx])
            put_bias(y, 1, heads_z, idx)
            keep(mm(wt_s[...], y, NT), c_z, [base + i for i in idx], n_res)
        grouped(res, 12, prep)
        @pl.when(c == 0)
        def _():
            relay(n_blocks - 1)

        ag_s[c, me] = stg_b[:heads_z * res, :].astype(BF16)
        start(gather_copies(4, c, ag_s))

    loop(crops, outer_product)

    def res_bias(c):
        return column((res_r[pl.ds(c, 1), :] - 1.0) * (MASK_SCALE * d_z ** 0.5))

    def piece_copies(first, c, g, snd, rcv):
        return copies(first + g, c, lambda peer: snd.at[c, g, peer], rcv.at[c, g, me])

    def send_rows(zs, snd, c, g):
        for t, z in enumerate(zs):
            stg_m[pl.ds(t, n_res, stride=part_rows), :] = z
        size = res * part_rows
        for q in range(n):
            snd[c, g, q] = stg_m[q * size:(q + 1) * size, :].astype(BF16)

    def take_columns(first, c, rcv):
        for g in range(pieces):
            arrivals(first + g, c, lambda sender: rcv.at[c, g, sender])
        for p in range(n):
            for g in range(pieces):
                block = rcv[c, g, p].astype(F32)
                row0 = p * res + g * part_rows
                for j in range(res):
                    xs[j, row0:row0 + part_rows, :] = block[j * part_rows:(j + 1) * part_rows]

    def tri_start(c):
        base = c * slots
        gather_wait(4, c, ag_s)
        gathered_bias(ag_s, c, heads_z, d_z, True, res_bias(c))
        stg_b[...] = jnp.zeros(stg_b.shape, F32)

        def group(g):
            idx = [g * part_rows + t for t in range(part_rows)]
            logits(idx, base, heads_z, d_z, hm4, n_res, False)
            softmax(idx, heads_z, d_z, n_res, True)
            upds = [mm(o, w_so[...], TN) for o in mixed(idx, base, heads_z, d_z, n_res)]
            zs = [(zw[c, i].astype(F32) + upd[:n_res]).astype(BF16).astype(F32) for i, upd in zip(idx, upds)]
            send_rows(zs, snd_z, c, g)
            start(piece_copies(10, c, g, snd_z, rcv_z))
            rcv_z[c, g, me] = snd_z[c, g, me]
            put_bias(stack([layer_norm(z) for z in zs]), 2, heads_z, idx)
        loop(pieces, group)
        ag_e[c, me] = stg_b[:heads_z * res, :].astype(BF16)
        start(gather_copies(5, c, ag_e))

    loop(crops, tri_start)

    def tri_end(c):
        base = c * slots
        take_columns(10, c, rcv_z)

        def prep(idx):
            keep(mm(wt_e[...], stack([layer_norm(xs[j]) for j in idx]), NT), c_z, [base + j for j in idx], n_res)
        grouped(res, 12, prep)
        gather_wait(5, c, ag_e)
        gathered_bias(ag_e, c, heads_z, d_z, False, res_bias(c))

        def step(g):
            idx = [g * part_rows + t for t in range(part_rows)]
            logits(idx, base, heads_z, d_z, hm4, n_res, False)
            softmax(idx, heads_z, d_z, n_res, True)
            upds = [mm(o, w_eo[...], TN) for o in mixed(idx, base, heads_z, d_z, n_res)]
            send_rows([xs[j] + upd[:n_res] for j, upd in zip(idx, upds)], snd_y, c, g)
            start(piece_copies(7, c, g, snd_y, zback))
            zback[c, g, me] = snd_y[c, g, me]
        loop(pieces, step)

    loop(crops, tri_end)

    def put_m(c):
        arrivals(3, c, lambda sender: rcv_b.at[c, sender])
        stg_m[...] = rcv_b[c].astype(F32).reshape(n * res * half, LANES)

        def step(idx):
            for s in idx:
                x2 = stg_m[pl.ds(s, n_res, stride=half), :].T
                m_out[c, s] = x2[:c_m].astype(BF16)
                m_out[c, s + half] = x2[c_m:].astype(BF16)
        grouped(half, 4, step)

    loop(crops, put_m)

    def put_z(c):
        take_columns(7, c, zback)

        def step(i):
            z_out[c, i] = xs[i].astype(BF16)
        for i in range(res):
            step(i)

    loop(crops, put_z)

    def drain(c):
        finish(gather_copies(0, c, ag_r))
        finish(swap_copies(1, c, snd_m, rcv_m))
        for g in range(pieces):
            for slot in range(n - 1):
                block_copy(c * pieces + g, me, device(1), slot).wait_send()
            finish(piece_copies(7, c, g, snd_y, zback))
            finish(piece_copies(10, c, g, snd_z, rcv_z))
        finish(swap_copies(3, c, snd_b, rcv_b))
        finish(gather_copies(4, c, ag_s))
        finish(gather_copies(5, c, ag_e))

    loop(crops, drain)


def solution(mesh):
    n = mesh.shape[GROUP_AXIS]
    rows_spec = P(PART_AXIS, GROUP_AXIS, None, None)
    in_specs = (rows_spec, rows_spec, P(PART_AXIS, None, None), P(PART_AXIS, None)) + (P(),) * N_WEIGHTS

    def local_block(m, z, msa_mask, res_mask, w_rb, w_rq, w_ro, w_cq, w_co, w_ac, w_oo, w_sb, w_sq, w_so,
                    w_eb, w_eq, w_eo):
        crops, seqs, n_res, c_m = m.shape
        res, c_z = z.shape[1], z.shape[3]
        heads_m, heads_z = w_rq.shape[2], w_sq.shape[2]
        o_w = w_ac.shape[2]
        half = seqs // 2
        assert n == 8 and crops == 2 and res % 3 == 0 and n * SLOT == LANES and res <= SLOT and n * seqs == LANES and 2 * c_m == LANES and c_z == LANES
        flat = lambda w: jnp.moveaxis(w, 0, -1).reshape(-1, w.shape[0])
        tall = lambda w: w.reshape(-1, w.shape[-1])
        args = (m.swapaxes(2, 3), z, msa_mask.swapaxes(1, 2), res_mask, w_rb.T, flat(w_rq), tall(w_ro), flat(w_cq),
                tall(w_co), flat(w_ac), tall(w_oo), w_sb.T, flat(w_sq), tall(w_so), w_eb.T, flat(w_eq), tall(w_eo))
        vm = pltpu.VMEM
        slots = max(seqs, res)
        pieces = 2
        piece = res * res // pieces
        scratch = [
            vm((crops, n, heads_m * res, LANES), BF16),
            vm((crops, pieces, n, res // pieces, o_w, LANES), BF16),
            vm((crops, n, heads_z * res, LANES), BF16),
            vm((crops, n, heads_z * res, LANES), BF16),
            vm((crops, n, res, half, LANES), BF16),
            vm((crops, n, res, half, LANES), BF16),
            vm((crops, n, res, half, LANES), BF16),
            vm((crops, n, res, half, LANES), BF16),
            vm((crops, pieces, n, piece, LANES), BF16),
            vm((crops, pieces, n, piece, LANES), BF16),
            vm((crops, pieces, n, piece, LANES), BF16),
            vm((crops, pieces, n, piece, LANES), BF16),
            pltpu.SemaphoreType.DMA((13, crops, n)),
            pltpu.SemaphoreType.DMA((13, crops, n)),
            pltpu.SemaphoreType.DMA((crops * pieces, n)),
            pltpu.SemaphoreType.DMA((crops * pieces, n)),
        ]
        local = [
            vm((crops, res, n_res, LANES), BF16),
            vm((crops * slots, c_m, LANES), F32),
            vm((crops * slots, LANES, LANES), BF16),
            vm((crops * slots, LANES, LANES), BF16),
            vm((crops * slots, LANES, LANES), BF16),
            vm((crops * slots, LANES, LANES), F32),
            vm((heads_m, n_res, LANES), F32),
            vm((res, o_w * o_w, LANES), BF16),
            vm((n * res * half, LANES), F32),
            vm((o_w * (n_res + 8), LANES), F32),
            vm((heads_m * res, LANES), F32),
            vm((n_res * res, LANES), F32),
            vm((crops, res * o_w, LANES), BF16),
            vm((crops, LANES, LANES), F32),
            vm((crops, n * seqs, LANES), F32),
            vm((crops, LANES), F32),
            vm((slots, heads_m // 2, LANES, 2 * LANES), F32),
            vm((slots, heads_m // 2, LANES, 2 * LANES), BF16),
            vm((slots, heads_m, LANES), F32),
            vm((SLOT, LANES), F32),
            vm((heads_m, c_m, LANES), BF16),
            vm((heads_z, c_z, LANES), BF16),
            vm((c_m, c_m), BF16),
            vm((c_m, c_m), BF16),
            vm((LANES, o_w * o_w), BF16),
            vm((3, SLOT, LANES), BF16),
            vm((AUG, LANES), F32),
            vm((AUG, 2 * LANES), BF16),
            vm((res, n_res, LANES), F32),
            vm((crops, LANES, LANES), BF16),
        ]
        cfg = dict(n=n, heads_m=heads_m, heads_z=heads_z, slots=slots, pieces=pieces, local=local)
        spec = pl.BlockSpec(memory_space=pltpu.VMEM)
        m_new, z_new = pl.pallas_call(
            functools.partial(body, cfg),
            out_shape=(jax.ShapeDtypeStruct((crops, seqs, c_m, n_res), BF16), jax.ShapeDtypeStruct(z.shape, BF16)),
            in_specs=[spec] * len(args),
            out_specs=(spec, spec),
            scratch_shapes=scratch,
            compiler_params=pltpu.CompilerParams(collective_id=0, has_side_effects=True,
                                                 vmem_limit_bytes=60 * 1024 * 1024),
        )(*args)
        return m_new.swapaxes(2, 3), z_new

    return jax.shard_map(local_block, mesh=mesh, in_specs=in_specs, out_specs=(rows_spec, rows_spec),
                         check_vma=False)
```

```python
import functools
import math

import jax
import jax.numpy as jnp
import numpy as np
from jax import lax
from jax.experimental import pallas as pl
from jax.experimental.pallas import tpu as pltpu
from jax.sharding import PartitionSpec as P

MASK_SCALE = 10000.0
LN_EPS = 1e-5
OPM_EPS = 1e-3
N_WEIGHTS = 13
PART_AXIS = 'data'
GROUP_AXIS = 'dap'
LOG2E = math.log2(math.e)
AUG = 16
LANES = 128
SLOT = 16
F32 = jnp.float32
BF16 = jnp.bfloat16
NN = (((1,), (0,)), ((), ()))
NT = (((1,), (1,)), ((), ()))
TN = (((0,), (0,)), ((), ()))


def mm(lhs, rhs, dims=NN):
    return lax.dot_general(lhs, rhs, dims, preferred_element_type=F32)


def layer_norm(x_float):
    mean_val = jnp.mean(x_float, axis=-1, keepdims=True)
    centred = x_float - mean_val
    var_val = jnp.mean(centred * centred, axis=-1, keepdims=True)
    return (centred * lax.rsqrt(var_val + LN_EPS)).astype(BF16)


def layer_norm_t(x_float):
    mean_val = jnp.mean(x_float, axis=0, keepdims=True)
    centred = x_float - mean_val
    var_val = jnp.mean(centred * centred, axis=0, keepdims=True)
    return (centred * lax.rsqrt(var_val + LN_EPS)).astype(BF16)


def iota(shape, axis):
    return lax.broadcasted_iota(jnp.int32, shape, axis)


def body(cfg, *refs):
    pl.run_scoped(functools.partial(scoped_body, cfg, refs), *cfg['local'])


def scoped_body(cfg, refs, *local):
    n = cfg['n']
    (m_in, z_in, mask_in, res_in, w_rb, wt_r, w_ro, wt_c, w_co, w_ac, w_oo,
     w_sb, wt_s, w_so, w_eb, wt_e, w_eo, m_out, z_out,
     ag_r, ag_c, ag_s, ag_e, snd_m, rcv_m, snd_b, rcv_b, snd_z, rcv_z, snd_y, zback, send_sem, recv_sem,
     ring_send, ring_recv) = refs
    (zw, xw, kbuf, qbuf, vbuf, gbuf, bias, obuf, stg_m, stg_c, stg_b, stg_z, abuf,
     mask_t, mask_r, res_r, raw, prob, inv, norm, hm8, hm4, wt_ro, wt_co, w_oo_t, wt_b, aug, one_rows, xs, mask_n) = local
    crops, seqs, c_m, n_res = m_in.shape
    res = z_in.shape[1]
    c_z = z_in.shape[3]
    half = seqs // 2
    heads_m, heads_z = cfg['heads_m'], cfg['heads_z']
    d_m, d_z = c_m // heads_m, c_z // heads_z
    n_seq = n * seqs
    slots, pieces = cfg['slots'], cfg['pieces']
    part_rows, n_blocks = res // pieces, crops * pieces
    me = lax.axis_index(GROUP_AXIS)

    barrier = pltpu.get_barrier_semaphore()
    for r in range(1, n):
        pl.semaphore_signal(barrier, inc=1, device_id={GROUP_AXIS: lax.rem(me + r, n)},
                            device_id_type=pl.DeviceIdType.MESH)

    def copies(exch, c, src_of, dst):
        out = []
        for r in range(1, n):
            peer = lax.rem(me + r, n)
            out.append(pltpu.make_async_remote_copy(
                src_ref=src_of(peer), dst_ref=dst, send_sem=send_sem.at[exch, c, r], recv_sem=recv_sem.at[exch, c, r],
                device_id={GROUP_AXIS: peer}, device_id_type=pl.DeviceIdType.MESH))
        return out

    def arrivals(exch, c, slot_of):
        for r in range(1, n):
            sender = lax.rem(me + n - r, n)
            ref = slot_of(sender)
            pltpu.make_async_remote_copy(
                src_ref=ref, dst_ref=ref, send_sem=send_sem.at[exch, c, r], recv_sem=recv_sem.at[exch, c, r],
                device_id={GROUP_AXIS: sender}, device_id_type=pl.DeviceIdType.MESH).wait_recv()

    def gather_copies(exch, c, buf):
        return copies(exch, c, lambda peer: buf.at[c, me], buf.at[c, me])

    def gather_wait(exch, c, buf):
        arrivals(exch, c, lambda sender: buf.at[c, sender])

    def swap_copies(exch, c, snd, rcv):
        return copies(exch, c, lambda peer: snd.at[c, peer], rcv.at[c, me])

    chips, core, chip = n // 2, lax.rem(me, 2), me // 2

    def device(offset, other=False):
        return lax.rem(chip + offset + chips, chips) * 2 + ((1 - core) if other else core)

    def block_copy(k, block, peer, slot):
        c, g = k // pieces, lax.rem(k, pieces)
        return pltpu.make_async_remote_copy(
            src_ref=ag_c.at[c, g, block], dst_ref=ag_c.at[c, g, block], send_sem=ring_send.at[k, slot],
            recv_sem=ring_recv.at[k, block], device_id={GROUP_AXIS: peer}, device_id_type=pl.DeviceIdType.MESH)

    def block_wait(k, block):
        block_copy(k, block, block, 0).wait_recv()

    def relay_own(k):
        for slot in range(chips):
            block_copy(k, me, device(slot, slot == 0), slot).start()

    def relay(k):
        for offset in range(1, chips):
            block_wait(k, device(offset))
        for offset in range(1, chips):
            block_copy(k, device(offset), device(0, True), chips - 1 + offset).start()

    def relay_done(k):
        for offset in range(chips):
            block_wait(k, device(offset, True))

    def start(descs):
        for d in descs:
            d.start()

    def finish(descs):
        for d in descs:
            d.wait_send()

    def loop(count, fn):
        def step(i, carry):
            fn(i)
            return carry
        lax.fori_loop(0, count, step, 0)

    def pad_matrix():
        row, col = iota((LANES, n_res), 0), iota((LANES, n_res), 1)
        hit = (col == (row // SLOT) * res + row % SLOT) & (row % SLOT < res)
        return jnp.where(hit, 1.0, 0.0).astype(BF16)

    def head_rows(heads, width, ref):
        for h in range(heads):
            row = iota((heads * width, LANES), 0)
            ref[h] = jnp.where((row >= h * width) & (row < (h + 1) * width), 1.0, 0.0).astype(BF16)

    pad = pad_matrix()
    tail = jnp.where(iota((n_res, LANES), 0) == iota((n_res, LANES), 1), 1.0, 0.0).astype(BF16)
    head_rows(heads_m, d_m, hm8)
    head_rows(heads_z, d_z, hm4)
    row, col = iota((LANES, LANES), 0), iota((LANES, LANES), 1)
    seq_of = ((col % (n_seq // 2)) // half) * seqs + (col // (n_seq // 2)) * half + col % half
    seq_perm = jnp.where(row == seq_of, 1.0, 0.0).astype(BF16)
    for c in range(crops):
        mask_bf = mask_in[c].astype(F32).astype(BF16)
        mask_t[c] = mm(mm(pad, mask_bf).astype(BF16), seq_perm)
        mask_n[c, :n_res] = mm(mask_bf, seq_perm).astype(BF16)
        mask_n[c, n_res:] = jnp.zeros((LANES - n_res, LANES), BF16)
        mask_r[c] = mm(mask_bf, tail, TN)
    res_r[...] = mm(res_in[...].astype(F32).astype(BF16), tail)
    term = MASK_SCALE * d_m ** 0.5
    aug[...] = jnp.zeros(aug.shape, F32)
    ones = jnp.zeros((AUG, 2 * LANES), F32)
    for k in range(3):
        piece = float(np.array(term, dtype=BF16))
        term = term - piece
        aug[k:k + 1, :] = jnp.full((1, LANES), piece, F32)
        ones = jnp.where(iota(ones.shape, 0) == k, 1.0, ones)
    one_rows[...] = ones.astype(BF16)
    for k, w in enumerate((w_rb, w_sb, w_eb)):
        wt_b[k] = jnp.zeros(wt_b.shape[1:], BF16)
        wt_b[k, :w.shape[0], :] = w[...]
    wt_ro[...] = w_ro[...].astype(F32).T.astype(BF16)
    wt_co[...] = w_co[...].astype(F32).T.astype(BF16)
    o_w = w_ac.shape[0] // 2
    stg_z[:o_w * o_w, :] = w_oo[...].astype(F32)
    for k in range(0, o_w, LANES // o_w):
        rows = [stg_z[pl.ds(f, o_w, stride=o_w), :] for f in range(k, k + LANES // o_w)]
        w_oo_t[:, k * o_w:k * o_w + LANES] = jnp.concatenate(rows, axis=0).T.astype(BF16)

    stg_b[...] = jnp.zeros(stg_b.shape, F32)

    def grouped(count, size, fn):
        while count % size:
            size -= 1

        def step(b, carry):
            fn([b * size + t for t in range(size)])
            return carry
        lax.fori_loop(0, count // size, step, 0)

    def put_bias(y, k, heads, rows):
        b = mm(wt_b[k], y, NT)
        for t, i in enumerate(rows):
            for h in range(heads):
                stg_b[pl.ds(h * res + i, 1), :] = b[h:h + 1, t * LANES:(t + 1) * LANES]

    def stack(ys):
        fill = jnp.zeros((LANES - n_res, ys[0].shape[1]), BF16)
        return jnp.concatenate([part for y in ys for part in (y, fill)], axis=0)

    def keep(p, width, slots, length, mask_rows=None):
        for t, slot in enumerate(slots):
            part = slice(t * LANES, (t + 1) * LANES)
            keys = p[width:2 * width, part]
            if mask_rows is not None:
                keys = jnp.concatenate([keys, (mask_rows[t] - 1.0) * aug[...]], axis=0)
            qbuf[slot, :width] = p[:width, part].astype(BF16)
            kbuf[slot, :length, :keys.shape[0]] = keys.T[:length].astype(BF16)
            vbuf[slot, :width] = p[2 * width:3 * width, part].astype(BF16)
            gbuf[slot, :width] = jax.nn.sigmoid(p[3 * width:, part])

    def column(rowvec):
        return jnp.broadcast_to(rowvec, (LANES, LANES)).T[:n_res]

    def gathered_bias(buf, c, heads, width, flip, add):
        parts = [buf[c, p].astype(F32) for p in range(n)]
        for h in range(heads):
            b = jnp.concatenate([part[h * res:(h + 1) * res] for part in parts], axis=0)
            if flip:
                b = jnp.concatenate([b, jnp.zeros((LANES - n_res, LANES), F32)], axis=0).T[:n_res]
            b = b * width ** 0.5
            bias[h] = b if add is None else b + add

    def logits(idx, base, heads, width, head_mask, length, masked):
        c = heads * width
        for i in idx:
            q_t, keys = qbuf[base + i, :c], kbuf[base + i, :length, :c + (AUG if masked else 0)]
            for pair in range(heads // 2):
                rhs = jnp.concatenate([q_t * head_mask[2 * pair], q_t * head_mask[2 * pair + 1]], axis=1)
                if masked:
                    rhs = jnp.concatenate([rhs, one_rows[...]], axis=0)
                raw[i, pair, :length] = mm(keys, rhs)

    def softmax(idx, heads, width, length, biased):
        scale2 = LOG2E * width ** -0.5
        for i in idx:
            for h in range(heads):
                part = slice((h % 2) * LANES, (h % 2 + 1) * LANES)
                x = raw[i, h // 2, :length, part]
                if biased:
                    x = x + bias[h]
                e = jnp.exp2((x - jnp.max(x, axis=0, keepdims=True)) * scale2)
                inv[i, h:h + 1, :] = 1.0 / jnp.sum(e, axis=0, keepdims=True)
                prob[i, h // 2, :length, part] = e.astype(BF16)

    def mixed(idx, base, heads, width, length):
        c = heads * width
        raws = [[mm(vbuf[base + i, 2 * p * width:2 * (p + 1) * width, :length], prob[i, p, :length])
                 for p in range(heads // 2)] for i in idx]
        outs = []
        for i, r in zip(idx, raws):
            parts = []
            for p in range(heads // 2):
                parts.append(r[p][:width, :LANES] * inv[i, 2 * p:2 * p + 1, :])
                parts.append(r[p][width:, LANES:] * inv[i, 2 * p + 1:2 * p + 2, :])
            outs.append((jnp.concatenate(parts, axis=0) * gbuf[base + i, :c]).astype(BF16))
        return outs

    pl.semaphore_wait(barrier, n - 1)

    def row_bias(c):
        def step(idx):
            put_bias(stack([layer_norm(z_in[c, i].astype(F32)) for i in idx]), 0, heads_m, idx)
        grouped(res, 12, step)
        ag_r[c, me] = stg_b[...].astype(BF16)
        start(gather_copies(0, c, ag_r))

    loop(crops, row_bias)

    def row_prep(c):
        def prep(idx):
            fill = jnp.zeros((c_m, LANES - n_res), F32)
            ms = [jnp.concatenate([m_in[c, s].astype(F32), fill], axis=1) for s in idx]
            keep(mm(wt_r[...], jnp.concatenate([layer_norm_t(x) for x in ms], axis=1)), c_m,
                 [c * slots + s for s in idx], n_res, [mask_r[c, pl.ds(me * seqs + s, 1), :] for s in idx])
            for s, x in zip(idx, ms):
                xw[c * slots + s] = x
        grouped(seqs, 16, prep)

    loop(crops, row_prep)

    def row_attention(c):
        base = c * slots
        grouped(seqs, 16, lambda idx: logits(idx, base, heads_m, d_m, hm8, n_res, True))
        gather_wait(0, c, ag_r)
        gathered_bias(ag_r, c, heads_m, d_m, True, None)
        grouped(seqs, 4, lambda idx: softmax(idx, heads_m, d_m, n_res, True))

        def step(idx):
            both = [s + t * half for s in idx for t in range(2)]
            upd = mm(wt_ro[...], jnp.concatenate(mixed(both, base, heads_m, d_m, n_res), axis=1))
            new = [xw[base + s] + upd[:, t * LANES:(t + 1) * LANES] for t, s in enumerate(both)]
            for k, s in enumerate(idx):
                x2 = jnp.concatenate(new[2 * k:2 * k + 2], axis=0).T
                stg_m[pl.ds(s, n_res, stride=half), :] = x2[:n_res]
        grouped(half, 8, step)
        for p in range(n):
            snd_m[c, p] = stg_m[p * res * half:(p + 1) * res * half, :].reshape(res, half, LANES).astype(BF16)
        rcv_m[c, me] = snd_m[c, me]
        start(swap_copies(1, c, snd_m, rcv_m))

    loop(crops, row_attention)

    def col_attention(c):
        base = c * slots
        arrivals(1, c, lambda sender: rcv_m.at[c, sender])
        hs = n_seq // 2

        def mask_row(i):
            return mask_t[c, pl.ds(me * SLOT + i, 1), :]

        def prep(idx):
            ys = []
            for k in range(0, len(idx), 2):
                x2 = jnp.concatenate([rcv_m[c, q, i].astype(F32) for i in idx[k:k + 2] for q in range(n)], axis=0).T
                for t, i in enumerate(idx[k:k + 2]):
                    x = jnp.concatenate([x2[:c_m, t * hs:(t + 1) * hs], x2[c_m:, t * hs:(t + 1) * hs]], axis=1)
                    xw[base + i] = x
                    ys.append(layer_norm_t(x))
            keep(mm(wt_c[...], jnp.concatenate(ys, axis=1)), c_m, [base + i for i in idx], LANES,
                 [mask_row(i) for i in idx])
        grouped(res, 12, prep)

        def group(g):
            idx = [g * part_rows + t for t in range(part_rows)]
            logits(idx, base, heads_m, d_m, hm8, LANES, True)
            softmax(idx, heads_m, d_m, LANES, False)
            upd = mm(wt_co[...], jnp.concatenate(mixed(idx, base, heads_m, d_m, LANES), axis=1))
            new = [(xw[base + i] + upd[:, t * LANES:(t + 1) * LANES]).astype(BF16).astype(F32)
                   for t, i in enumerate(idx)]
            ac = mm(w_ac[...], jnp.concatenate([layer_norm_t(x) for x in new], axis=1)).astype(BF16).astype(F32)
            for t, i in enumerate(idx):
                part = ac[:, t * LANES:(t + 1) * LANES] * mask_row(i)
                ag_c[c, g, me, t] = part[o_w:].astype(BF16)
                abuf[c, pl.ds(pl.multiple_of(i * o_w, o_w), o_w), :] = part[:o_w].astype(BF16)
            k = c * pieces + g
            relay_own(k)

            @pl.when(k >= 2)
            def _():
                relay(k - 2)

            for t in range(0, part_rows, 2):
                two = jnp.concatenate([
                    jnp.concatenate([x[:, :hs] for x in new[t:t + 2]], axis=1),
                    jnp.concatenate([x[:, hs:] for x in new[t:t + 2]], axis=1)], axis=0).T
                for u, i in enumerate(idx[t:t + 2]):
                    for q in range(n):
                        snd_b[c, q, i] = two[u * hs + q * half:u * hs + (q + 1) * half].astype(BF16)
        loop(pieces, group)
        rcv_b[c, me] = snd_b[c, me]

    loop(crops, col_attention)

    def outer_product(c):
        base = c * slots
        mloc = mask_t[c, pl.ds(pl.multiple_of(me * SLOT, SLOT), SLOT), :].astype(BF16)
        norm[...] = 1.0 / (mm(mloc, mask_n[c], NT) + OPM_EPS)
        pitch = n_res + 8

        for g in range(pieces):
            relay_done(c * pieces + g)

            def spread(p):
                for t in range(part_rows):
                    stg_c[pl.ds(p * res + g * part_rows + t, o_w, stride=pitch), :] = ag_c[c, g, p, t].astype(F32)
            loop(n, spread)


        def outer(fs):
            rows = [stg_c[pl.ds(pl.multiple_of(f * pitch, 8), n_res), :].astype(BF16) for f in fs]
            outs = [mm(abuf[c], stack(rows[k:k + 2]), NT) for k in range(0, len(fs), 2)]
            for k, f in enumerate(fs):
                out = outs[k // 2][:, (k % 2) * LANES:(k % 2 + 1) * LANES]
                for i in range(res):
                    obuf[i, pl.ds(pl.multiple_of(f * o_w, o_w), o_w), :] = (
                        out[i * o_w:(i + 1) * o_w] * norm[i:i + 1, :]).astype(BF16)
        grouped(o_w, 16, outer)

        start(swap_copies(3, c, snd_b, rcv_b))

        def update(idx):
            rhs = [jnp.concatenate([obuf[i] for i in idx[k:k + 2]], axis=1) for k in range(0, len(idx), 2)]
            upds = [mm(w_oo_t[...], r) for r in rhs]
            for k, i in enumerate(idx):
                upd = upds[k // 2][:, (k % 2) * LANES:(k % 2 + 1) * LANES].T
                zw[c, i] = (z_in[c, i].astype(F32) + upd[:n_res]).astype(BF16)
        grouped(res, 12, update)

        @pl.when(c == 0)
        def _():
            relay(n_blocks - 2)

        def prep(idx):
            y = stack([layer_norm(zw[c, i].astype(F32)) for i in idx])
            put_bias(y, 1, heads_z, idx)
            keep(mm(wt_s[...], y, NT), c_z, [base + i for i in idx], n_res)
        grouped(res, 12, prep)
        @pl.when(c == 0)
        def _():
            relay(n_blocks - 1)

        ag_s[c, me] = stg_b[:heads_z * res, :].astype(BF16)
        start(gather_copies(4, c, ag_s))

    loop(crops, outer_product)

    def res_bias(c):
        return column((res_r[pl.ds(c, 1), :] - 1.0) * (MASK_SCALE * d_z ** 0.5))

    def piece_copies(first, c, g, snd, rcv):
        return copies(first + g, c, lambda peer: snd.at[c, g, peer], rcv.at[c, g, me])

    def send_rows(zs, snd, c, g):
        for t, z in enumerate(zs):
            stg_m[pl.ds(t, n_res, stride=part_rows), :] = z
        size = res * part_rows
        for q in range(n):
            snd[c, g, q] = stg_m[q * size:(q + 1) * size, :].astype(BF16)

    def take_columns(first, c, rcv):
        for g in range(pieces):
            arrivals(first + g, c, lambda sender: rcv.at[c, g, sender])
        for p in range(n):
            for g in range(pieces):
                block = rcv[c, g, p].astype(F32)
                row0 = p * res + g * part_rows
                for j in range(res):
                    xs[j, row0:row0 + part_rows, :] = block[j * part_rows:(j + 1) * part_rows]

    def tri_start(c):
        base = c * slots
        gather_wait(4, c, ag_s)
        gathered_bias(ag_s, c, heads_z, d_z, True, res_bias(c))
        stg_b[...] = jnp.zeros(stg_b.shape, F32)

        def group(g):
            idx = [g * part_rows + t for t in range(part_rows)]
            logits(idx, base, heads_z, d_z, hm4, n_res, False)
            softmax(idx, heads_z, d_z, n_res, True)
            upds = [mm(o, w_so[...], TN) for o in mixed(idx, base, heads_z, d_z, n_res)]
            zs = [(zw[c, i].astype(F32) + upd[:n_res]).astype(BF16).astype(F32) for i, upd in zip(idx, upds)]
            send_rows(zs, snd_z, c, g)
            start(piece_copies(10, c, g, snd_z, rcv_z))
            rcv_z[c, g, me] = snd_z[c, g, me]
            put_bias(stack([layer_norm(z) for z in zs]), 2, heads_z, idx)
        loop(pieces, group)
        ag_e[c, me] = stg_b[:heads_z * res, :].astype(BF16)
        start(gather_copies(5, c, ag_e))

    loop(crops, tri_start)

    def tri_end(c):
        base = c * slots
        take_columns(10, c, rcv_z)

        def prep(idx):
            keep(mm(wt_e[...], stack([layer_norm(xs[j]) for j in idx]), NT), c_z, [base + j for j in idx], n_res)
        grouped(res, 12, prep)
        gather_wait(5, c, ag_e)
        gathered_bias(ag_e, c, heads_z, d_z, False, res_bias(c))

        def step(g):
            idx = [g * part_rows + t for t in range(part_rows)]
            logits(idx, base, heads_z, d_z, hm4, n_res, False)
            softmax(idx, heads_z, d_z, n_res, True)
            upds = [mm(o, w_eo[...], TN) for o in mixed(idx, base, heads_z, d_z, n_res)]
            send_rows([xs[j] + upd[:n_res] for j, upd in zip(idx, upds)], snd_y, c, g)
            start(piece_copies(7, c, g, snd_y, zback))
            zback[c, g, me] = snd_y[c, g, me]
        loop(pieces, step)

    loop(crops, tri_end)

    def put_m(c):
        arrivals(3, c, lambda sender: rcv_b.at[c, sender])
        stg_m[...] = rcv_b[c].astype(F32).reshape(n * res * half, LANES)

        def step(idx):
            for s in idx:
                x2 = stg_m[pl.ds(s, n_res, stride=half), :].T
                m_out[c, s] = x2[:c_m].astype(BF16)
                m_out[c, s + half] = x2[c_m:].astype(BF16)
        grouped(half, 4, step)

    loop(crops, put_m)

    def put_z(c):
        take_columns(7, c, zback)

        def step(i):
            z_out[c, i] = xs[i].astype(BF16)
        for i in range(res):
            step(i)

    loop(crops, put_z)

    def drain(c):
        finish(gather_copies(0, c, ag_r))
        finish(swap_copies(1, c, snd_m, rcv_m))
        for g in range(pieces):
            for slot in range(n - 1):
                block_copy(c * pieces + g, me, device(1), slot).wait_send()
            finish(piece_copies(7, c, g, snd_y, zback))
            finish(piece_copies(10, c, g, snd_z, rcv_z))
        finish(swap_copies(3, c, snd_b, rcv_b))
        finish(gather_copies(4, c, ag_s))
        finish(gather_copies(5, c, ag_e))

    loop(crops, drain)


def solution(mesh):
    n = mesh.shape[GROUP_AXIS]
    rows_spec = P(PART_AXIS, GROUP_AXIS, None, None)
    in_specs = (rows_spec, rows_spec, P(PART_AXIS, None, None), P(PART_AXIS, None)) + (P(),) * N_WEIGHTS

    def local_block(m, z, msa_mask, res_mask, w_rb, w_rq, w_ro, w_cq, w_co, w_ac, w_oo, w_sb, w_sq, w_so,
                    w_eb, w_eq, w_eo):
        crops, seqs, n_res, c_m = m.shape
        res, c_z = z.shape[1], z.shape[3]
        heads_m, heads_z = w_rq.shape[2], w_sq.shape[2]
        o_w = w_ac.shape[2]
        half = seqs // 2
        assert n == 8 and crops == 2 and res % 3 == 0 and n * SLOT == LANES and res <= SLOT and n * seqs == LANES and 2 * c_m == LANES and c_z == LANES
        flat = lambda w: jnp.moveaxis(w, 0, -1).reshape(-1, w.shape[0])
        tall = lambda w: w.reshape(-1, w.shape[-1])
        args = (m.swapaxes(2, 3), z, msa_mask.swapaxes(1, 2), res_mask, w_rb.T, flat(w_rq), tall(w_ro), flat(w_cq),
                tall(w_co), flat(w_ac), tall(w_oo), w_sb.T, flat(w_sq), tall(w_so), w_eb.T, flat(w_eq), tall(w_eo))
        vm = pltpu.VMEM
        slots = max(seqs, res)
        pieces = 2
        piece = res * res // pieces
        scratch = [
            vm((crops, n, heads_m * res, LANES), BF16),
            vm((crops, pieces, n, res // pieces, o_w, LANES), BF16),
            vm((crops, n, heads_z * res, LANES), BF16),
            vm((crops, n, heads_z * res, LANES), BF16),
            vm((crops, n, res, half, LANES), BF16),
            vm((crops, n, res, half, LANES), BF16),
            vm((crops, n, res, half, LANES), BF16),
            vm((crops, n, res, half, LANES), BF16),
            vm((crops, pieces, n, piece, LANES), BF16),
            vm((crops, pieces, n, piece, LANES), BF16),
            vm((crops, pieces, n, piece, LANES), BF16),
            vm((crops, pieces, n, piece, LANES), BF16),
            pltpu.SemaphoreType.DMA((13, crops, n)),
            pltpu.SemaphoreType.DMA((13, crops, n)),
            pltpu.SemaphoreType.DMA((crops * pieces, n)),
            pltpu.SemaphoreType.DMA((crops * pieces, n)),
        ]
        local = [
            vm((crops, res, n_res, LANES), BF16),
            vm((crops * slots, c_m, LANES), F32),
            vm((crops * slots, LANES, LANES), BF16),
            vm((crops * slots, LANES, LANES), BF16),
            vm((crops * slots, LANES, LANES), BF16),
            vm((crops * slots, LANES, LANES), F32),
            vm((heads_m, n_res, LANES), F32),
            vm((res, o_w * o_w, LANES), BF16),
            vm((n * res * half, LANES), F32),
            vm((o_w * (n_res + 8), LANES), F32),
            vm((heads_m * res, LANES), F32),
            vm((n_res * res, LANES), F32),
            vm((crops, res * o_w, LANES), BF16),
            vm((crops, LANES, LANES), F32),
            vm((crops, n * seqs, LANES), F32),
            vm((crops, LANES), F32),
            vm((slots, heads_m // 2, LANES, 2 * LANES), F32),
            vm((slots, heads_m // 2, LANES, 2 * LANES), BF16),
            vm((slots, heads_m, LANES), F32),
            vm((SLOT, LANES), F32),
            vm((heads_m, c_m, LANES), BF16),
            vm((heads_z, c_z, LANES), BF16),
            vm((c_m, c_m), BF16),
            vm((c_m, c_m), BF16),
            vm((LANES, o_w * o_w), BF16),
            vm((3, SLOT, LANES), BF16),
            vm((AUG, LANES), F32),
            vm((AUG, 2 * LANES), BF16),
            vm((res, n_res, LANES), F32),
            vm((crops, LANES, LANES), BF16),
        ]
        cfg = dict(n=n, heads_m=heads_m, heads_z=heads_z, slots=slots, pieces=pieces, local=local)
        spec = pl.BlockSpec(memory_space=pltpu.VMEM)
        m_new, z_new = pl.pallas_call(
            functools.partial(body, cfg),
            out_shape=(jax.ShapeDtypeStruct((crops, seqs, c_m, n_res), BF16), jax.ShapeDtypeStruct(z.shape, BF16)),
            in_specs=[spec] * len(args),
            out_specs=(spec, spec),
            scratch_shapes=scratch,
            compiler_params=pltpu.CompilerParams(collective_id=0, has_side_effects=True,
                                                 vmem_limit_bytes=60 * 1024 * 1024),
        )(*args)
        return m_new.swapaxes(2, 3), z_new

    return jax.shard_map(local_block, mesh=mesh, in_specs=in_specs, out_specs=(rows_spec, rows_spec),
                         check_vma=False)
```
